256 devices in a mesh: member: 2 (over z), graph: 64 (over y, x), chan: 2 (over core).
Axes of the slice: x: 8, y: 8, z: 2, core: 2. Of those that a mesh axis runs over, the one named last changes fastest.
The devices are a block of a 8x8x16 slice.
Arguments:
- grid_state: bfloat16 [131072, 256], P(('member', 'graph')), parts along dimension 0, may hold values from -6 to 6
- w_src: bfloat16 [256, 512], P(None, 'chan'), may hold values from -0.375 to 0.375
- bias_src: float32 [512], P('chan'), may hold values from -3 to 3
- mesh_embed: bfloat16 [40960, 512], P('graph', 'chan'), may hold values from -6 to 6
- w_node: bfloat16 [512, 512], P('chan'), may hold values from -0.25 to 0.25
- w_dec: bfloat16 [512, 256], P('chan'), may hold values from -0.125 to 0.125
- slot_src: int32 [64, 64, 128], P('graph'), may hold values from 0 to 1023, as said below
- slot_dst: int32 [64, 64, 128], P(None, 'graph'), may hold values from 0 to 639, as said below
- slot_count: int32 [64, 64], replicated, may hold values from 1 to 128, as said below
Outputs:
- grid_out: bfloat16 [131072, 256], P(('member', 'graph'), 'chan'), parts along dimension 0
The draws below stay inside these ranges and needn't reach their ends.
There are 2 independent parts, one for each index of `member`. The reference program is written for one: setup_inputs(seed, part) draws one part's arguments, and reference() takes and returns one part's arrays. A program takes and returns all parts, laid end to end along the dimension named above; an argument that names none is the same for every part. Nothing has to cross between parts.
Inputs may be any that keep to these rules, and one draw needn't show every extreme that they name: `slot_src`: slots at or past the live count hold arbitrary values in the same range. `slot_dst`: slots at or past the live count hold arbitrary values in the same range. slot_count[s, d] counts the live leading slots of the 128 from shard s to shard d; in every draw some receiving shard has all 128 slots live from every sender.
All inputs are finite; a program needn't handle non-finite values.
Results may differ from the reference program's by a relative error of at most 0.0056.
Values may be sent and summed in bfloat16 or wider, within the bound.
A program may use at most 64 MiB of HBM per device.

```python
import jax
import jax.numpy as jnp
from jax import lax

C = 256
H = 512
GD = 1024
MD = 640
CAP = 128
G = 65536
M = 40960
N_GRAPH = 64


def edge_tables(key):
    owners = jnp.arange(N_GRAPH, dtype=jnp.int32)
    offset = jnp.abs(owners[:, None] - owners[None, :])
    cycle_gap = jnp.minimum(offset, N_GRAPH - offset)
    near_bits = jax.random.randint(jax.random.fold_in(key, 12), (N_GRAPH, N_GRAPH), 0, 1 << 20)
    near_count = CAP // 2 + near_bits % (CAP - CAP // 2 + 1)
    levels = jax.random.randint(jax.random.fold_in(key, 11), (N_GRAPH,), 1, 5)
    tail_top = jnp.maximum(levels * (CAP // 16), 1)
    tail_bits = jax.random.randint(jax.random.fold_in(key, 14), (N_GRAPH, N_GRAPH), 0, 1 << 20)
    tail_pick = jax.random.randint(jax.random.fold_in(key, 15), (N_GRAPH, N_GRAPH), 0, 8)
    tail_count = jnp.where(tail_pick == 0, 1 + tail_bits % tail_top[None, :], 1)
    counts = jnp.where(cycle_gap <= 2, near_count, tail_count)
    fullest = jax.random.randint(jax.random.fold_in(key, 13), (), 0, N_GRAPH)
    return jnp.where(owners[None, :] == fullest, CAP, counts).astype(jnp.int32)


def draw_slot_count(key, part):
    return edge_tables(key)


def draw_slot_src(key, part):
    return jax.random.randint(jax.random.fold_in(key, 21), (N_GRAPH, N_GRAPH, CAP), 0, GD).astype(jnp.int32)


def draw_slot_dst(key, part):
    return jax.random.randint(jax.random.fold_in(key, 31), (N_GRAPH, N_GRAPH, CAP), 0, MD).astype(jnp.int32)


def block_scale(own_key, shape, shards, low, high):
    gain = 1.0
    for axis_at, blocks in shards:
        steps = jax.random.uniform(jax.random.fold_in(jax.random.fold_in(own_key, 6), axis_at), (blocks,), jnp.float32, low / len(shards), high / len(shards))
        gain = gain * jnp.repeat(jnp.exp(steps), shape[axis_at] // blocks).reshape((-1,) + (1,) * (len(shape) - 1 - axis_at))
    return gain


def scatter_about(rng, extent, spread, reach, cuts=(), kind=jnp.bfloat16):
    gain = block_scale(rng, extent, cuts, -0.22, 0.18) if cuts else 1.0
    array = jax.random.normal(rng, extent, jnp.float32) * spread * gain
    return jnp.minimum(jnp.maximum(array, -reach), reach).astype(kind)


def setup_inputs(seed: int = 0, part: int = 0) -> dict:
    arg_keys = jax.random.split(jax.random.key(seed), 10)
    own_keys = jax.random.split(jax.random.fold_in(arg_keys[9], part), 10)
    grid_state = scatter_about(own_keys[0], (G, C), 1.0, 6.0, ((0, 64),))
    w_src = scatter_about(arg_keys[1], (C, H), C ** -0.5, 0.375, ((1, 2),))
    bias_src = scatter_about(arg_keys[2], (H,), 0.5, 3.0, ((0, 2),), jnp.float32)
    mesh_embed = scatter_about(arg_keys[3], (M, H), 1.0, 6.0, ((0, 64), (1, 2)))
    w_node = scatter_about(arg_keys[4], (H, H), H ** -0.5, 0.25, ((0, 2),))
    w_dec = scatter_about(arg_keys[5], (H, C), (4 * H) ** -0.5, 0.125, ((0, 2),))
    slot_src = draw_slot_src(jax.random.fold_in(arg_keys[9], 71), part)
    slot_dst = draw_slot_dst(jax.random.fold_in(arg_keys[9], 71), part)
    slot_count = draw_slot_count(jax.random.fold_in(arg_keys[9], 71), part)
    return {"grid_state": grid_state, "w_src": w_src, "bias_src": bias_src, "mesh_embed": mesh_embed, "w_node": w_node, "w_dec": w_dec, "slot_src": slot_src, "slot_dst": slot_dst, "slot_count": slot_count}


def reference(grid_state, w_src, bias_src, mesh_embed, w_node, w_dec, slot_src, slot_dst, slot_count):
    positions = jnp.arange(CAP, dtype=jnp.int32)
    owners = jnp.arange(N_GRAPH, dtype=jnp.int32)

    def send_part(aggregate, sender):
        picked = jnp.take(grid_state, (sender * GD + slot_src[sender]).reshape(-1), axis=0)
        messages = jax.nn.silu(jnp.dot(picked, w_src, preferred_element_type=jnp.float32) + bias_src).astype(jnp.bfloat16)
        usable = (positions[None, :] < slot_count[sender][:, None]).reshape(-1)
        mesh_ids = (owners[:, None] * MD + slot_dst[sender]).reshape(-1).astype(jnp.int32)
        terms = jnp.where(usable[:, None], messages.astype(jnp.float32), jnp.zeros((), jnp.float32))
        return aggregate + jax.ops.segment_sum(terms, mesh_ids, num_segments=N_GRAPH * MD), None

    aggregate, unused = lax.scan(send_part, jnp.zeros((N_GRAPH * MD, H), jnp.float32), owners)
    hidden_pre = jnp.dot(aggregate.astype(jnp.bfloat16), w_node, preferred_element_type=jnp.float32)
    latent = (mesh_embed.astype(jnp.float32) + jax.nn.silu(hidden_pre)).astype(jnp.bfloat16)
    projected = jnp.dot(latent, w_dec, preferred_element_type=jnp.float32).astype(jnp.bfloat16)

    def decode_part(sender):
        usable = (positions[None, :] < slot_count[sender][:, None]).reshape(-1)
        mesh_ids = (owners[:, None] * MD + slot_dst[sender]).reshape(-1).astype(jnp.int32)
        returned = jnp.where(usable[:, None], jnp.take(projected, mesh_ids, axis=0).astype(jnp.float32), jnp.zeros((), jnp.float32))
        decoded = jax.ops.segment_sum(returned, slot_src[sender].reshape(-1).astype(jnp.int32), num_segments=GD)
        own_rows = lax.dynamic_slice_in_dim(grid_state, (sender * GD).astype(jnp.int32), GD, 0)
        return (own_rows.astype(jnp.float32) + decoded).astype(jnp.bfloat16)

    return lax.map(decode_part, owners).reshape(N_GRAPH * GD, C)
```

```python
import functools
import math

import jax
import jax.numpy as jnp
from jax import lax
from jax.experimental import pallas as pl
from jax.experimental.pallas import tpu as pltpu
from jax.sharding import PartitionSpec as P

MESH_ID = pl.DeviceIdType.MESH
KEEP = 32
HALF = KEEP // 2
REACH = 2
OWN = 16
NEAR_ROWS = 256
CHUNK = 256

def split_up(value, dim, count):
    lengths = value.shape
    parts = value.reshape(*lengths[:dim], count, lengths[dim] // count, *lengths[dim + 1 :])
    return jnp.moveaxis(parts, dim, 0)


def sum_at_owner(value, axis, dim):
    parts = split_up(value, dim, lax.axis_size(axis))
    arrived = lax.all_to_all(parts, axis, split_axis=0, concat_axis=0, tiled=True)
    return arrived.sum(axis=0)


def edge_network(source_rows, w_src, bias_src):
    return jax.nn.silu(
        jnp.dot(source_rows, w_src, preferred_element_type=jnp.float32) + bias_src
    ).astype(jnp.bfloat16)


def segment_rows(values, indices, usable, row_count):
    slot_total = values.shape[0]
    width = values.shape[1]
    block_len = math.gcd(slot_total, 2048)
    block_count = slot_total // block_len
    targets = jnp.where(usable, indices, -1).reshape(block_count, block_len)
    pieces = values.reshape(block_count, block_len, width)
    row_ids = jnp.arange(row_count, dtype=jnp.int32)

    def add_block(summed, scan_item):
        row_target, piece_vals = scan_item
        one_hot = (row_ids[:, None] == row_target[None, :]).astype(jnp.bfloat16)
        return (summed + jnp.dot(one_hot, piece_vals, preferred_element_type=jnp.float32), None)

    result, unused = lax.scan(
        add_block, jnp.zeros((row_count, width), jnp.float32), (targets, pieces)
    )
    return result


def dense(
    grid_state, w_src, bias_src, mesh_embed, w_node, w_dec, slot_src, slot_dst, slot_count
):
    peers = lax.axis_size("graph")
    own_index = lax.axis_index("graph")
    core_index = lax.axis_index("chan")
    capacity = slot_src.shape[2]
    positions = jnp.arange(capacity, dtype=jnp.int32)
    grid_rows = grid_state.shape[0]
    mesh_rows = mesh_embed.shape[0]
    sent_counts = lax.dynamic_slice_in_dim(slot_count, own_index, 1, 0)[0]
    recv_counts = lax.dynamic_slice_in_dim(slot_count, own_index, 1, 1)[:, 0]
    half_slots = capacity // 2
    chosen = lax.dynamic_slice_in_dim(slot_src[0], core_index * half_slots, half_slots, 1)
    picked = jnp.take(grid_state, chosen.reshape(-1), axis=0).reshape(
        peers, half_slots, grid_state.shape[1]
    )
    arrived = lax.all_to_all(picked, "graph", split_axis=0, concat_axis=0, tiled=True)
    joined = lax.all_gather(arrived, "chan", axis=1, tiled=True)
    messages = edge_network(joined.reshape(peers * capacity, grid_state.shape[1]), w_src, bias_src)
    arrive_ok = (positions[None, :] < recv_counts[:, None]).reshape(-1)
    dst_rows = slot_dst[:, 0, :].reshape(-1)
    aggregate = segment_rows(messages, dst_rows, arrive_ok, mesh_rows)
    partial_hidden = jnp.dot(
        aggregate.astype(jnp.bfloat16), w_node, preferred_element_type=jnp.float32
    )
    hidden_pre = sum_at_owner(partial_hidden, "chan", 1)
    latent = (mesh_embed.astype(jnp.float32) + jax.nn.silu(hidden_pre)).astype(jnp.bfloat16)
    partial_proj = jnp.dot(latent, w_dec, preferred_element_type=jnp.float32)
    projected = sum_at_owner(partial_proj, "chan", 1).astype(jnp.bfloat16)
    returned = jnp.take(projected, dst_rows, axis=0).reshape(peers, capacity, projected.shape[1])
    came_back = lax.all_to_all(returned, "graph", split_axis=0, concat_axis=0, tiled=True).reshape(
        peers * capacity, projected.shape[1]
    )
    send_ok = (positions[None, :] < sent_counts[:, None]).reshape(-1)
    decoded = segment_rows(came_back, slot_src[0].reshape(-1), send_ok, grid_rows)
    width_half = decoded.shape[1]
    own_cols = lax.dynamic_slice_in_dim(grid_state, core_index * width_half, width_half, 1)
    return (own_cols.astype(jnp.float32) + decoded).astype(jnp.bfloat16)


def silu(v):
    return v / (1.0 + jnp.exp(-v))


def pick_turned(table, idx):
    rows = table.shape[0]
    hot = jnp.where(
        lax.broadcasted_iota(jnp.int32, (rows, idx.shape[1]), 0) == idx, 1.0, 0.0
    ).astype(jnp.bfloat16)
    return lax.dot_general(table, hot, (((0,), (0,)), ((), ())), preferred_element_type=jnp.float32)


def spread(rows, idx):
    return jnp.where(
        lax.broadcasted_iota(jnp.int32, (rows, idx.shape[1]), 0) == idx, 1.0, 0.0
    ).astype(jnp.bfloat16)


def step_kernel(
    n, hot_ref, grid_ref, wsrc_ref, bias_ref, embed_ref, wnode_ref, wdec_ref,
    srcx_ref, dstx_ref, hsrc_ref, dst_ref, out_ref,
    base_out, near_out, base_in, near_in, dst_in, emb_in, part_out, part_in,
    acc, hid_out, hid_in, prj_out, prj_in, back_out, nback_out, back_in, nback_in, hot_out, hot_in, dec,
    ssem, rsem,
):
    me = lax.axis_index("graph")
    core = lax.axis_index("chan")
    other = 1 - core
    grid_rows = grid_ref.shape[0]
    mesh_rows = embed_ref.shape[0]
    owners = mesh_rows // OWN
    span = cap_near(dst_ref.shape[2])
    bf = jnp.bfloat16

    barrier = pltpu.get_barrier_semaphore()

    @pl.loop(1, n)
    def _(i):
        pl.semaphore_signal(barrier, inc=1, device_id={"graph": lax.rem(me + i, n)}, device_id_type=MESH_ID)

    pl.semaphore_signal(barrier, inc=1, device_id={"chan": other}, device_id_type=MESH_ID)

    def to_graph(src, dst, k, peer):
        return pltpu.make_async_remote_copy(
            src_ref=src, dst_ref=dst, send_sem=ssem.at[k], recv_sem=rsem.at[k],
            device_id={"graph": peer}, device_id_type=MESH_ID)

    def to_core(src, dst, k):
        return pltpu.make_async_remote_copy(
            src_ref=src, dst_ref=dst, send_sem=ssem.at[k], recv_sem=rsem.at[k],
            device_id={"chan": other}, device_id_type=MESH_ID)

    DST, EMB, BASE, NEAR, PART, FWDB, FWDN, HID, PRJ, BACK, NBACK, HOT = range(12)

    @pl.loop(0, (n * HALF) // CHUNK)
    def _(j):
        idx = srcx_ref[core, :, pl.ds(pl.multiple_of(j * CHUNK, CHUNK), CHUNK)]
        rows = pick_turned(grid_ref[...], idx).T.astype(bf)
        base_out[pl.ds(j * (CHUNK // HALF), CHUNK // HALF)] = rows.reshape(CHUNK // HALF, HALF, rows.shape[1])

    near_out[...] = pick_turned(grid_ref[...], srcx_ref[core, :, n * HALF:]).T.astype(bf)
    used = (2 * REACH + 1) * span
    near_in[core, used:, :] = jnp.zeros((NEAR_ROWS - used, near_in.shape[2]), bf)

    pl.semaphore_wait(barrier, n)

    @pl.loop(1, n)
    def _(i):
        peer = lax.rem(me + i, n)
        to_graph(dst_ref.at[peer], dst_in.at[me], DST, peer).start()

    @pl.loop(1, n)
    def _(i):
        peer = lax.rem(me + i, n)
        to_graph(base_out.at[peer], base_in.at[core, me], BASE, peer).start()

    for o in range(-REACH, REACH + 1):
        rows = pl.ds((o + REACH) * span, span)
        if o == 0:
            near_in[core, (o + REACH) * span:(o + REACH + 1) * span] = near_out[(o + REACH) * span:(o + REACH + 1) * span]
        else:
            to_graph(near_out.at[rows], near_in.at[core, rows], NEAR, lax.rem(me + o + n, n)).start()

    @pl.loop(0, owners)
    def _(p):
        @pl.when(p != me)
        def _():
            to_graph(embed_ref.at[pl.ds(p * OWN, OWN)], emb_in.at[me], EMB, p).start()

    base_in[core, pl.ds(me, 1)] = base_out[pl.ds(me, 1)]
    dst_in[pl.ds(me, 1)] = dst_ref[pl.ds(me, 1)]

    to_graph(dst_ref.at[pl.ds(0, n - 1)], dst_in.at[pl.ds(0, n - 1)], DST, me).wait_recv()
    hot = hot_ref[0]
    live = lax.broadcasted_iota(jnp.int32, (1, dst_ref.shape[2]), 1) < hot_ref[1]
    hot_dst = jnp.where(live, dst_in[hot], -1)
    hot_src = hsrc_ref[...]
    rows = pick_turned(grid_ref[...], hot_src).T.astype(bf)
    msgs = silu(jnp.dot(rows, wsrc_ref[...], preferred_element_type=jnp.float32) + bias_ref[...]).astype(bf)
    part = jnp.dot(spread(mesh_rows, hot_dst), msgs, preferred_element_type=jnp.float32).astype(bf)
    part_out[...] = part.reshape(owners, OWN, part.shape[1])

    @pl.loop(0, owners)
    def _(p):
        @pl.when(p != me)
        def _():
            to_graph(part_out.at[p], part_in.at[me], PART, p).start()

    def wait_in(ref, k):
        to_graph(ref, ref, k, me).wait_recv()

    wait_in(base_in.at[core, pl.ds(0, n - 1)], BASE)
    to_core(base_in.at[core], base_in.at[core], FWDB).start()
    wait_in(near_in.at[core, pl.ds(0, 2 * REACH * span)], NEAR)
    to_core(near_in.at[core], near_in.at[core], FWDN).start()

    acc[...] = jnp.zeros_like(acc)

    def add_rows(rows, idx):
        m = silu(jnp.dot(rows, wsrc_ref[...], preferred_element_type=jnp.float32) + bias_ref[...]).astype(bf)
        acc[0:mesh_rows] += jnp.dot(spread(mesh_rows, idx), m, preferred_element_type=jnp.float32)

    def add_half(h):
        @pl.loop(0, (n * HALF) // CHUNK)
        def _(j):
            rows = base_in[h, pl.ds(j * (CHUNK // HALF), CHUNK // HALF)].reshape(CHUNK, base_in.shape[3])
            add_rows(rows, dstx_ref[h, :, pl.ds(pl.multiple_of(j * CHUNK, CHUNK), CHUNK)])
        add_rows(near_in[h], dstx_ref[h, :, n * HALF:])

    add_half(core)
    to_core(base_in.at[other], base_in.at[other], FWDB).wait_recv()
    to_core(near_in.at[other], near_in.at[other], FWDN).wait_recv()
    add_half(other)

    @pl.when(me < owners)
    def _():
        wait_in(part_in.at[pl.ds(0, n - 1)], PART)
        wait_in(emb_in.at[pl.ds(0, n - 1)], EMB)
        part_in[pl.ds(me, 1)] = part_out[pl.ds(me, 1)]
        emb_in[pl.ds(me, 1)] = embed_ref[pl.ds(me * OWN, OWN)].reshape(1, OWN, embed_ref.shape[1])
        acc[mesh_rows:mesh_rows + OWN] = part_in[...].astype(jnp.float32).sum(axis=0)

    half = hid_out.shape[1]
    agg = acc[...].astype(bf)
    hid_out[...] = jnp.dot(agg, wnode_ref[:, pl.ds(pl.multiple_of(other * half, half), half)], preferred_element_type=jnp.float32)
    send = to_core(hid_out, hid_in, HID)
    send.start()
    own = jnp.dot(agg, wnode_ref[:, pl.ds(pl.multiple_of(core * half, half), half)], preferred_element_type=jnp.float32)
    send.wait_recv()
    nodes = silu(own + hid_in[...])
    quarter = prj_out.shape[1]
    lat = (embed_ref[...].astype(jnp.float32) + nodes[0:mesh_rows]).astype(bf)
    hot_lat = (emb_in[hot].astype(jnp.float32) + nodes[mesh_rows:]).astype(bf)
    w_other = wdec_ref[:, pl.ds(pl.multiple_of(other * quarter, quarter), quarter)]
    w_own = wdec_ref[:, pl.ds(pl.multiple_of(core * quarter, quarter), quarter)]
    prj_out[0:mesh_rows] = jnp.dot(lat, w_other, preferred_element_type=jnp.float32)
    prj_out[mesh_rows:] = jnp.dot(hot_lat, w_other, preferred_element_type=jnp.float32)
    send2 = to_core(prj_out, prj_in, PRJ)
    send2.start()
    own_p = jnp.dot(lat, w_own, preferred_element_type=jnp.float32)
    own_h = jnp.dot(hot_lat, w_own, preferred_element_type=jnp.float32)
    send2.wait_recv()
    proj = (own_p + prj_in[0:mesh_rows]).astype(bf)
    hot_out[...] = (own_h + prj_in[mesh_rows:]).astype(bf)

    @pl.when(me < owners)
    def _():
        @pl.loop(1, n)
        def _(i):
            peer = lax.rem(me + i, n)
            to_graph(hot_out, hot_in.at[me], HOT, peer).start()

    for h in range(2):
        @pl.loop(0, (n * HALF) // CHUNK)
        def _(j):
            idx = dstx_ref[h, :, pl.ds(pl.multiple_of(j * CHUNK, CHUNK), CHUNK)]
            rows = pick_turned(proj, idx).T.astype(bf)
            back_out[h, pl.ds(j * (CHUNK // HALF), CHUNK // HALF)] = rows.reshape(CHUNK // HALF, HALF, rows.shape[1])
        nback_out[h] = pick_turned(proj, dstx_ref[h, :, n * HALF:]).T.astype(bf)

    @pl.loop(1, n)
    def _(i):
        peer = lax.rem(me + i, n)
        to_graph(back_out.at[:, peer], back_in.at[:, me], BACK, peer).start()

    for h in range(2):
        for o in range(-REACH, REACH + 1):
            a = (o + REACH) * span
            if o == 0:
                nback_in[h, a:a + span] = nback_out[h, a:a + span]
            else:
                to_graph(nback_out.at[h, pl.ds(a, span)], nback_in.at[h, pl.ds(a, span)], NBACK, lax.rem(me - o + n, n)).start()
        nback_in[h, used:, :] = jnp.zeros((NEAR_ROWS - used, nback_in.shape[2]), bf)
    for h in range(2):
        back_in[h, pl.ds(me, 1)] = back_out[h, pl.ds(me, 1)]

    dec[...] = grid_ref[:, pl.ds(pl.multiple_of(core * quarter, quarter), quarter)].astype(jnp.float32)
    wait_in(nback_in.at[:, pl.ds(0, 2 * REACH * span)], NBACK)
    for h in range(2):
        dec[...] += jnp.dot(spread(grid_rows, srcx_ref[h, :, n * HALF:]), nback_in[h], preferred_element_type=jnp.float32)

    @pl.when(me < owners)
    def _():
        wait_in(hot_in.at[pl.ds(0, owners - 1)], HOT)
        hot_in[pl.ds(me, 1)] = hot_out[...].reshape(1, OWN, quarter)

    @pl.when(me >= owners)
    def _():
        wait_in(hot_in, HOT)

    hot_rows = pick_turned(hot_in[...].reshape(mesh_rows, quarter), hot_dst).astype(bf)
    dec[...] += lax.dot_general(spread(grid_rows, hot_src), hot_rows, (((1,), (1,)), ((), ())), preferred_element_type=jnp.float32)

    wait_in(back_in.at[:, pl.ds(0, n - 1)], BACK)
    for h in range(2):
        @pl.loop(0, (n * HALF) // CHUNK)
        def _(j):
            rows = back_in[h, pl.ds(j * (CHUNK // HALF), CHUNK // HALF)].reshape(CHUNK, quarter)
            idx = srcx_ref[h, :, pl.ds(pl.multiple_of(j * CHUNK, CHUNK), CHUNK)]
            dec[...] += jnp.dot(spread(grid_rows, idx), rows, preferred_element_type=jnp.float32)

    out_ref[...] = dec[...].astype(bf)

    def wait_out(ref, k):
        to_graph(ref, ref, k, me).wait_send()

    wait_out(dst_ref.at[pl.ds(0, n - 1)], DST)
    wait_out(base_out.at[pl.ds(0, n - 1)], BASE)
    wait_out(near_out.at[pl.ds(0, 2 * REACH * span)], NEAR)

    @pl.when(me < owners)
    def _():
        wait_out(embed_ref.at[pl.ds(0, mesh_rows - OWN)], EMB)
        wait_out(part_out.at[pl.ds(0, owners - 1)], PART)
        wait_out(back_out.at[0, pl.ds(0, n - 1)], HOT)

    @pl.when(me >= owners)
    def _():
        wait_out(embed_ref, EMB)
        wait_out(part_out, PART)

    to_core(base_in.at[core], base_in.at[core], FWDB).wait_send()
    to_core(near_in.at[core], near_in.at[core], FWDN).wait_send()
    send.wait_send()
    send2.wait_send()
    wait_out(back_out.at[:, pl.ds(0, n - 1)], BACK)
    wait_out(nback_out.at[:, pl.ds(0, 2 * REACH * span)], NBACK)


def cap_near(capacity):
    return (capacity - KEEP) // 2


def halves(table):
    return table.reshape(table.shape[0], 2, HALF).transpose(1, 0, 2).reshape(2, -1)


def near_halves(table, span):
    rows = table.reshape(2 * REACH + 1, 2, span).transpose(1, 0, 2).reshape(2, -1)
    return jnp.pad(rows, ((0, 0), (0, NEAR_ROWS - rows.shape[1])), constant_values=-1)


def around(table, middle):
    ring = jnp.concatenate([table[-REACH:], table, table[:REACH]], axis=0)
    return lax.dynamic_slice_in_dim(ring, middle, 2 * REACH + 1, 0)


def compact(hot, grid_state, w_src, bias_src, mesh_embed, w_node, w_dec, slot_src, slot_dst, slot_count):
    n = lax.axis_size("graph")
    me = lax.axis_index("graph")
    capacity = slot_src.shape[2]
    span = cap_near(capacity)
    pos = jnp.arange(capacity, dtype=jnp.int32)[None, :]
    ids = jnp.arange(n, dtype=jnp.int32)[:, None]
    sent = lax.dynamic_slice_in_dim(slot_count, me, 1, 0).reshape(n, 1)
    came = lax.dynamic_slice_in_dim(slot_count, me, 1, 1)
    src_live = jnp.where(pos < sent, slot_src[0], -1)
    src = jnp.where(ids != hot, src_live, -1)
    dst = jnp.where((pos < came) & (me != hot), slot_dst[:, 0, :], -1)
    srcx = jnp.concatenate([halves(src[:, :KEEP]), near_halves(around(src, me)[:, KEEP:], span)], axis=1)[:, None, :]
    dstx = jnp.concatenate([halves(dst[:, :KEEP]), near_halves(around(dst, me)[::-1, KEEP:], span)], axis=1)[:, None, :]
    hsrc = lax.dynamic_slice_in_dim(src_live, hot, 1, 0)
    hot_info = jnp.stack([hot, lax.dynamic_slice(slot_count, (me, hot), (1, 1))[0, 0]]).astype(jnp.int32)
    grid_rows, width = grid_state.shape
    mesh_rows, half = mesh_embed.shape
    quarter = width // 2
    owners = mesh_rows // OWN
    bf, f32 = jnp.bfloat16, jnp.float32
    vm = pltpu.VMEM
    return pl.pallas_call(
        functools.partial(step_kernel, n),
        out_shape=jax.ShapeDtypeStruct((grid_rows, quarter), bf),
        in_specs=[pl.BlockSpec(memory_space=pltpu.SMEM)] + [pl.BlockSpec(memory_space=vm)] * 10,
        out_specs=pl.BlockSpec(memory_space=vm),
        scratch_shapes=[
            vm((n, HALF, width), bf), vm((NEAR_ROWS, width), bf),
            vm((2, n, HALF, width), bf), vm((2, NEAR_ROWS, width), bf),
            vm((n, 1, capacity), jnp.int32), vm((n, OWN, half), bf),
            vm((owners, OWN, half), bf), vm((n, OWN, half), bf),
            vm((mesh_rows + OWN, half), f32),
            vm((mesh_rows + OWN, half), f32), vm((mesh_rows + OWN, half), f32),
            vm((mesh_rows + OWN, quarter), f32), vm((mesh_rows + OWN, quarter), f32),
            vm((2, n, HALF, quarter), bf), vm((2, NEAR_ROWS, quarter), bf),
            vm((2, n, HALF, quarter), bf), vm((2, NEAR_ROWS, quarter), bf),
            vm((OWN, quarter), bf), vm((owners, OWN, quarter), bf),
            vm((grid_rows, quarter), f32),
            pltpu.SemaphoreType.DMA((12,)), pltpu.SemaphoreType.DMA((12,)),
        ],
        compiler_params=pltpu.CompilerParams(collective_id=0, has_side_effects=True, vmem_limit_bytes=48 * 1024 * 1024),
    )(hot_info, grid_state, w_src, bias_src[None, :], mesh_embed, w_node, w_dec, srcx, dstx, hsrc, slot_dst)


def on_device(grid_state, w_src, bias_src, mesh_embed, w_node, w_dec, slot_src, slot_dst, slot_count):
    args = (grid_state, w_src, bias_src, mesh_embed, w_node, w_dec, slot_src, slot_dst, slot_count)
    n = slot_count.shape[0]
    apart = jnp.abs(jnp.arange(n)[:, None] - jnp.arange(n)[None, :])
    far = jnp.minimum(apart, n - apart) > REACH
    over = jnp.any(far & (slot_count > KEEP), axis=0)
    hot = jnp.argmax(over).astype(jnp.int32)
    fits = jnp.sum(over.astype(jnp.int32)) <= 1
    return lax.cond(fits, lambda: compact(hot, *args), lambda: dense(*args))


def solution(mesh):
    placed = (
        P(("member", "graph"), None),
        P(None, "chan"),
        P("chan"),
        P("graph", "chan"),
        P("chan", None),
        P("chan", None),
        P("graph", None, None),
        P(None, "graph", None),
        P(),
    )
    return jax.shard_map(
        on_device,
        mesh=mesh,
        in_specs=placed,
        out_specs=P(("member", "graph"), "chan"),
        check_vma=False,
    )
```

```python
import functools
import math

import jax
import jax.numpy as jnp
from jax import lax
from jax.experimental import pallas as pl
from jax.experimental.pallas import tpu as pltpu
from jax.sharding import PartitionSpec as P

MESH_ID = pl.DeviceIdType.MESH
KEEP = 32
HALF = KEEP // 2
REACH = 2
OWN = 16
NEAR_ROWS = 256
CHUNK = 256

def split_up(value, dim, count):
    lengths = value.shape
    parts = value.reshape(*lengths[:dim], count, lengths[dim] // count, *lengths[dim + 1 :])
    return jnp.moveaxis(parts, dim, 0)


def sum_at_owner(value, axis, dim):
    parts = split_up(value, dim, lax.axis_size(axis))
    arrived = lax.all_to_all(parts, axis, split_axis=0, concat_axis=0, tiled=True)
    return arrived.sum(axis=0)


def edge_network(source_rows, w_src, bias_src):
    return jax.nn.silu(
        jnp.dot(source_rows, w_src, preferred_element_type=jnp.float32) + bias_src
    ).astype(jnp.bfloat16)


def segment_rows(values, indices, usable, row_count):
    slot_total = values.shape[0]
    width = values.shape[1]
    block_len = math.gcd(slot_total, 2048)
    block_count = slot_total // block_len
    targets = jnp.where(usable, indices, -1).reshape(block_count, block_len)
    pieces = values.reshape(block_count, block_len, width)
    row_ids = jnp.arange(row_count, dtype=jnp.int32)

    def add_block(summed, scan_item):
        row_target, piece_vals = scan_item
        one_hot = (row_ids[:, None] == row_target[None, :]).astype(jnp.bfloat16)
        return (summed + jnp.dot(one_hot, piece_vals, preferred_element_type=jnp.float32), None)

    result, unused = lax.scan(
        add_block, jnp.zeros((row_count, width), jnp.float32), (targets, pieces)
    )
    return result


def dense(
    grid_state, w_src, bias_src, mesh_embed, w_node, w_dec, slot_src, slot_dst, slot_count
):
    peers = lax.axis_size("graph")
    own_index = lax.axis_index("graph")
    core_index = lax.axis_index("chan")
    capacity = slot_src.shape[2]
    positions = jnp.arange(capacity, dtype=jnp.int32)
    grid_rows = grid_state.shape[0]
    mesh_rows = mesh_embed.shape[0]
    sent_counts = lax.dynamic_slice_in_dim(slot_count, own_index, 1, 0)[0]
    recv_counts = lax.dynamic_slice_in_dim(slot_count, own_index, 1, 1)[:, 0]
    half_slots = capacity // 2
    chosen = lax.dynamic_slice_in_dim(slot_src[0], core_index * half_slots, half_slots, 1)
    picked = jnp.take(grid_state, chosen.reshape(-1), axis=0).reshape(
        peers, half_slots, grid_state.shape[1]
    )
    arrived = lax.all_to_all(picked, "graph", split_axis=0, concat_axis=0, tiled=True)
    partner = lax.ppermute(arrived, "chan", [(0, 1), (1, 0)])
    joined = jnp.where(
        core_index == 0,
        jnp.concatenate([arrived, partner], axis=1),
        jnp.concatenate([partner, arrived], axis=1),
    )
    messages = edge_network(joined.reshape(peers * capacity, grid_state.shape[1]), w_src, bias_src)
    arrive_ok = (positions[None, :] < recv_counts[:, None]).reshape(-1)
    dst_rows = slot_dst[:, 0, :].reshape(-1)
    aggregate = segment_rows(messages, dst_rows, arrive_ok, mesh_rows)
    partial_hidden = jnp.dot(
        aggregate.astype(jnp.bfloat16), w_node, preferred_element_type=jnp.float32
    )
    hidden_pre = sum_at_owner(partial_hidden, "chan", 1)
    latent = (mesh_embed.astype(jnp.float32) + jax.nn.silu(hidden_pre)).astype(jnp.bfloat16)
    partial_proj = jnp.dot(latent, w_dec, preferred_element_type=jnp.float32)
    projected = sum_at_owner(partial_proj, "chan", 1).astype(jnp.bfloat16)
    returned = jnp.take(projected, dst_rows, axis=0).reshape(peers, capacity, projected.shape[1])
    came_back = lax.all_to_all(returned, "graph", split_axis=0, concat_axis=0, tiled=True).reshape(
        peers * capacity, projected.shape[1]
    )
    send_ok = (positions[None, :] < sent_counts[:, None]).reshape(-1)
    decoded = segment_rows(came_back, slot_src[0].reshape(-1), send_ok, grid_rows)
    width_half = decoded.shape[1]
    own_cols = lax.dynamic_slice_in_dim(grid_state, core_index * width_half, width_half, 1)
    return (own_cols.astype(jnp.float32) + decoded).astype(jnp.bfloat16)


def silu(v):
    return v / (1.0 + jnp.exp(-v))


def pick_turned(table, idx):
    rows = table.shape[0]
    hot = jnp.where(
        lax.broadcasted_iota(jnp.int32, (rows, idx.shape[1]), 0) == idx, 1.0, 0.0
    ).astype(jnp.bfloat16)
    return lax.dot_general(table, hot, (((0,), (0,)), ((), ())), preferred_element_type=jnp.float32)


def spread(rows, idx):
    return jnp.where(
        lax.broadcasted_iota(jnp.int32, (rows, idx.shape[1]), 0) == idx, 1.0, 0.0
    ).astype(jnp.bfloat16)


def step_kernel(
    n, hot_ref, grid_ref, wsrc_ref, bias_ref, embed_ref, wnode_ref, wdec_ref,
    src_ref, dst_ref, count_ref, out_ref,
    src_live, dst_live, srcx_ref, dstx_ref,
    base_out, near_out, base_in, near_in, dst_in, emb_in, part_out, part_in,
    acc, hid_out, hid_in, prj_out, prj_in, back_out, nback_out, back_in, nback_in, hot_out, hot_in, dec,
    ssem, rsem,
):
    me = lax.axis_index("graph")
    core = lax.axis_index("chan")
    other = 1 - core
    grid_rows = grid_ref.shape[0]
    mesh_rows = embed_ref.shape[0]
    owners = mesh_rows // OWN
    span = cap_near(dst_ref.shape[2])
    bf = jnp.bfloat16

    barrier = pltpu.get_barrier_semaphore()

    @pl.loop(1, n)
    def _(i):
        pl.semaphore_signal(barrier, inc=1, device_id={"graph": lax.rem(me + i, n)}, device_id_type=MESH_ID)

    pl.semaphore_signal(barrier, inc=1, device_id={"chan": other}, device_id_type=MESH_ID)

    def to_graph(src, dst, k, peer):
        return pltpu.make_async_remote_copy(
            src_ref=src, dst_ref=dst, send_sem=ssem.at[k], recv_sem=rsem.at[k],
            device_id={"graph": peer}, device_id_type=MESH_ID)

    def to_core(src, dst, k):
        return pltpu.make_async_remote_copy(
            src_ref=src, dst_ref=dst, send_sem=ssem.at[k], recv_sem=rsem.at[k],
            device_id={"chan": other}, device_id_type=MESH_ID)

    DST, EMB, BASE, NEAR, PART, FWDB, FWDN, HID, PRJ, BACK, NBACK, HOT = range(12)

    blocks = (n * HALF) // CHUNK
    capacity = dst_ref.shape[2]
    with jax.named_scope("index"):
        hot = hot_ref[0]
        ids = lax.broadcasted_iota(jnp.int32, (n, n), 0)
        cols = lax.broadcasted_iota(jnp.int32, (n, n), 1)
        counts = count_ref[...]
        sent = jnp.where(ids == me, counts, 0).sum(axis=0, keepdims=True)
        sent = jnp.where(ids == cols, sent, 0).sum(axis=1, keepdims=True)
        came = jnp.where(cols == me, counts, 0).sum(axis=1, keepdims=True)
        pos = lax.broadcasted_iota(jnp.int32, (n, capacity), 1)
        src_all = jnp.where(pos < sent, src_ref[0] + 1, 0).astype(jnp.float32)
        src_live[...] = src_all
        came = jnp.where(me == hot, 0, came)
        dst_all = jnp.where(pos < came, dst_ref[:, 0, :] + 1, 0).astype(jnp.float32)
        dst_live[...] = dst_all
        rows_id = lax.broadcasted_iota(jnp.int32, (n, capacity), 0)
        src_all = jnp.where(rows_id == hot, 0.0, src_all)
        near_id = lax.broadcasted_iota(jnp.int32, (8, capacity), 0)
        near_src = jnp.zeros((8, capacity), jnp.float32)
        near_dst = jnp.zeros((8, capacity), jnp.float32)
        for o in range(-REACH, REACH + 1):
            to = lax.rem(me + o + n, n)
            row = jnp.where(to == hot, 0.0, src_live[pl.ds(to, 1)])
            near_src = jnp.where(near_id == o + REACH, row, near_src)
            near_dst = jnp.where(near_id == o + REACH, dst_live[pl.ds(lax.rem(me - o + n, n), 1)], near_dst)
        for h in range(2):
            base = base_layout(capacity, h)
            srcx_ref[h, 0:blocks] = lay_out(src_all, *base)
            dstx_ref[h, 0:blocks] = lay_out(dst_all, *base)
            near = near_layout(capacity, h)
            srcx_ref[h, blocks:] = lay_out(near_src, *near)[:, 0:CHUNK]
            dstx_ref[h, blocks:] = lay_out(near_dst, *near)[:, 0:CHUNK]

    @pl.loop(0, blocks)
    def _(j):
        idx = srcx_ref[core, pl.ds(j, 1)]
        rows = pick_turned(grid_ref[...], idx).T.astype(bf)
        base_out[pl.ds(j * (CHUNK // HALF), CHUNK // HALF)] = rows.reshape(CHUNK // HALF, HALF, rows.shape[1])

    near_out[...] = pick_turned(grid_ref[...], srcx_ref[core, blocks:]).T.astype(bf)
    used = (2 * REACH + 1) * span
    near_in[core, used:, :] = jnp.zeros((NEAR_ROWS - used, near_in.shape[2]), bf)

    pl.semaphore_wait(barrier, n)

    @pl.loop(1, n)
    def _(i):
        peer = lax.rem(me + i, n)
        to_graph(dst_ref.at[peer], dst_in.at[me], DST, peer).start()

    @pl.loop(1, n)
    def _(i):
        peer = lax.rem(me + i, n)
        to_graph(base_out.at[peer], base_in.at[core, me], BASE, peer).start()

    for o in range(-REACH, REACH + 1):
        rows = pl.ds((o + REACH) * span, span)
        if o == 0:
            near_in[core, (o + REACH) * span:(o + REACH + 1) * span] = near_out[(o + REACH) * span:(o + REACH + 1) * span]
        else:
            to_graph(near_out.at[rows], near_in.at[core, rows], NEAR, lax.rem(me + o + n, n)).start()

    @pl.loop(0, owners)
    def _(p):
        @pl.when(p != me)
        def _():
            to_graph(embed_ref.at[pl.ds(p * OWN, OWN)], emb_in.at[me], EMB, p).start()

    base_in[core, pl.ds(me, 1)] = base_out[pl.ds(me, 1)]
    dst_in[pl.ds(me, 1)] = dst_ref[pl.ds(me, 1)]

    to_graph(dst_ref.at[pl.ds(0, n - 1)], dst_in.at[pl.ds(0, n - 1)], DST, me).wait_recv()
    hot_src = src_live[pl.ds(hot, 1)].astype(jnp.int32) - 1
    hot_dst = jnp.where(hot_src >= 0, dst_in[hot], -1)
    rows = pick_turned(grid_ref[...], hot_src).T.astype(bf)
    msgs = silu(jnp.dot(rows, wsrc_ref[...], preferred_element_type=jnp.float32) + bias_ref[...]).astype(bf)
    part = jnp.dot(spread(mesh_rows, hot_dst), msgs, preferred_element_type=jnp.float32).astype(bf)
    part_out[...] = part.reshape(owners, OWN, part.shape[1])

    @pl.loop(0, owners)
    def _(p):
        @pl.when(p != me)
        def _():
            to_graph(part_out.at[p], part_in.at[me], PART, p).start()

    def wait_in(ref, k):
        to_graph(ref, ref, k, me).wait_recv()

    wait_in(base_in.at[core, pl.ds(0, n - 1)], BASE)
    to_core(base_in.at[core], base_in.at[core], FWDB).start()
    wait_in(near_in.at[core, pl.ds(0, 2 * REACH * span)], NEAR)
    to_core(near_in.at[core], near_in.at[core], FWDN).start()

    acc[...] = jnp.zeros_like(acc)

    def add_rows(rows, idx):
        m = silu(jnp.dot(rows, wsrc_ref[...], preferred_element_type=jnp.float32) + bias_ref[...]).astype(bf)
        acc[0:mesh_rows] += jnp.dot(spread(mesh_rows, idx), m, preferred_element_type=jnp.float32)

    def add_half(h):
        @pl.loop(0, blocks)
        def _(j):
            rows = base_in[h, pl.ds(j * (CHUNK // HALF), CHUNK // HALF)].reshape(CHUNK, base_in.shape[3])
            add_rows(rows, dstx_ref[h, pl.ds(j, 1)])
        add_rows(near_in[h], dstx_ref[h, blocks:])

    add_half(core)
    to_core(base_in.at[other], base_in.at[other], FWDB).wait_recv()
    to_core(near_in.at[other], near_in.at[other], FWDN).wait_recv()
    add_half(other)

    @pl.when(me < owners)
    def _():
        wait_in(part_in.at[pl.ds(0, n - 1)], PART)
        wait_in(emb_in.at[pl.ds(0, n - 1)], EMB)
        part_in[pl.ds(me, 1)] = part_out[pl.ds(me, 1)]
        emb_in[pl.ds(me, 1)] = embed_ref[pl.ds(me * OWN, OWN)].reshape(1, OWN, embed_ref.shape[1])
        acc[mesh_rows:mesh_rows + OWN] = part_in[...].astype(jnp.float32).sum(axis=0)

    half = hid_out.shape[1]
    agg = acc[...].astype(bf)
    hid_out[...] = jnp.dot(agg, wnode_ref[:, pl.ds(pl.multiple_of(other * half, half), half)], preferred_element_type=jnp.float32)
    send = to_core(hid_out, hid_in, HID)
    send.start()
    own = jnp.dot(agg, wnode_ref[:, pl.ds(pl.multiple_of(core * half, half), half)], preferred_element_type=jnp.float32)
    send.wait_recv()
    nodes = silu(own + hid_in[...])
    quarter = prj_out.shape[1]
    lat = (embed_ref[...].astype(jnp.float32) + nodes[0:mesh_rows]).astype(bf)
    hot_lat = (emb_in[hot].astype(jnp.float32) + nodes[mesh_rows:]).astype(bf)
    w_other = wdec_ref[:, pl.ds(pl.multiple_of(other * quarter, quarter), quarter)]
    w_own = wdec_ref[:, pl.ds(pl.multiple_of(core * quarter, quarter), quarter)]
    prj_out[0:mesh_rows] = jnp.dot(lat, w_other, preferred_element_type=jnp.float32)
    prj_out[mesh_rows:] = jnp.dot(hot_lat, w_other, preferred_element_type=jnp.float32)
    send2 = to_core(prj_out, prj_in, PRJ)
    send2.start()
    own_p = jnp.dot(lat, w_own, preferred_element_type=jnp.float32)
    own_h = jnp.dot(hot_lat, w_own, preferred_element_type=jnp.float32)
    send2.wait_recv()
    proj = (own_p + prj_in[0:mesh_rows]).astype(bf)
    hot_out[...] = (own_h + prj_in[mesh_rows:]).astype(bf)

    @pl.when(me < owners)
    def _():
        @pl.loop(1, n)
        def _(i):
            peer = lax.rem(me + i, n)
            to_graph(hot_out, hot_in.at[me], HOT, peer).start()

    for h in range(2):
        @pl.loop(0, blocks)
        def _(j):
            idx = dstx_ref[h, pl.ds(j, 1)]
            rows = pick_turned(proj, idx).T.astype(bf)
            back_out[h, pl.ds(j * (CHUNK // HALF), CHUNK // HALF)] = rows.reshape(CHUNK // HALF, HALF, rows.shape[1])
        nback_out[h] = pick_turned(proj, dstx_ref[h, blocks:]).T.astype(bf)

    @pl.loop(1, n)
    def _(i):
        peer = lax.rem(me + i, n)
        to_graph(back_out.at[:, peer], back_in.at[:, me], BACK, peer).start()

    for h in range(2):
        for o in range(-REACH, REACH + 1):
            a = (o + REACH) * span
            if o == 0:
                nback_in[h, a:a + span] = nback_out[h, a:a + span]
            else:
                to_graph(nback_out.at[h, pl.ds(a, span)], nback_in.at[h, pl.ds(a, span)], NBACK, lax.rem(me - o + n, n)).start()
        nback_in[h, used:, :] = jnp.zeros((NEAR_ROWS - used, nback_in.shape[2]), bf)
    for h in range(2):
        back_in[h, pl.ds(me, 1)] = back_out[h, pl.ds(me, 1)]

    dec[...] = grid_ref[:, pl.ds(pl.multiple_of(core * quarter, quarter), quarter)].astype(jnp.float32)
    wait_in(nback_in.at[:, pl.ds(0, 2 * REACH * span)], NBACK)
    for h in range(2):
        dec[...] += jnp.dot(spread(grid_rows, srcx_ref[h, blocks:]), nback_in[h], preferred_element_type=jnp.float32)

    @pl.when(me < owners)
    def _():
        wait_in(hot_in.at[pl.ds(0, owners - 1)], HOT)
        hot_in[pl.ds(me, 1)] = hot_out[...].reshape(1, OWN, quarter)

    @pl.when(me >= owners)
    def _():
        wait_in(hot_in, HOT)

    hot_rows = pick_turned(hot_in[...].reshape(mesh_rows, quarter), hot_dst).astype(bf)
    dec[...] += lax.dot_general(spread(grid_rows, hot_src), hot_rows, (((1,), (1,)), ((), ())), preferred_element_type=jnp.float32)

    wait_in(back_in.at[:, pl.ds(0, n - 1)], BACK)
    for h in range(2):
        @pl.loop(0, blocks)
        def _(j):
            rows = back_in[h, pl.ds(j * (CHUNK // HALF), CHUNK // HALF)].reshape(CHUNK, quarter)
            idx = srcx_ref[h, pl.ds(j, 1)]
            dec[...] += jnp.dot(spread(grid_rows, idx), rows, preferred_element_type=jnp.float32)

    out_ref[...] = dec[...].astype(bf)

    def wait_out(ref, k):
        to_graph(ref, ref, k, me).wait_send()

    wait_out(dst_ref.at[pl.ds(0, n - 1)], DST)
    wait_out(base_out.at[pl.ds(0, n - 1)], BASE)
    wait_out(near_out.at[pl.ds(0, 2 * REACH * span)], NEAR)

    @pl.when(me < owners)
    def _():
        wait_out(embed_ref.at[pl.ds(0, mesh_rows - OWN)], EMB)
        wait_out(part_out.at[pl.ds(0, owners - 1)], PART)
        wait_out(back_out.at[0, pl.ds(0, n - 1)], HOT)

    @pl.when(me >= owners)
    def _():
        wait_out(embed_ref, EMB)
        wait_out(part_out, PART)

    to_core(base_in.at[core], base_in.at[core], FWDB).wait_send()
    to_core(near_in.at[core], near_in.at[core], FWDN).wait_send()
    send.wait_send()
    send2.wait_send()
    wait_out(back_out.at[:, pl.ds(0, n - 1)], BACK)
    wait_out(nback_out.at[:, pl.ds(0, 2 * REACH * span)], NBACK)


def cap_near(capacity):
    return (capacity - KEEP) // 2


def lay_out(table, take, mark):
    high = jnp.floor(table * (1.0 / 32.0))
    low = table - 32.0 * high
    dot = functools.partial(jnp.dot, preferred_element_type=jnp.float32)
    moved = 32.0 * dot(high.astype(jnp.bfloat16), take) + dot(low.astype(jnp.bfloat16), take)
    group = mark.shape[0]
    moved = moved.reshape(table.shape[0] // group, group, take.shape[1])
    return (moved * mark[None]).sum(axis=1).astype(jnp.int32) - 1


def base_layout(capacity, h):
    shape = (capacity, CHUNK)
    lane = lax.broadcasted_iota(jnp.int32, shape, 1)
    slot = lax.broadcasted_iota(jnp.int32, shape, 0)
    take = jnp.where(slot == h * HALF + (lane & (HALF - 1)), 1.0, 0.0).astype(jnp.bfloat16)
    group = CHUNK // HALF
    lane = lax.broadcasted_iota(jnp.int32, (group, CHUNK), 1)
    row = lax.broadcasted_iota(jnp.int32, (group, CHUNK), 0)
    return take, jnp.where(row * HALF <= lane, 1.0, 0.0) * jnp.where(lane < row * HALF + HALF, 1.0, 0.0)


def near_layout(capacity, h):
    span = cap_near(capacity)
    count = 2 * REACH + 1
    shape = (capacity, NEAR_ROWS)
    lane = lax.broadcasted_iota(jnp.int32, shape, 1)
    slot = lax.broadcasted_iota(jnp.int32, shape, 0)
    within = lane
    for i in range(1, count + 1):
        within = within - jnp.where(lane >= i * span, span, 0)
    take = jnp.where(slot == KEEP + h * span + within, 1.0, 0.0).astype(jnp.bfloat16)
    lane = lax.broadcasted_iota(jnp.int32, (8, NEAR_ROWS), 1)
    row = lax.broadcasted_iota(jnp.int32, (8, NEAR_ROWS), 0)
    inside = jnp.where(row * span <= lane, 1.0, 0.0) * jnp.where(lane < row * span + span, 1.0, 0.0)
    return take, inside * jnp.where(row < count, 1.0, 0.0)


def compact(hot, grid_state, w_src, bias_src, mesh_embed, w_node, w_dec, slot_src, slot_dst, slot_count):
    n = lax.axis_size("graph")
    capacity = slot_src.shape[2]
    grid_rows, width = grid_state.shape
    mesh_rows, half = mesh_embed.shape
    quarter = width // 2
    owners = mesh_rows // OWN
    bf, f32 = jnp.bfloat16, jnp.float32
    vm = pltpu.VMEM
    return pl.pallas_call(
        functools.partial(step_kernel, n),
        out_shape=jax.ShapeDtypeStruct((grid_rows, quarter), bf),
        in_specs=[pl.BlockSpec(memory_space=pltpu.SMEM)] + [pl.BlockSpec(memory_space=vm)] * 9,
        out_specs=pl.BlockSpec(memory_space=vm),
        scratch_shapes=[
            vm((n, capacity), f32), vm((n, capacity), f32),
            vm((2, n * HALF // CHUNK + 1, CHUNK), jnp.int32), vm((2, n * HALF // CHUNK + 1, CHUNK), jnp.int32),
            vm((n, HALF, width), bf), vm((NEAR_ROWS, width), bf),
            vm((2, n, HALF, width), bf), vm((2, NEAR_ROWS, width), bf),
            vm((n, 1, capacity), jnp.int32), vm((n, OWN, half), bf),
            vm((owners, OWN, half), bf), vm((n, OWN, half), bf),
            vm((mesh_rows + OWN, half), f32),
            vm((mesh_rows + OWN, half), f32), vm((mesh_rows + OWN, half), f32),
            vm((mesh_rows + OWN, quarter), f32), vm((mesh_rows + OWN, quarter), f32),
            vm((2, n, HALF, quarter), bf), vm((2, NEAR_ROWS, quarter), bf),
            vm((2, n, HALF, quarter), bf), vm((2, NEAR_ROWS, quarter), bf),
            vm((OWN, quarter), bf), vm((owners, OWN, quarter), bf),
            vm((grid_rows, quarter), f32),
            pltpu.SemaphoreType.DMA((12,)), pltpu.SemaphoreType.DMA((12,)),
        ],
        compiler_params=pltpu.CompilerParams(collective_id=0, has_side_effects=True, vmem_limit_bytes=48 * 1024 * 1024),
    )(hot, grid_state, w_src, bias_src[None, :], mesh_embed, w_node, w_dec, slot_src, slot_dst, slot_count)


def on_device(grid_state, w_src, bias_src, mesh_embed, w_node, w_dec, slot_src, slot_dst, slot_count):
    args = (grid_state, w_src, bias_src, mesh_embed, w_node, w_dec, slot_src, slot_dst, slot_count)
    n = slot_count.shape[0]
    apart = jnp.abs(jnp.arange(n)[:, None] - jnp.arange(n)[None, :])
    far = jnp.minimum(apart, n - apart) > REACH
    over = far & (slot_count > KEEP)
    column = jnp.broadcast_to(jnp.arange(n, dtype=jnp.int32)[None, :], (n, n))
    last = jnp.max(jnp.where(over, column, 0))
    first = jnp.min(jnp.where(over, column, n))
    fits = last <= first
    hot = last.reshape(1)
    return lax.cond(fits, lambda: compact(hot, *args), lambda: dense(*args))


def solution(mesh):
    placed = (
        P(("member", "graph"), None),
        P(None, "chan"),
        P("chan"),
        P("graph", "chan"),
        P("chan", None),
        P("chan", None),
        P("graph", None, None),
        P(None, "graph", None),
        P(),
    )
    return jax.shard_map(
        on_device,
        mesh=mesh,
        in_specs=placed,
        out_specs=P(("member", "graph"), "chan"),
        check_vma=False,
    )
```

```python
import functools
import math

import jax
import jax.numpy as jnp
from jax import lax
from jax.experimental import pallas as pl
from jax.experimental.pallas import tpu as pltpu
from jax.sharding import PartitionSpec as P

MESH_ID = pl.DeviceIdType.MESH
KEEP = 32
HALF = KEEP // 2
GROUP = 7
REACH = 2
OWN = 16
NEAR_ROWS = 256
CHUNK = 256

def split_up(value, dim, count):
    lengths = value.shape
    parts = value.reshape(*lengths[:dim], count, lengths[dim] // count, *lengths[dim + 1 :])
    return jnp.moveaxis(parts, dim, 0)


def sum_at_owner(value, axis, dim):
    parts = split_up(value, dim, lax.axis_size(axis))
    arrived = lax.all_to_all(parts, axis, split_axis=0, concat_axis=0, tiled=True)
    return arrived.sum(axis=0)


def edge_network(source_rows, w_src, bias_src):
    return jax.nn.silu(
        jnp.dot(source_rows, w_src, preferred_element_type=jnp.float32) + bias_src
    ).astype(jnp.bfloat16)


def segment_rows(values, indices, usable, row_count):
    slot_total = values.shape[0]
    width = values.shape[1]
    block_len = math.gcd(slot_total, 2048)
    block_count = slot_total // block_len
    targets = jnp.where(usable, indices, -1).reshape(block_count, block_len)
    pieces = values.reshape(block_count, block_len, width)
    row_ids = jnp.arange(row_count, dtype=jnp.int32)

    def add_block(summed, scan_item):
        row_target, piece_vals = scan_item
        one_hot = (row_ids[:, None] == row_target[None, :]).astype(jnp.bfloat16)
        return (summed + jnp.dot(one_hot, piece_vals, preferred_element_type=jnp.float32), None)

    result, unused = lax.scan(
        add_block, jnp.zeros((row_count, width), jnp.float32), (targets, pieces)
    )
    return result


def dense(
    grid_state, w_src, bias_src, mesh_embed, w_node, w_dec, slot_src, slot_dst, slot_count
):
    peers = lax.axis_size("graph")
    own_index = lax.axis_index("graph")
    core_index = lax.axis_index("chan")
    capacity = slot_src.shape[2]
    positions = jnp.arange(capacity, dtype=jnp.int32)
    grid_rows = grid_state.shape[0]
    mesh_rows = mesh_embed.shape[0]
    sent_counts = lax.dynamic_slice_in_dim(slot_count, own_index, 1, 0)[0]
    recv_counts = lax.dynamic_slice_in_dim(slot_count, own_index, 1, 1)[:, 0]
    half_slots = capacity // 2
    chosen = lax.dynamic_slice_in_dim(slot_src[0], core_index * half_slots, half_slots, 1)
    picked = jnp.take(grid_state, chosen.reshape(-1), axis=0).reshape(
        peers, half_slots, grid_state.shape[1]
    )
    arrived = lax.all_to_all(picked, "graph", split_axis=0, concat_axis=0, tiled=True)
    partner = lax.ppermute(arrived, "chan", [(0, 1), (1, 0)])
    joined = jnp.where(
        core_index == 0,
        jnp.concatenate([arrived, partner], axis=1),
        jnp.concatenate([partner, arrived], axis=1),
    )
    messages = edge_network(joined.reshape(peers * capacity, grid_state.shape[1]), w_src, bias_src)
    arrive_ok = (positions[None, :] < recv_counts[:, None]).reshape(-1)
    dst_rows = slot_dst[:, 0, :].reshape(-1)
    aggregate = segment_rows(messages, dst_rows, arrive_ok, mesh_rows)
    partial_hidden = jnp.dot(
        aggregate.astype(jnp.bfloat16), w_node, preferred_element_type=jnp.float32
    )
    hidden_pre = sum_at_owner(partial_hidden, "chan", 1)
    latent = (mesh_embed.astype(jnp.float32) + jax.nn.silu(hidden_pre)).astype(jnp.bfloat16)
    partial_proj = jnp.dot(latent, w_dec, preferred_element_type=jnp.float32)
    projected = sum_at_owner(partial_proj, "chan", 1).astype(jnp.bfloat16)
    returned = jnp.take(projected, dst_rows, axis=0).reshape(peers, capacity, projected.shape[1])
    came_back = lax.all_to_all(returned, "graph", split_axis=0, concat_axis=0, tiled=True).reshape(
        peers * capacity, projected.shape[1]
    )
    send_ok = (positions[None, :] < sent_counts[:, None]).reshape(-1)
    decoded = segment_rows(came_back, slot_src[0].reshape(-1), send_ok, grid_rows)
    width_half = decoded.shape[1]
    own_cols = lax.dynamic_slice_in_dim(grid_state, core_index * width_half, width_half, 1)
    return (own_cols.astype(jnp.float32) + decoded).astype(jnp.bfloat16)


def torus(n):
    wide = 1 << (n.bit_length() // 2)
    return n // wide, wide


def visit_order(n):
    tall, wide = torus(n)
    offsets = [(r, c) for r in range(tall) for c in range(wide)][1:]
    offsets.sort(key=lambda o: min(o[0], tall - o[0]) + min(o[1], wide - o[1]))
    return [offsets[i // 2] if i % 2 == 0 else offsets[-1 - i // 2] for i in range(n - 1)]


def silu(v):
    return v / (1.0 + jnp.exp(-v))


def pick_turned(table, idx):
    rows = table.shape[0]
    hot = jnp.where(
        lax.broadcasted_iota(jnp.int32, (rows, idx.shape[1]), 0) == idx, 1.0, 0.0
    ).astype(jnp.bfloat16)
    return lax.dot_general(table, hot, (((0,), (0,)), ((), ())), preferred_element_type=jnp.float32)


def spread(rows, idx):
    return jnp.where(
        lax.broadcasted_iota(jnp.int32, (rows, idx.shape[1]), 0) == idx, 1.0, 0.0
    ).astype(jnp.bfloat16)


def step_kernel(
    n, hot_ref, grid_ref, wsrc_ref, bias_ref, embed_ref, wnode_ref, wdec_ref,
    src_ref, dst_ref, count_ref, out_ref,
    src_live, dst_live, srcx_ref, dstx_ref,
    base_out, near_out, base_in, near_in, dst_in, emb_in, emb_out, emb_half, part_out, part_in,
    acc, hid_out, hid_in, prj_out, prj_in, prj_bf, back_out, nback_out, back_in, nback_in, hot_out, hot_in, dec,
    ssem, rsem,
):
    me = lax.axis_index("graph")
    core = lax.axis_index("chan")
    other = 1 - core
    grid_rows = grid_ref.shape[0]
    mesh_rows = embed_ref.shape[0]
    owners = mesh_rows // OWN
    span = cap_near(dst_ref.shape[2])
    bf = jnp.bfloat16

    barrier = pltpu.get_barrier_semaphore()

    @pl.loop(1, n)
    def _(i):
        pl.semaphore_signal(barrier, inc=1, device_id={"graph": lax.rem(me + i, n)}, device_id_type=MESH_ID)

    pl.semaphore_signal(barrier, inc=1, device_id={"chan": other}, device_id_type=MESH_ID)

    def to_graph(src, dst, k, peer):
        return pltpu.make_async_remote_copy(
            src_ref=src, dst_ref=dst, send_sem=ssem.at[k], recv_sem=rsem.at[k],
            device_id={"graph": peer}, device_id_type=MESH_ID)

    def to_core(src, dst, k):
        return pltpu.make_async_remote_copy(
            src_ref=src, dst_ref=dst, send_sem=ssem.at[k], recv_sem=rsem.at[k],
            device_id={"chan": other}, device_id_type=MESH_ID)

    tall, wide = torus(n)
    codes = [r * wide + c for r, c in visit_order(n)]
    groups = [codes[i:i + GROUP] for i in range(0, n - 1, GROUP)]
    my_row, my_column = me // wide, lax.rem(me, wide)
    turn = 1 - 2 * core

    def each_peer(visit):
        parts = (range(0, 4), range(4, GROUP))

        @pl.loop(0, len(groups))
        def _(g):
            for part in parts:
                packed = jnp.int32(0)
                for i, group in enumerate(groups):
                    packed = jnp.where(g == i, sum(group[k] * n ** j for j, k in enumerate(part)), packed)
                for j in range(len(part)):
                    code = lax.rem(lax.div(packed, jnp.int32(n ** j)), jnp.int32(n))
                    to_row = lax.rem(my_row + turn * lax.div(code, jnp.int32(wide)) + tall, tall)
                    to_column = lax.rem(my_column + turn * lax.rem(code, jnp.int32(wide)) + wide, wide)
                    visit(to_row * wide + to_column)

    DST, EMB, BASE, NEAR, PART, FWDB, FWDN, HID, PRJ, BACK, NBACK, HOT, PRJ0, BACK1 = range(14)

    blocks = (n * HALF) // CHUNK
    capacity = dst_ref.shape[2]
    with jax.named_scope("index"):
        hot = hot_ref[0]
        ids = lax.broadcasted_iota(jnp.int32, (n, n), 0)
        cols = lax.broadcasted_iota(jnp.int32, (n, n), 1)
        counts = count_ref[...]
        sent = jnp.where(ids == me, counts, 0).sum(axis=0, keepdims=True)
        sent = jnp.where(ids == cols, sent, 0).sum(axis=1, keepdims=True)
        came = jnp.where(cols == me, counts, 0).sum(axis=1, keepdims=True)
        pos = lax.broadcasted_iota(jnp.int32, (n, capacity), 1)
        src_all = jnp.where(pos < sent, src_ref[0] + 1, 0).astype(jnp.float32)
        src_live[...] = src_all
        came = jnp.where(me == hot, 0, came)
        dst_all = jnp.where(pos < came, dst_ref[:, 0, :] + 1, 0).astype(jnp.float32)
        dst_live[...] = dst_all
        rows_id = lax.broadcasted_iota(jnp.int32, (n, capacity), 0)
        src_all = jnp.where(rows_id == hot, 0.0, src_all)
        near_id = lax.broadcasted_iota(jnp.int32, (8, capacity), 0)
        near_src = jnp.zeros((8, capacity), jnp.float32)
        near_dst = jnp.zeros((8, capacity), jnp.float32)
        for o in range(-REACH, REACH + 1):
            to = lax.rem(me + o + n, n)
            row = jnp.where(to == hot, 0.0, src_live[pl.ds(to, 1)])
            near_src = jnp.where(near_id == o + REACH, row, near_src)
            near_dst = jnp.where(near_id == o + REACH, dst_live[pl.ds(lax.rem(me - o + n, n), 1)], near_dst)
        for h in range(2):
            base = base_layout(capacity, h)
            srcx_ref[h, 0:blocks] = lay_out(src_all, *base)
            dstx_ref[h, 0:blocks] = lay_out(dst_all, *base)
            near = near_layout(capacity, h)
            srcx_ref[h, blocks:] = lay_out(near_src, *near)[:, 0:CHUNK]
            dstx_ref[h, blocks:] = lay_out(near_dst, *near)[:, 0:CHUNK]

    @pl.loop(0, blocks)
    def _(j):
        idx = srcx_ref[core, pl.ds(j, 1)]
        rows = pick_turned(grid_ref[...], idx).T.astype(bf)
        base_out[pl.ds(j * (CHUNK // HALF), CHUNK // HALF)] = rows.reshape(CHUNK // HALF, HALF, rows.shape[1])

    near_out[...] = pick_turned(grid_ref[...], srcx_ref[core, blocks:]).T.astype(bf)
    used = (2 * REACH + 1) * span
    near_in[core, used:, :] = jnp.zeros((NEAR_ROWS - used, near_in.shape[2]), bf)

    pl.semaphore_wait(barrier, n)

    each_peer(lambda peer: to_graph(dst_ref.at[peer], dst_in.at[me], DST, peer).start())
    each_peer(lambda peer: to_graph(base_out.at[peer], base_in.at[core, me], BASE, peer).start())

    for o in range(-REACH, REACH + 1):
        rows = pl.ds((o + REACH) * span, span)
        if o == 0:
            near_in[core, (o + REACH) * span:(o + REACH + 1) * span] = near_out[(o + REACH) * span:(o + REACH + 1) * span]
        else:
            to_graph(near_out.at[rows], near_in.at[core, rows], NEAR, lax.rem(me + o + n, n)).start()

    base_in[core, pl.ds(me, 1)] = base_out[pl.ds(me, 1)]
    dst_in[pl.ds(me, 1)] = dst_ref[pl.ds(me, 1)]

    to_graph(dst_ref.at[pl.ds(0, n - 1)], dst_in.at[pl.ds(0, n - 1)], DST, me).wait_recv()
    hot_src = src_live[pl.ds(hot, 1)].astype(jnp.int32) - 1
    hot_dst = jnp.where(hot_src >= 0, dst_in[hot], -1)
    rows = pick_turned(grid_ref[...], hot_src).T.astype(bf)
    msgs = silu(jnp.dot(rows, wsrc_ref[...], preferred_element_type=jnp.float32) + bias_ref[...]).astype(bf)
    part = jnp.dot(spread(mesh_rows, hot_dst), msgs, preferred_element_type=jnp.float32).astype(bf)
    part_out[...] = part.reshape(owners, OWN, part.shape[1])

    def send_part(peer):
        @pl.when(peer < owners)
        def _():
            to_graph(part_out.at[peer], part_in.at[me], PART, peer).start()

    each_peer(send_part)

    quarter = prj_out.shape[1]
    w_other = wdec_ref[:, pl.ds(pl.multiple_of(other * quarter, quarter), quarter)]
    w_own = wdec_ref[:, pl.ds(pl.multiple_of(core * quarter, quarter), quarter)]
    prj_out[0:mesh_rows] = jnp.dot(embed_ref[...], w_other, preferred_element_type=jnp.float32)
    send0 = to_core(prj_out.at[pl.ds(0, mesh_rows)], emb_half, PRJ0)
    send0.start()
    emb_own = jnp.dot(embed_ref[...], w_own, preferred_element_type=jnp.float32)
    send0.wait_recv()
    emb_out[...] = (emb_own + emb_half[...]).astype(bf).reshape(owners, OWN, quarter)

    def send_emb(peer):
        @pl.when(peer < owners)
        def _():
            to_graph(emb_out.at[peer], emb_in.at[me], EMB, peer).start()

    each_peer(send_emb)

    def wait_in(ref, k):
        to_graph(ref, ref, k, me).wait_recv()

    wait_in(base_in.at[core, pl.ds(0, n - 1)], BASE)
    to_core(base_in.at[core], base_in.at[core], FWDB).start()
    wait_in(near_in.at[core, pl.ds(0, 2 * REACH * span)], NEAR)
    to_core(near_in.at[core], near_in.at[core], FWDN).start()

    acc[...] = jnp.zeros_like(acc)

    def add_rows(rows, idx):
        m = silu(jnp.dot(rows, wsrc_ref[...], preferred_element_type=jnp.float32) + bias_ref[...]).astype(bf)
        acc[0:mesh_rows] += jnp.dot(spread(mesh_rows, idx), m, preferred_element_type=jnp.float32)

    def add_half(h):
        @pl.loop(0, blocks)
        def _(j):
            rows = base_in[h, pl.ds(j * (CHUNK // HALF), CHUNK // HALF)].reshape(CHUNK, base_in.shape[3])
            add_rows(rows, dstx_ref[h, pl.ds(j, 1)])
        add_rows(near_in[h], dstx_ref[h, blocks:])

    add_half(core)
    to_core(base_in.at[other], base_in.at[other], FWDB).wait_recv()
    to_core(near_in.at[other], near_in.at[other], FWDN).wait_recv()
    add_half(other)

    @pl.when(me < owners)
    def _():
        wait_in(part_in.at[pl.ds(0, n - 1)], PART)
        wait_in(emb_in.at[pl.ds(0, n - 1)], EMB)
        part_in[pl.ds(me, 1)] = part_out[pl.ds(me, 1)]
        emb_in[pl.ds(me, 1)] = emb_out[pl.ds(me, 1)]
        acc[mesh_rows:mesh_rows + OWN] = part_in[...].astype(jnp.float32).sum(axis=0)

    half = hid_out.shape[1]
    agg = acc[...].astype(bf)
    hid_out[...] = jnp.dot(agg, wnode_ref[:, pl.ds(pl.multiple_of(other * half, half), half)], preferred_element_type=jnp.float32)
    send = to_core(hid_out, hid_in, HID)
    send.start()
    own = jnp.dot(agg, wnode_ref[:, pl.ds(pl.multiple_of(core * half, half), half)], preferred_element_type=jnp.float32)
    send.wait_recv()
    nodes = silu(own + hid_in[...])
    lat = (embed_ref[...].astype(jnp.float32) + nodes[0:mesh_rows]).astype(bf)
    hot_lat = nodes[mesh_rows:].astype(bf)
    send0.wait_send()
    prj_out[0:mesh_rows] = jnp.dot(lat, w_other, preferred_element_type=jnp.float32)
    prj_out[mesh_rows:] = jnp.dot(hot_lat, w_other, preferred_element_type=jnp.float32)
    send2 = to_core(prj_out, prj_in, PRJ)
    send2.start()
    own_p = jnp.dot(lat, w_own, preferred_element_type=jnp.float32)
    own_h = jnp.dot(hot_lat, w_own, preferred_element_type=jnp.float32)
    send2.wait_recv()
    proj = (own_p + prj_in[0:mesh_rows]).astype(bf)
    hot_out[...] = (own_h + prj_in[mesh_rows:] + emb_in[hot].astype(jnp.float32)).astype(bf)

    @pl.when(me < owners)
    def _():
        each_peer(lambda peer: to_graph(hot_out, hot_in.at[me], HOT, peer).start())

    prj_bf[...] = proj
    for h in range(2):
        nback_out[h] = pick_turned(prj_bf[...], dstx_ref[h, blocks:]).T.astype(bf)
        nback_in[h, used:, :] = jnp.zeros((NEAR_ROWS - used, nback_in.shape[2]), bf)
        for o in range(-REACH, REACH + 1):
            a = (o + REACH) * span
            if o == 0:
                nback_in[h, a:a + span] = nback_out[h, a:a + span]
            else:
                to_graph(nback_out.at[h, pl.ds(a, span)], nback_in.at[h, pl.ds(a, span)], NBACK, lax.rem(me - o + n, n)).start()

    for h in range(2):
        @pl.loop(0, blocks)
        def _(j):
            idx = dstx_ref[h, pl.ds(j, 1)]
            rows = pick_turned(prj_bf[...], idx).T.astype(bf)
            back_out[h, pl.ds(j * (CHUNK // HALF), CHUNK // HALF)] = rows.reshape(CHUNK // HALF, HALF, rows.shape[1])

        back_in[h, pl.ds(me, 1)] = back_out[h, pl.ds(me, 1)]
        each_peer(lambda peer, h=h: to_graph(back_out.at[h, peer], back_in.at[h, me], BACK1 if h else BACK, peer).start())

    dec[...] = grid_ref[:, pl.ds(pl.multiple_of(core * quarter, quarter), quarter)].astype(jnp.float32)
    wait_in(nback_in.at[:, pl.ds(0, 2 * REACH * span)], NBACK)
    for h in range(2):
        dec[...] += jnp.dot(spread(grid_rows, srcx_ref[h, blocks:]), nback_in[h], preferred_element_type=jnp.float32)

    @pl.when(me < owners)
    def _():
        wait_in(hot_in.at[pl.ds(0, owners - 1)], HOT)
        hot_in[pl.ds(me, 1)] = hot_out[...].reshape(1, OWN, quarter)

    @pl.when(me >= owners)
    def _():
        wait_in(hot_in, HOT)

    hot_rows = pick_turned(hot_in[...].reshape(mesh_rows, quarter), hot_dst).astype(bf)
    dec[...] += lax.dot_general(spread(grid_rows, hot_src), hot_rows, (((1,), (1,)), ((), ())), preferred_element_type=jnp.float32)

    for h in range(2):
        wait_in(back_in.at[h, pl.ds(0, n - 1)], BACK1 if h else BACK)

        @pl.loop(0, blocks)
        def _(j):
            rows = back_in[h, pl.ds(j * (CHUNK // HALF), CHUNK // HALF)].reshape(CHUNK, quarter)
            idx = srcx_ref[h, pl.ds(j, 1)]
            dec[...] += jnp.dot(spread(grid_rows, idx), rows, preferred_element_type=jnp.float32)

    out_ref[...] = dec[...].astype(bf)

    def wait_out(ref, k):
        to_graph(ref, ref, k, me).wait_send()

    wait_out(dst_ref.at[pl.ds(0, n - 1)], DST)
    wait_out(base_out.at[pl.ds(0, n - 1)], BASE)
    wait_out(near_out.at[pl.ds(0, 2 * REACH * span)], NEAR)

    @pl.when(me < owners)
    def _():
        wait_out(emb_out.at[pl.ds(0, owners - 1)], EMB)
        wait_out(part_out.at[pl.ds(0, owners - 1)], PART)
        wait_out(back_out.at[0, pl.ds(0, n - 1)], HOT)

    @pl.when(me >= owners)
    def _():
        wait_out(emb_out, EMB)
        wait_out(part_out, PART)

    to_core(base_in.at[core], base_in.at[core], FWDB).wait_send()
    to_core(near_in.at[core], near_in.at[core], FWDN).wait_send()
    send.wait_send()
    send2.wait_send()
    for h in range(2):
        wait_out(back_out.at[h, pl.ds(0, n - 1)], BACK1 if h else BACK)
    wait_out(nback_out.at[:, pl.ds(0, 2 * REACH * span)], NBACK)


def cap_near(capacity):
    return (capacity - KEEP) // 2


def lay_out(table, take, mark):
    high = jnp.floor(table * (1.0 / 32.0))
    low = table - 32.0 * high
    dot = functools.partial(jnp.dot, preferred_element_type=jnp.float32)
    moved = 32.0 * dot(high.astype(jnp.bfloat16), take) + dot(low.astype(jnp.bfloat16), take)
    group = mark.shape[0]
    moved = moved.reshape(table.shape[0] // group, group, take.shape[1])
    return (moved * mark[None]).sum(axis=1).astype(jnp.int32) - 1


def base_layout(capacity, h):
    shape = (capacity, CHUNK)
    lane = lax.broadcasted_iota(jnp.int32, shape, 1)
    slot = lax.broadcasted_iota(jnp.int32, shape, 0)
    take = jnp.where(slot == h * HALF + (lane & (HALF - 1)), 1.0, 0.0).astype(jnp.bfloat16)
    group = CHUNK // HALF
    lane = lax.broadcasted_iota(jnp.int32, (group, CHUNK), 1)
    row = lax.broadcasted_iota(jnp.int32, (group, CHUNK), 0)
    return take, jnp.where(row * HALF <= lane, 1.0, 0.0) * jnp.where(lane < row * HALF + HALF, 1.0, 0.0)


def near_layout(capacity, h):
    span = cap_near(capacity)
    count = 2 * REACH + 1
    shape = (capacity, NEAR_ROWS)
    lane = lax.broadcasted_iota(jnp.int32, shape, 1)
    slot = lax.broadcasted_iota(jnp.int32, shape, 0)
    within = lane
    for i in range(1, count + 1):
        within = within - jnp.where(lane >= i * span, span, 0)
    take = jnp.where(slot == KEEP + h * span + within, 1.0, 0.0).astype(jnp.bfloat16)
    lane = lax.broadcasted_iota(jnp.int32, (8, NEAR_ROWS), 1)
    row = lax.broadcasted_iota(jnp.int32, (8, NEAR_ROWS), 0)
    inside = jnp.where(row * span <= lane, 1.0, 0.0) * jnp.where(lane < row * span + span, 1.0, 0.0)
    return take, inside * jnp.where(row < count, 1.0, 0.0)


def compact(hot, grid_state, w_src, bias_src, mesh_embed, w_node, w_dec, slot_src, slot_dst, slot_count):
    n = lax.axis_size("graph")
    capacity = slot_src.shape[2]
    grid_rows, width = grid_state.shape
    mesh_rows, half = mesh_embed.shape
    quarter = width // 2
    owners = mesh_rows // OWN
    bf, f32 = jnp.bfloat16, jnp.float32
    vm = pltpu.VMEM
    return pl.pallas_call(
        functools.partial(step_kernel, n),
        out_shape=jax.ShapeDtypeStruct((grid_rows, quarter), bf),
        in_specs=[pl.BlockSpec(memory_space=pltpu.SMEM)] + [pl.BlockSpec(memory_space=vm)] * 9,
        out_specs=pl.BlockSpec(memory_space=vm),
        scratch_shapes=[
            vm((n, capacity), f32), vm((n, capacity), f32),
            vm((2, n * HALF // CHUNK + 1, CHUNK), jnp.int32), vm((2, n * HALF // CHUNK + 1, CHUNK), jnp.int32),
            vm((n, HALF, width), bf), vm((NEAR_ROWS, width), bf),
            vm((2, n, HALF, width), bf), vm((2, NEAR_ROWS, width), bf),
            vm((n, 1, capacity), jnp.int32), vm((n, OWN, quarter), bf), vm((owners, OWN, quarter), bf), vm((mesh_rows, quarter), f32),
            vm((owners, OWN, half), bf), vm((n, OWN, half), bf),
            vm((mesh_rows + OWN, half), f32),
            vm((mesh_rows + OWN, half), f32), vm((mesh_rows + OWN, half), f32),
            vm((mesh_rows + OWN, quarter), f32), vm((mesh_rows + OWN, quarter), f32), vm((mesh_rows, quarter), bf),
            vm((2, n, HALF, quarter), bf), vm((2, NEAR_ROWS, quarter), bf),
            vm((2, n, HALF, quarter), bf), vm((2, NEAR_ROWS, quarter), bf),
            vm((OWN, quarter), bf), vm((owners, OWN, quarter), bf),
            vm((grid_rows, quarter), f32),
            pltpu.SemaphoreType.DMA((14,)), pltpu.SemaphoreType.DMA((14,)),
        ],
        compiler_params=pltpu.CompilerParams(collective_id=0, has_side_effects=True, vmem_limit_bytes=48 * 1024 * 1024),
    )(hot, grid_state, w_src, bias_src[None, :], mesh_embed, w_node, w_dec, slot_src, slot_dst, slot_count)


def on_device(grid_state, w_src, bias_src, mesh_embed, w_node, w_dec, slot_src, slot_dst, slot_count):
    args = (grid_state, w_src, bias_src, mesh_embed, w_node, w_dec, slot_src, slot_dst, slot_count)
    n = slot_count.shape[0]
    apart = jnp.abs(jnp.arange(n)[:, None] - jnp.arange(n)[None, :])
    far = jnp.minimum(apart, n - apart) > REACH
    over = far & (slot_count > KEEP)
    column = jnp.broadcast_to(jnp.arange(n, dtype=jnp.int32)[None, :], (n, n))
    last = jnp.max(jnp.where(over, column, 0))
    first = jnp.min(jnp.where(over, column, n))
    fits = last <= first
    hot = last.reshape(1)
    return lax.cond(fits, lambda: compact(hot, *args), lambda: dense(*args))


def solution(mesh):
    placed = (
        P(("member", "graph"), None),
        P(None, "chan"),
        P("chan"),
        P("graph", "chan"),
        P("chan", None),
        P("chan", None),
        P("graph", None, None),
        P(None, "graph", None),
        P(),
    )
    return jax.shard_map(
        on_device,
        mesh=mesh,
        in_specs=placed,
        out_specs=P(("member", "graph"), "chan"),
        check_vma=False,
    )
```

```python
import functools
import math

import jax
import jax.numpy as jnp
from jax import lax
from jax.experimental import pallas as pl
from jax.experimental.pallas import tpu as pltpu
from jax.sharding import PartitionSpec as P

MESH_ID = pl.DeviceIdType.MESH
KEEP = 32
HALF = KEEP // 2
GROUP = 7
SEMS = 16
REACH = 2
OWN = 16
NEAR_ROWS = 256
CHUNK = 256

def split_up(value, dim, count):
    lengths = value.shape
    parts = value.reshape(*lengths[:dim], count, lengths[dim] // count, *lengths[dim + 1 :])
    return jnp.moveaxis(parts, dim, 0)


def sum_at_owner(value, axis, dim):
    parts = split_up(value, dim, lax.axis_size(axis))
    arrived = lax.all_to_all(parts, axis, split_axis=0, concat_axis=0, tiled=True)
    return arrived.sum(axis=0)


def edge_network(source_rows, w_src, bias_src):
    return jax.nn.silu(
        jnp.dot(source_rows, w_src, preferred_element_type=jnp.float32) + bias_src
    ).astype(jnp.bfloat16)


def segment_rows(values, indices, usable, row_count):
    slot_total = values.shape[0]
    width = values.shape[1]
    block_len = math.gcd(slot_total, 2048)
    block_count = slot_total // block_len
    targets = jnp.where(usable, indices, -1).reshape(block_count, block_len)
    pieces = values.reshape(block_count, block_len, width)
    row_ids = jnp.arange(row_count, dtype=jnp.int32)

    def add_block(summed, scan_item):
        row_target, piece_vals = scan_item
        one_hot = (row_ids[:, None] == row_target[None, :]).astype(jnp.bfloat16)
        return (summed + jnp.dot(one_hot, piece_vals, preferred_element_type=jnp.float32), None)

    result, unused = lax.scan(
        add_block, jnp.zeros((row_count, width), jnp.float32), (targets, pieces)
    )
    return result


def dense(
    grid_state, w_src, bias_src, mesh_embed, w_node, w_dec, slot_src, slot_dst, slot_count
):
    peers = lax.axis_size("graph")
    own_index = lax.axis_index("graph")
    core_index = lax.axis_index("chan")
    capacity = slot_src.shape[2]
    positions = jnp.arange(capacity, dtype=jnp.int32)
    grid_rows = grid_state.shape[0]
    mesh_rows = mesh_embed.shape[0]
    sent_counts = lax.dynamic_slice_in_dim(slot_count, own_index, 1, 0)[0]
    recv_counts = lax.dynamic_slice_in_dim(slot_count, own_index, 1, 1)[:, 0]
    half_slots = capacity // 2
    chosen = lax.dynamic_slice_in_dim(slot_src[0], core_index * half_slots, half_slots, 1)
    picked = jnp.take(grid_state, chosen.reshape(-1), axis=0).reshape(
        peers, half_slots, grid_state.shape[1]
    )
    arrived = lax.all_to_all(picked, "graph", split_axis=0, concat_axis=0, tiled=True)
    partner = lax.ppermute(arrived, "chan", [(0, 1), (1, 0)])
    joined = jnp.where(
        core_index == 0,
        jnp.concatenate([arrived, partner], axis=1),
        jnp.concatenate([partner, arrived], axis=1),
    )
    messages = edge_network(joined.reshape(peers * capacity, grid_state.shape[1]), w_src, bias_src)
    arrive_ok = (positions[None, :] < recv_counts[:, None]).reshape(-1)
    dst_rows = slot_dst[:, 0, :].reshape(-1)
    aggregate = segment_rows(messages, dst_rows, arrive_ok, mesh_rows)
    partial_hidden = jnp.dot(
        aggregate.astype(jnp.bfloat16), w_node, preferred_element_type=jnp.float32
    )
    hidden_pre = sum_at_owner(partial_hidden, "chan", 1)
    latent = (mesh_embed.astype(jnp.float32) + jax.nn.silu(hidden_pre)).astype(jnp.bfloat16)
    partial_proj = jnp.dot(latent, w_dec, preferred_element_type=jnp.float32)
    projected = sum_at_owner(partial_proj, "chan", 1).astype(jnp.bfloat16)
    returned = jnp.take(projected, dst_rows, axis=0).reshape(peers, capacity, projected.shape[1])
    came_back = lax.all_to_all(returned, "graph", split_axis=0, concat_axis=0, tiled=True).reshape(
        peers * capacity, projected.shape[1]
    )
    send_ok = (positions[None, :] < sent_counts[:, None]).reshape(-1)
    decoded = segment_rows(came_back, slot_src[0].reshape(-1), send_ok, grid_rows)
    width_half = decoded.shape[1]
    own_cols = lax.dynamic_slice_in_dim(grid_state, core_index * width_half, width_half, 1)
    return (own_cols.astype(jnp.float32) + decoded).astype(jnp.bfloat16)


def torus(n):
    wide = 1 << (n.bit_length() // 2)
    return n // wide, wide


def visit_order(n):
    tall, wide = torus(n)
    offsets = [(r, c) for r in range(tall) for c in range(wide)][1:]
    offsets.sort(key=lambda o: min(o[0], tall - o[0]) + min(o[1], wide - o[1]))
    return [offsets[i // 2] if i % 2 == 0 else offsets[-1 - i // 2] for i in range(n - 1)]


def silu(v):
    h = 0.5 * v
    return h + h * jnp.tanh(h)


def pick_turned(table, idx):
    rows = table.shape[0]
    hot = jnp.where(
        lax.broadcasted_iota(jnp.int32, (rows, idx.shape[1]), 0) == idx, 1.0, 0.0
    ).astype(jnp.bfloat16)
    return lax.dot_general(table, hot, (((0,), (0,)), ((), ())), preferred_element_type=jnp.float32)


def spread(rows, idx):
    return jnp.where(
        lax.broadcasted_iota(jnp.int32, (rows, idx.shape[1]), 0) == idx, 1.0, 0.0
    ).astype(jnp.bfloat16)


def step_kernel(
    n, hot_ref, grid_hbm, wsrc_hbm, bias_hbm, embed_hbm, wnode_hbm, wdec_hbm, src_hbm, dst_hbm, count_hbm, out_ref,
    grid_ref, wsrc_ref, bias_ref, embed_ref, wnode_ref, wdec_ref, src_ref, dst_ref, count_ref,
    src_live, dst_live, srcx_ref, dstx_ref,
    base_out, near_out, base_in, near_in, dst_in, emb_in, emb_out, emb_half, part_out, part_in,
    acc, hid_out, hid_in, prj_out, prj_in, prj_bf, back_out, nback_out, back_in, nback_in, hot_out, hot_in, dec,
    hhid_out, hhid_in, hprj_out, hprj_in,
    lsem, ssem, rsem,
):
    me = lax.axis_index("graph")
    core = lax.axis_index("chan")
    other = 1 - core
    grid_rows = grid_ref.shape[0]
    mesh_rows = embed_ref.shape[0]
    owners = mesh_rows // OWN
    span = cap_near(dst_ref.shape[2])
    used = (2 * REACH + 1) * span
    half = hid_out.shape[1]
    quarter = prj_out.shape[1]
    bf = jnp.bfloat16
    dot = functools.partial(jnp.dot, preferred_element_type=jnp.float32)

    pairs = (
        (src_hbm, src_ref), (dst_hbm, dst_ref), (count_hbm, count_ref), (grid_hbm, grid_ref), (embed_hbm, embed_ref),
        (wdec_hbm, wdec_ref), (wsrc_hbm, wsrc_ref), (bias_hbm, bias_ref), (wnode_hbm, wnode_ref),
    )
    SRC, DSTS, COUNT, GRID, EMBED, WDEC, WSRC, BIAS, WNODE = (
        pltpu.make_async_copy(x, y, lsem.at[i]) for i, (x, y) in enumerate(pairs))
    for copy in (SRC, DSTS, COUNT, GRID, EMBED, WDEC, WSRC, BIAS, WNODE):
        copy.start()

    tall, wide = torus(n)
    codes = [r * 2 * wide + c for r, c in visit_order(n)]
    groups = [codes[i:i + GROUP] for i in range(0, n - 1, GROUP)]
    spot = 2 * wide * (me // wide) + lax.rem(me, wide) + core * (2 * wide * tall + wide)
    turn = 1 - 2 * core

    def each_peer(visit):
        @pl.loop(0, len(groups))
        def _(g):
            for part in (range(0, 4), range(4, GROUP)):
                packed = jnp.int32(0)
                for i, group in enumerate(groups):
                    packed = jnp.where(g == i, sum(group[k] << (7 * j) for j, k in enumerate(part)), packed)
                for j in range(len(part)):
                    code = lax.shift_right_logical(packed, jnp.int32(7 * j)) & 127
                    at = spot + turn * code
                    visit((lax.shift_right_logical(at, jnp.int32(1)) & ((tall - 1) * wide)) + (at & (wide - 1)))

    barrier = pltpu.get_barrier_semaphore()
    each_peer(lambda peer: pl.semaphore_signal(barrier, inc=1, device_id={"graph": peer}, device_id_type=MESH_ID))
    pl.semaphore_signal(barrier, inc=1, device_id={"chan": other}, device_id_type=MESH_ID)

    def to_graph(src, dst, k, peer):
        return pltpu.make_async_remote_copy(
            src_ref=src, dst_ref=dst, send_sem=ssem.at[k], recv_sem=rsem.at[k],
            device_id={"graph": peer}, device_id_type=MESH_ID)

    def to_core(src, dst, k):
        return pltpu.make_async_remote_copy(
            src_ref=src, dst_ref=dst, send_sem=ssem.at[k], recv_sem=rsem.at[k],
            device_id={"chan": other}, device_id_type=MESH_ID)

    def wait_in(ref, k):
        to_graph(ref, ref, k, me).wait_recv()

    def wait_out(ref, k):
        to_graph(ref, ref, k, me).wait_send()

    DST, EMB, BASE, NEAR, PART, FWDB, FWDN, HID, PRJ, BACK, NBACK, HOT, PRJ0, BACK1, HIDH, PRJH = range(SEMS)

    blocks = (n * HALF) // CHUNK
    capacity = dst_ref.shape[2]
    SRC.wait()
    DSTS.wait()
    COUNT.wait()
    with jax.named_scope("index"):
        hot = hot_ref[0]
        ids = lax.broadcasted_iota(jnp.int32, (n, n), 0)
        cols = lax.broadcasted_iota(jnp.int32, (n, n), 1)
        counts = count_ref[...]
        sent = jnp.where(ids == me, counts, 0).sum(axis=0, keepdims=True)
        sent = jnp.where(ids == cols, sent, 0).sum(axis=1, keepdims=True)
        came = jnp.where(cols == me, counts, 0).sum(axis=1, keepdims=True)
        pos = lax.broadcasted_iota(jnp.int32, (n, capacity), 1)
        src_all = jnp.where(pos < sent, src_ref[0] + 1, 0).astype(jnp.float32)
        src_live[...] = src_all
        came = jnp.where(me == hot, 0, came)
        dst_all = jnp.where(pos < came, dst_ref[:, 0, :] + 1, 0).astype(jnp.float32)
        dst_live[...] = dst_all
        rows_id = lax.broadcasted_iota(jnp.int32, (n, capacity), 0)
        src_all = jnp.where(rows_id == hot, 0.0, src_all)
        near_id = lax.broadcasted_iota(jnp.int32, (8, capacity), 0)
        near_src = jnp.zeros((8, capacity), jnp.float32)
        near_dst = jnp.zeros((8, capacity), jnp.float32)
        for o in range(-REACH, REACH + 1):
            to = lax.rem(me + o + n, n)
            row = jnp.where(to == hot, 0.0, src_live[pl.ds(to, 1)])
            near_src = jnp.where(near_id == o + REACH, row, near_src)
            near_dst = jnp.where(near_id == o + REACH, dst_live[pl.ds(lax.rem(me - o + n, n), 1)], near_dst)
        for h in range(2):
            base = base_layout(capacity, h)
            srcx_ref[h, 0:blocks] = lay_out(src_all, *base)
            dstx_ref[h, 0:blocks] = lay_out(dst_all, *base)
            near = near_layout(capacity, h)
            srcx_ref[h, blocks:] = lay_out(near_src, *near)[:, 0:CHUNK]
            dstx_ref[h, blocks:] = lay_out(near_dst, *near)[:, 0:CHUNK]

    GRID.wait()

    @pl.loop(0, blocks)
    def _(j):
        rows = pick_turned(grid_ref[...], srcx_ref[core, pl.ds(j, 1)]).T.astype(bf)
        base_out[pl.ds(j * (CHUNK // HALF), CHUNK // HALF)] = rows.reshape(CHUNK // HALF, HALF, rows.shape[1])

    near_out[...] = pick_turned(grid_ref[...], srcx_ref[core, blocks:]).T.astype(bf)
    near_in[core, used:, :] = jnp.zeros((NEAR_ROWS - used, near_in.shape[2]), bf)

    pl.semaphore_wait(barrier, n)
    each_peer(lambda peer: to_graph(dst_ref.at[peer], dst_in.at[me], DST, peer).start())
    for o in range(-REACH, REACH + 1):
        rows = pl.ds((o + REACH) * span, span)
        if o == 0:
            near_in[core, (o + REACH) * span:(o + REACH + 1) * span] = near_out[(o + REACH) * span:(o + REACH + 1) * span]
        else:
            to_graph(near_out.at[rows], near_in.at[core, rows], NEAR, lax.rem(me + o + n, n)).start()
    each_peer(lambda peer: to_graph(base_out.at[peer], base_in.at[core, me], BASE, peer).start())
    base_in[core, pl.ds(me, 1)] = base_out[pl.ds(me, 1)]
    dst_in[pl.ds(me, 1)] = dst_ref[pl.ds(me, 1)]

    EMBED.wait()
    WDEC.wait()
    w_other = wdec_ref[:, pl.ds(pl.multiple_of(other * quarter, quarter), quarter)]
    w_own = wdec_ref[:, pl.ds(pl.multiple_of(core * quarter, quarter), quarter)]
    prj_out[...] = dot(embed_ref[...], w_other)
    send0 = to_core(prj_out, emb_half, PRJ0)
    send0.start()
    WSRC.wait()
    BIAS.wait()
    hot_src = src_live[pl.ds(hot, 1)].astype(jnp.int32) - 1
    msgs = silu(dot(pick_turned(grid_ref[...], hot_src).T.astype(bf), wsrc_ref[...]) + bias_ref[...]).astype(bf)
    emb_own = dot(embed_ref[...], w_own)
    send0.wait_recv()
    emb_out[...] = (emb_own + emb_half[...]).astype(bf).reshape(owners, OWN, quarter)

    wait_in(dst_in.at[pl.ds(0, n - 1)], DST)
    hot_dst = jnp.where(hot_src >= 0, dst_in[hot], -1)
    part_out[...] = dot(spread(mesh_rows, hot_dst), msgs).astype(bf).reshape(owners, OWN, half)

    def send_share(peer):
        @pl.when(peer < owners)
        def _():
            to_graph(part_out.at[peer], part_in.at[me], PART, peer).start()
            to_graph(emb_out.at[peer], emb_in.at[me], EMB, peer).start()

    each_peer(send_share)

    wait_in(base_in.at[core, pl.ds(0, n - 1)], BASE)
    to_core(base_in.at[core], base_in.at[core], FWDB).start()
    wait_in(near_in.at[core, pl.ds(0, 2 * REACH * span)], NEAR)
    to_core(near_in.at[core], near_in.at[core], FWDN).start()
    acc[...] = jnp.zeros_like(acc)

    def add_rows(rows, idx):
        m = silu(dot(rows, wsrc_ref[...]) + bias_ref[...]).astype(bf)
        acc[...] += dot(spread(mesh_rows, idx), m)

    def add_half(h):
        @pl.loop(0, blocks)
        def _(j):
            rows = base_in[h, pl.ds(j * (CHUNK // HALF), CHUNK // HALF)].reshape(CHUNK, base_in.shape[3])
            add_rows(rows, dstx_ref[h, pl.ds(j, 1)])
        add_rows(near_in[h], dstx_ref[h, blocks:])

    add_half(core)
    to_core(base_in.at[other], base_in.at[other], FWDB).wait_recv()
    to_core(near_in.at[other], near_in.at[other], FWDN).wait_recv()
    add_half(other)

    WNODE.wait()
    n_other = wnode_ref[:, pl.ds(pl.multiple_of(other * half, half), half)]
    n_own = wnode_ref[:, pl.ds(pl.multiple_of(core * half, half), half)]
    agg = acc[...].astype(bf)
    hid_out[...] = dot(agg, n_other)
    send = to_core(hid_out, hid_in, HID)
    send.start()
    own = dot(agg, n_own)
    send0.wait_send()
    send.wait_recv()
    lat = (embed_ref[...].astype(jnp.float32) + silu(own + hid_in[...])).astype(bf)
    prj_out[...] = dot(lat, w_other)
    send2 = to_core(prj_out, prj_in, PRJ)
    send2.start()
    own_p = dot(lat, w_own)

    @pl.when(me < owners)
    def _():
        wait_in(part_in.at[pl.ds(0, n - 1)], PART)
        wait_in(emb_in.at[pl.ds(0, n - 1)], EMB)
        part_in[pl.ds(me, 1)] = part_out[pl.ds(me, 1)]
        emb_in[pl.ds(me, 1)] = emb_out[pl.ds(me, 1)]

    hot_agg = part_in[...].astype(jnp.float32).sum(axis=0).astype(bf)
    hhid_out[...] = dot(hot_agg, n_other)
    send3 = to_core(hhid_out, hhid_in, HIDH)
    send3.start()
    hot_own = dot(hot_agg, n_own)

    send2.wait_recv()
    prj_bf[...] = (own_p + prj_in[...]).astype(bf)
    for h in range(2):
        nback_out[h] = pick_turned(prj_bf[...], dstx_ref[h, blocks:]).T.astype(bf)
        nback_in[h, used:, :] = jnp.zeros((NEAR_ROWS - used, quarter), bf)
        for o in range(-REACH, REACH + 1):
            a = (o + REACH) * span
            if o == 0:
                nback_in[h, a:a + span] = nback_out[h, a:a + span]
            else:
                to_graph(nback_out.at[h, pl.ds(a, span)], nback_in.at[h, pl.ds(a, span)], NBACK, lax.rem(me - o + n, n)).start()

    def return_half(h):
        @pl.loop(0, blocks)
        def _(j):
            rows = pick_turned(prj_bf[...], dstx_ref[h, pl.ds(j, 1)]).T.astype(bf)
            back_out[h, pl.ds(j * (CHUNK // HALF), CHUNK // HALF)] = rows.reshape(CHUNK // HALF, HALF, quarter)

        back_in[h, pl.ds(me, 1)] = back_out[h, pl.ds(me, 1)]

    return_half(0)
    send3.wait_recv()
    hot_lat = silu(hot_own + hhid_in[...]).astype(bf)
    hprj_out[...] = dot(hot_lat, w_other)
    send4 = to_core(hprj_out, hprj_in, PRJH)
    send4.start()
    hot_prj = dot(hot_lat, w_own) + emb_in[hot].astype(jnp.float32)
    each_peer(lambda peer: to_graph(back_out.at[0, peer], back_in.at[0, me], BACK, peer).start())
    return_half(1)
    send4.wait_recv()
    hot_out[...] = (hot_prj + hprj_in[...]).astype(bf)

    def send_rest(peer):
        to_graph(back_out.at[1, peer], back_in.at[1, me], BACK1, peer).start()

        @pl.when(me < owners)
        def _():
            to_graph(hot_out, hot_in.at[me], HOT, peer).start()

    each_peer(send_rest)

    dec[...] = grid_ref[:, pl.ds(pl.multiple_of(core * quarter, quarter), quarter)].astype(jnp.float32)
    wait_in(nback_in.at[:, pl.ds(0, 2 * REACH * span)], NBACK)
    for h in range(2):
        dec[...] += dot(spread(grid_rows, srcx_ref[h, blocks:]), nback_in[h])

    for h in range(2):
        wait_in(back_in.at[h, pl.ds(0, n - 1)], BACK1 if h else BACK)

        @pl.loop(0, blocks)
        def _(j):
            rows = back_in[h, pl.ds(j * (CHUNK // HALF), CHUNK // HALF)].reshape(CHUNK, quarter)
            dec[...] += dot(spread(grid_rows, srcx_ref[h, pl.ds(j, 1)]), rows)

    @pl.when(me < owners)
    def _():
        wait_in(hot_in.at[pl.ds(0, owners - 1)], HOT)
        hot_in[pl.ds(me, 1)] = hot_out[...].reshape(1, OWN, quarter)

    @pl.when(me >= owners)
    def _():
        wait_in(hot_in, HOT)

    hot_rows = pick_turned(hot_in[...].reshape(mesh_rows, quarter), hot_dst).astype(bf)
    back = lax.dot_general(spread(grid_rows, hot_src), hot_rows, (((1,), (1,)), ((), ())), preferred_element_type=jnp.float32)
    out_ref[...] = (dec[...] + back).astype(bf)

    wait_out(dst_ref.at[pl.ds(0, n - 1)], DST)
    wait_out(base_out.at[pl.ds(0, n - 1)], BASE)
    wait_out(near_out.at[pl.ds(0, 2 * REACH * span)], NEAR)

    @pl.when(me < owners)
    def _():
        wait_out(emb_out.at[pl.ds(0, owners - 1)], EMB)
        wait_out(part_out.at[pl.ds(0, owners - 1)], PART)
        wait_out(back_out.at[0, pl.ds(0, n - 1)], HOT)

    @pl.when(me >= owners)
    def _():
        wait_out(emb_out, EMB)
        wait_out(part_out, PART)

    to_core(base_in.at[core], base_in.at[core], FWDB).wait_send()
    to_core(near_in.at[core], near_in.at[core], FWDN).wait_send()
    for copy in (send, send2, send3, send4):
        copy.wait_send()
    for h in range(2):
        wait_out(back_out.at[h, pl.ds(0, n - 1)], BACK1 if h else BACK)
    wait_out(nback_out.at[:, pl.ds(0, 2 * REACH * span)], NBACK)


def cap_near(capacity):
    return (capacity - KEEP) // 2


def lay_out(table, take, mark):
    high = jnp.floor(table * (1.0 / 32.0))
    low = table - 32.0 * high
    dot = functools.partial(jnp.dot, preferred_element_type=jnp.float32)
    moved = 32.0 * dot(high.astype(jnp.bfloat16), take) + dot(low.astype(jnp.bfloat16), take)
    group = mark.shape[0]
    moved = moved.reshape(table.shape[0] // group, group, take.shape[1])
    return (moved * mark[None]).sum(axis=1).astype(jnp.int32) - 1


def base_layout(capacity, h):
    shape = (capacity, CHUNK)
    lane = lax.broadcasted_iota(jnp.int32, shape, 1)
    slot = lax.broadcasted_iota(jnp.int32, shape, 0)
    take = jnp.where(slot == h * HALF + (lane & (HALF - 1)), 1.0, 0.0).astype(jnp.bfloat16)
    group = CHUNK // HALF
    lane = lax.broadcasted_iota(jnp.int32, (group, CHUNK), 1)
    row = lax.broadcasted_iota(jnp.int32, (group, CHUNK), 0)
    return take, jnp.where(row * HALF <= lane, 1.0, 0.0) * jnp.where(lane < row * HALF + HALF, 1.0, 0.0)


def near_layout(capacity, h):
    span = cap_near(capacity)
    count = 2 * REACH + 1
    shape = (capacity, NEAR_ROWS)
    lane = lax.broadcasted_iota(jnp.int32, shape, 1)
    slot = lax.broadcasted_iota(jnp.int32, shape, 0)
    within = lane
    for i in range(1, count + 1):
        within = within - jnp.where(lane >= i * span, span, 0)
    take = jnp.where(slot == KEEP + h * span + within, 1.0, 0.0).astype(jnp.bfloat16)
    lane = lax.broadcasted_iota(jnp.int32, (8, NEAR_ROWS), 1)
    row = lax.broadcasted_iota(jnp.int32, (8, NEAR_ROWS), 0)
    inside = jnp.where(row * span <= lane, 1.0, 0.0) * jnp.where(lane < row * span + span, 1.0, 0.0)
    return take, inside * jnp.where(row < count, 1.0, 0.0)


def compact(hot, grid_state, w_src, bias_src, mesh_embed, w_node, w_dec, slot_src, slot_dst, slot_count):
    n = lax.axis_size("graph")
    capacity = slot_src.shape[2]
    grid_rows, width = grid_state.shape
    mesh_rows, half = mesh_embed.shape
    quarter = width // 2
    owners = mesh_rows // OWN
    bf, f32 = jnp.bfloat16, jnp.float32
    vm = pltpu.VMEM
    return pl.pallas_call(
        functools.partial(step_kernel, n),
        out_shape=jax.ShapeDtypeStruct((grid_rows, quarter), bf),
        in_specs=[pl.BlockSpec(memory_space=pltpu.SMEM)] + [pl.BlockSpec(memory_space=pl.ANY)] * 9,
        out_specs=pl.BlockSpec(memory_space=vm),
        scratch_shapes=[
            vm((grid_rows, width), bf), vm(w_src.shape, bf), vm((1, half), f32), vm((mesh_rows, half), bf), vm(w_node.shape, bf),
            vm(w_dec.shape, bf), vm(slot_src.shape, jnp.int32), vm(slot_dst.shape, jnp.int32), vm(slot_count.shape, jnp.int32),
            vm((n, capacity), f32), vm((n, capacity), f32),
            vm((2, n * HALF // CHUNK + 1, CHUNK), jnp.int32), vm((2, n * HALF // CHUNK + 1, CHUNK), jnp.int32),
            vm((n, HALF, width), bf), vm((NEAR_ROWS, width), bf),
            vm((2, n, HALF, width), bf), vm((2, NEAR_ROWS, width), bf),
            vm((n, 1, capacity), jnp.int32), vm((n, OWN, quarter), bf), vm((owners, OWN, quarter), bf), vm((mesh_rows, quarter), f32),
            vm((owners, OWN, half), bf), vm((n, OWN, half), bf),
            vm((mesh_rows, half), f32),
            vm((mesh_rows, half), f32), vm((mesh_rows, half), f32),
            vm((mesh_rows, quarter), f32), vm((mesh_rows, quarter), f32), vm((mesh_rows, quarter), bf),
            vm((2, n, HALF, quarter), bf), vm((2, NEAR_ROWS, quarter), bf),
            vm((2, n, HALF, quarter), bf), vm((2, NEAR_ROWS, quarter), bf),
            vm((OWN, quarter), bf), vm((owners, OWN, quarter), bf),
            vm((grid_rows, quarter), f32),
            vm((OWN, half), f32), vm((OWN, half), f32), vm((OWN, quarter), f32), vm((OWN, quarter), f32),
            pltpu.SemaphoreType.DMA((9,)), pltpu.SemaphoreType.DMA((SEMS,)), pltpu.SemaphoreType.DMA((SEMS,)),
        ],
        compiler_params=pltpu.CompilerParams(collective_id=0, has_side_effects=True, vmem_limit_bytes=48 * 1024 * 1024),
    )(hot, grid_state, w_src, bias_src[None, :], mesh_embed, w_node, w_dec, slot_src, slot_dst, slot_count)


def on_device(grid_state, w_src, bias_src, mesh_embed, w_node, w_dec, slot_src, slot_dst, slot_count):
    args = (grid_state, w_src, bias_src, mesh_embed, w_node, w_dec, slot_src, slot_dst, slot_count)
    n = slot_count.shape[0]
    apart = jnp.abs(jnp.arange(n)[:, None] - jnp.arange(n)[None, :])
    far = jnp.minimum(apart, n - apart) > REACH
    over = far & (slot_count > KEEP)
    column = jnp.broadcast_to(jnp.arange(n, dtype=jnp.int32)[None, :], (n, n))
    last = jnp.max(jnp.where(over, column, 0))
    first = jnp.min(jnp.where(over, column, n))
    fits = last <= first
    hot = last.reshape(1)
    return lax.cond(fits, lambda: compact(hot, *args), lambda: dense(*args))


def solution(mesh):
    placed = (
        P(("member", "graph"), None),
        P(None, "chan"),
        P("chan"),
        P("graph", "chan"),
        P("chan", None),
        P("chan", None),
        P("graph", None, None),
        P(None, "graph", None),
        P(),
    )
    return jax.shard_map(
        on_device,
        mesh=mesh,
        in_specs=placed,
        out_specs=P(("member", "graph"), "chan"),
        check_vma=False,
    )
```

```python
import functools
import math

import jax
import jax.numpy as jnp
from jax import lax
from jax.experimental import pallas as pl
from jax.experimental.pallas import tpu as pltpu
from jax.sharding import PartitionSpec as P

MESH_ID = pl.DeviceIdType.MESH
KEEP = 32
HALF = KEEP // 2
GROUP = 7
SEMS = 16
REACH = 2
OWN = 16
NEAR_ROWS = 256
CHUNK = 256

def split_up(value, dim, count):
    lengths = value.shape
    parts = value.reshape(*lengths[:dim], count, lengths[dim] // count, *lengths[dim + 1 :])
    return jnp.moveaxis(parts, dim, 0)


def sum_at_owner(value, axis, dim):
    parts = split_up(value, dim, lax.axis_size(axis))
    arrived = lax.all_to_all(parts, axis, split_axis=0, concat_axis=0, tiled=True)
    return arrived.sum(axis=0)


def edge_network(source_rows, w_src, bias_src):
    return jax.nn.silu(
        jnp.dot(source_rows, w_src, preferred_element_type=jnp.float32) + bias_src
    ).astype(jnp.bfloat16)


def segment_rows(values, indices, usable, row_count):
    slot_total = values.shape[0]
    width = values.shape[1]
    block_len = math.gcd(slot_total, 2048)
    block_count = slot_total // block_len
    targets = jnp.where(usable, indices, -1).reshape(block_count, block_len)
    pieces = values.reshape(block_count, block_len, width)
    row_ids = jnp.arange(row_count, dtype=jnp.int32)

    def add_block(summed, scan_item):
        row_target, piece_vals = scan_item
        one_hot = (row_ids[:, None] == row_target[None, :]).astype(jnp.bfloat16)
        return (summed + jnp.dot(one_hot, piece_vals, preferred_element_type=jnp.float32), None)

    result, unused = lax.scan(
        add_block, jnp.zeros((row_count, width), jnp.float32), (targets, pieces)
    )
    return result


def dense(
    grid_state, w_src, bias_src, mesh_embed, w_node, w_dec, slot_src, slot_dst, slot_count
):
    peers = lax.axis_size("graph")
    own_index = lax.axis_index("graph")
    core_index = lax.axis_index("chan")
    capacity = slot_src.shape[2]
    positions = jnp.arange(capacity, dtype=jnp.int32)
    grid_rows = grid_state.shape[0]
    mesh_rows = mesh_embed.shape[0]
    sent_counts = lax.dynamic_slice_in_dim(slot_count, own_index, 1, 0)[0]
    recv_counts = lax.dynamic_slice_in_dim(slot_count, own_index, 1, 1)[:, 0]
    half_slots = capacity // 2
    chosen = lax.dynamic_slice_in_dim(slot_src[0], core_index * half_slots, half_slots, 1)
    picked = jnp.take(grid_state, chosen.reshape(-1), axis=0).reshape(
        peers, half_slots, grid_state.shape[1]
    )
    arrived = lax.all_to_all(picked, "graph", split_axis=0, concat_axis=0, tiled=True)
    partner = lax.ppermute(arrived, "chan", [(0, 1), (1, 0)])
    joined = jnp.where(
        core_index == 0,
        jnp.concatenate([arrived, partner], axis=1),
        jnp.concatenate([partner, arrived], axis=1),
    )
    messages = edge_network(joined.reshape(peers * capacity, grid_state.shape[1]), w_src, bias_src)
    arrive_ok = (positions[None, :] < recv_counts[:, None]).reshape(-1)
    dst_rows = slot_dst[:, 0, :].reshape(-1)
    aggregate = segment_rows(messages, dst_rows, arrive_ok, mesh_rows)
    partial_hidden = jnp.dot(
        aggregate.astype(jnp.bfloat16), w_node, preferred_element_type=jnp.float32
    )
    hidden_pre = sum_at_owner(partial_hidden, "chan", 1)
    latent = (mesh_embed.astype(jnp.float32) + jax.nn.silu(hidden_pre)).astype(jnp.bfloat16)
    partial_proj = jnp.dot(latent, w_dec, preferred_element_type=jnp.float32)
    projected = sum_at_owner(partial_proj, "chan", 1).astype(jnp.bfloat16)
    returned = jnp.take(projected, dst_rows, axis=0).reshape(peers, capacity, projected.shape[1])
    came_back = lax.all_to_all(returned, "graph", split_axis=0, concat_axis=0, tiled=True).reshape(
        peers * capacity, projected.shape[1]
    )
    send_ok = (positions[None, :] < sent_counts[:, None]).reshape(-1)
    decoded = segment_rows(came_back, slot_src[0].reshape(-1), send_ok, grid_rows)
    width_half = decoded.shape[1]
    own_cols = lax.dynamic_slice_in_dim(grid_state, core_index * width_half, width_half, 1)
    return (own_cols.astype(jnp.float32) + decoded).astype(jnp.bfloat16)


def torus(n):
    wide = 1 << (n.bit_length() // 2)
    return n // wide, wide


def visit_order(n):
    tall, wide = torus(n)
    offsets = [(r, c) for r in range(tall) for c in range(wide)][1:]
    offsets.sort(key=lambda o: min(o[0], tall - o[0]) + min(o[1], wide - o[1]))
    return [offsets[i // 2] if i % 2 == 0 else offsets[-1 - i // 2] for i in range(n - 1)]


def silu(v):
    h = 0.5 * v
    return h + h * jnp.tanh(h)


def pick_turned(table, idx):
    rows = table.shape[0]
    hot = jnp.where(
        lax.broadcasted_iota(jnp.int32, (rows, idx.shape[1]), 0) == idx, 1.0, 0.0
    ).astype(jnp.bfloat16)
    return lax.dot_general(table, hot, (((0,), (0,)), ((), ())), preferred_element_type=jnp.float32)


def spread(rows, idx):
    return jnp.where(
        lax.broadcasted_iota(jnp.int32, (rows, idx.shape[1]), 0) == idx, 1.0, 0.0
    ).astype(jnp.bfloat16)


def step_kernel(
    n, hot_ref, grid_hbm, wsrc_hbm, bias_hbm, embed_hbm, wnode_hbm, wdec_hbm, src_hbm, dst_hbm, count_hbm, out_ref,
    grid_ref, wsrc_ref, bias_ref, embed_ref, wnode_ref, wdec_ref, src_ref, dst_ref, count_ref,
    src_live, dst_live, srcx_ref, dstx_ref,
    base_out, near_out, base_in, near_in, dst_in, emb_in, emb_out, emb_half, part_out, part_in,
    acc, hid_out, hid_in, prj_out, prj_in, prj_bf, back_out, nback_out, back_in, nback_in, hot_out, hot_in, dec,
    hhid_out, hhid_in, hprj_out, hprj_in,
    lsem, ssem, rsem,
):
    me = lax.axis_index("graph")
    core = lax.axis_index("chan")
    other = 1 - core
    grid_rows = grid_ref.shape[0]
    mesh_rows = embed_ref.shape[0]
    owners = mesh_rows // OWN
    span = cap_near(dst_ref.shape[2])
    used = (2 * REACH + 1) * span
    half = hid_out.shape[1]
    quarter = prj_out.shape[1]
    bf = jnp.bfloat16
    dot = functools.partial(jnp.dot, preferred_element_type=jnp.float32)

    pairs = (
        (src_hbm, src_ref), (dst_hbm, dst_ref), (count_hbm, count_ref), (grid_hbm, grid_ref), (embed_hbm, embed_ref),
        (wdec_hbm, wdec_ref), (wsrc_hbm, wsrc_ref), (bias_hbm, bias_ref), (wnode_hbm, wnode_ref),
    )
    SRC, DSTS, COUNT, GRID, EMBED, WDEC, WSRC, BIAS, WNODE = (
        pltpu.make_async_copy(x, y, lsem.at[i]) for i, (x, y) in enumerate(pairs))
    for copy in (SRC, DSTS, COUNT, GRID, EMBED, WDEC, WSRC, BIAS, WNODE):
        copy.start()

    tall, wide = torus(n)
    codes = [r * 2 * wide + c for r, c in visit_order(n)]
    groups = [codes[i:i + GROUP] for i in range(0, n - 1, GROUP)]
    spot = 2 * wide * (me // wide) + lax.rem(me, wide) + core * (2 * wide * tall + wide)
    turn = 1 - 2 * core

    def each_peer(visit):
        @pl.loop(0, len(groups))
        def _(g):
            for part in (range(0, 4), range(4, GROUP)):
                packed = jnp.int32(0)
                for i, group in enumerate(groups):
                    packed = jnp.where(g == i, sum(group[k] << (7 * j) for j, k in enumerate(part)), packed)
                for j in range(len(part)):
                    code = lax.shift_right_logical(packed, jnp.int32(7 * j)) & 127
                    at = spot + turn * code
                    visit((lax.shift_right_logical(at, jnp.int32(1)) & ((tall - 1) * wide)) + (at & (wide - 1)))

    barrier = pltpu.get_barrier_semaphore()
    each_peer(lambda peer: pl.semaphore_signal(barrier, inc=1, device_id={"graph": peer}, device_id_type=MESH_ID))
    pl.semaphore_signal(barrier, inc=1, device_id={"chan": other}, device_id_type=MESH_ID)

    def to_graph(src, dst, k, peer):
        return pltpu.make_async_remote_copy(
            src_ref=src, dst_ref=dst, send_sem=ssem.at[k], recv_sem=rsem.at[k],
            device_id={"graph": peer}, device_id_type=MESH_ID)

    def to_core(src, dst, k):
        return pltpu.make_async_remote_copy(
            src_ref=src, dst_ref=dst, send_sem=ssem.at[k], recv_sem=rsem.at[k],
            device_id={"chan": other}, device_id_type=MESH_ID)

    def wait_in(ref, k):
        to_graph(ref, ref, k, me).wait_recv()

    def wait_out(ref, k):
        to_graph(ref, ref, k, me).wait_send()

    DST, EMB, BASE, NEAR, PART, FWDB, FWDN, HID, PRJ, BACK, NBACK, HOT, PRJ0, BACK1, HIDH, PRJH = range(SEMS)

    blocks = (n * HALF) // CHUNK
    capacity = dst_ref.shape[2]
    SRC.wait()
    DSTS.wait()
    COUNT.wait()
    with jax.named_scope("index"):
        hot = hot_ref[0]
        ids = lax.broadcasted_iota(jnp.int32, (n, n), 0)
        cols = lax.broadcasted_iota(jnp.int32, (n, n), 1)
        counts = count_ref[...]
        sent = jnp.where(ids == me, counts, 0).sum(axis=0, keepdims=True)
        sent = jnp.where(ids == cols, sent, 0).sum(axis=1, keepdims=True)
        came = jnp.where(cols == me, counts, 0).sum(axis=1, keepdims=True)
        pos = lax.broadcasted_iota(jnp.int32, (n, capacity), 1)
        src_all = jnp.where(pos < sent, src_ref[0] + 1, 0).astype(jnp.float32)
        src_live[...] = src_all
        came = jnp.where(me == hot, 0, came)
        dst_all = jnp.where(pos < came, dst_ref[:, 0, :] + 1, 0).astype(jnp.float32)
        dst_live[...] = dst_all
        rows_id = lax.broadcasted_iota(jnp.int32, (n, capacity), 0)
        src_all = jnp.where(rows_id == hot, 0.0, src_all)
        near_id = lax.broadcasted_iota(jnp.int32, (8, capacity), 0)
        near_src = jnp.zeros((8, capacity), jnp.float32)
        near_dst = jnp.zeros((8, capacity), jnp.float32)
        for o in range(-REACH, REACH + 1):
            to = lax.rem(me + o + n, n)
            row = jnp.where(to == hot, 0.0, src_live[pl.ds(to, 1)])
            near_src = jnp.where(near_id == o + REACH, row, near_src)
            near_dst = jnp.where(near_id == o + REACH, dst_live[pl.ds(lax.rem(me - o + n, n), 1)], near_dst)
        for h in range(2):
            base = base_layout(capacity, h)
            srcx_ref[h, 0:blocks] = lay_out(src_all, *base)
            dstx_ref[h, 0:blocks] = lay_out(dst_all, *base)
            near = near_layout(capacity, h)
            srcx_ref[h, blocks:] = lay_out(near_src, *near)[:, 0:CHUNK]
            dstx_ref[h, blocks:] = lay_out(near_dst, *near)[:, 0:CHUNK]

    GRID.wait()

    for j in range(blocks):
        rows = pick_turned(grid_ref[...], srcx_ref[core, j:j + 1]).T.astype(bf)
        base_out[j * (CHUNK // HALF):(j + 1) * (CHUNK // HALF)] = rows.reshape(CHUNK // HALF, HALF, rows.shape[1])

    near_out[...] = pick_turned(grid_ref[...], srcx_ref[core, blocks:]).T.astype(bf)
    near_in[core, used:, :] = jnp.zeros((NEAR_ROWS - used, near_in.shape[2]), bf)

    pl.semaphore_wait(barrier, n)
    each_peer(lambda peer: to_graph(dst_ref.at[peer], dst_in.at[me], DST, peer).start())
    for o in range(-REACH, REACH + 1):
        rows = pl.ds((o + REACH) * span, span)
        if o == 0:
            near_in[core, (o + REACH) * span:(o + REACH + 1) * span] = near_out[(o + REACH) * span:(o + REACH + 1) * span]
        else:
            to_graph(near_out.at[rows], near_in.at[core, rows], NEAR, lax.rem(me + o + n, n)).start()
    each_peer(lambda peer: to_graph(base_out.at[peer], base_in.at[core, me], BASE, peer).start())
    base_in[core, pl.ds(me, 1)] = base_out[pl.ds(me, 1)]
    dst_in[pl.ds(me, 1)] = dst_ref[pl.ds(me, 1)]

    EMBED.wait()
    WDEC.wait()
    w_other = wdec_ref[:, pl.ds(pl.multiple_of(other * quarter, quarter), quarter)]
    w_own = wdec_ref[:, pl.ds(pl.multiple_of(core * quarter, quarter), quarter)]
    prj_out[...] = dot(embed_ref[...], w_other)
    send0 = to_core(prj_out, emb_half, PRJ0)
    send0.start()
    WSRC.wait()
    BIAS.wait()
    hot_src = src_live[pl.ds(hot, 1)].astype(jnp.int32) - 1
    msgs = silu(dot(pick_turned(grid_ref[...], hot_src).T.astype(bf), wsrc_ref[...]) + bias_ref[...]).astype(bf)
    emb_own = dot(embed_ref[...], w_own)
    send0.wait_recv()
    emb_out[...] = (emb_own + emb_half[...]).astype(bf).reshape(owners, OWN, quarter)

    wait_in(dst_in.at[pl.ds(0, n - 1)], DST)
    hot_dst = jnp.where(hot_src >= 0, dst_in[hot], -1)
    part_out[...] = dot(spread(mesh_rows, hot_dst), msgs).astype(bf).reshape(owners, OWN, half)

    def send_share(peer):
        @pl.when(peer < owners)
        def _():
            to_graph(part_out.at[peer], part_in.at[me], PART, peer).start()
            to_graph(emb_out.at[peer], emb_in.at[me], EMB, peer).start()

    each_peer(send_share)

    wait_in(base_in.at[core, pl.ds(0, n - 1)], BASE)
    to_core(base_in.at[core], base_in.at[core], FWDB).start()
    wait_in(near_in.at[core, pl.ds(0, 2 * REACH * span)], NEAR)
    to_core(near_in.at[core], near_in.at[core], FWDN).start()
    def share(rows, idx):
        m = silu(dot(rows, wsrc_ref[...]) + bias_ref[...]).astype(bf)
        return dot(spread(mesh_rows, idx), m)

    def half_sum(h):
        total = share(near_in[h], dstx_ref[h, blocks:])
        for j in range(blocks):
            rows = base_in[h, j * (CHUNK // HALF):(j + 1) * (CHUNK // HALF)].reshape(CHUNK, base_in.shape[3])
            total = total + share(rows, dstx_ref[h, j:j + 1])
        return total

    acc[...] = half_sum(core)
    to_core(base_in.at[other], base_in.at[other], FWDB).wait_recv()
    to_core(near_in.at[other], near_in.at[other], FWDN).wait_recv()

    WNODE.wait()
    n_other = wnode_ref[:, pl.ds(pl.multiple_of(other * half, half), half)]
    n_own = wnode_ref[:, pl.ds(pl.multiple_of(core * half, half), half)]
    agg = (acc[...] + half_sum(other)).astype(bf)
    hid_out[...] = dot(agg, n_other)
    send = to_core(hid_out, hid_in, HID)
    send.start()
    own = dot(agg, n_own)
    send0.wait_send()
    send.wait_recv()
    lat = (embed_ref[...].astype(jnp.float32) + silu(own + hid_in[...])).astype(bf)
    prj_out[...] = dot(lat, w_other)
    send2 = to_core(prj_out, prj_in, PRJ)
    send2.start()
    own_p = dot(lat, w_own)

    send2.wait_recv()
    prj_bf[...] = (own_p + prj_in[...]).astype(bf)
    for h in range(2):
        nback_out[h] = pick_turned(prj_bf[...], dstx_ref[h, blocks:]).T.astype(bf)
        nback_in[h, used:, :] = jnp.zeros((NEAR_ROWS - used, quarter), bf)
        for o in range(-REACH, REACH + 1):
            a = (o + REACH) * span
            if o == 0:
                nback_in[h, a:a + span] = nback_out[h, a:a + span]
            else:
                to_graph(nback_out.at[h, pl.ds(a, span)], nback_in.at[h, pl.ds(a, span)], NBACK, lax.rem(me - o + n, n)).start()

    for h in range(2):
        for j in range(blocks):
            rows = pick_turned(prj_bf[...], dstx_ref[h, j:j + 1]).T.astype(bf)
            back_out[h, j * (CHUNK // HALF):(j + 1) * (CHUNK // HALF)] = rows.reshape(CHUNK // HALF, HALF, quarter)
        back_in[h, pl.ds(me, 1)] = back_out[h, pl.ds(me, 1)]
        each_peer(lambda peer, h=h: to_graph(back_out.at[h, peer], back_in.at[h, me], BACK1 if h else BACK, peer).start())

    @pl.when(me < owners)
    def _():
        wait_in(part_in.at[pl.ds(0, n - 1)], PART)
        wait_in(emb_in.at[pl.ds(0, n - 1)], EMB)
        part_in[pl.ds(me, 1)] = part_out[pl.ds(me, 1)]
        emb_in[pl.ds(me, 1)] = emb_out[pl.ds(me, 1)]

    hot_agg = part_in[...].astype(jnp.float32).sum(axis=0).astype(bf)
    hhid_out[...] = dot(hot_agg, n_other)
    send3 = to_core(hhid_out, hhid_in, HIDH)
    send3.start()
    hot_own = dot(hot_agg, n_own)

    send3.wait_recv()
    hot_lat = silu(hot_own + hhid_in[...]).astype(bf)
    hprj_out[...] = dot(hot_lat, w_other)
    send4 = to_core(hprj_out, hprj_in, PRJH)
    send4.start()
    hot_prj = dot(hot_lat, w_own) + emb_in[hot].astype(jnp.float32)
    send4.wait_recv()
    hot_out[...] = (hot_prj + hprj_in[...]).astype(bf)

    @pl.when(me < owners)
    def _():
        each_peer(lambda peer: to_graph(hot_out, hot_in.at[me], HOT, peer).start())

    wait_in(nback_in.at[:, pl.ds(0, 2 * REACH * span)], NBACK)
    total = grid_ref[:, pl.ds(pl.multiple_of(core * quarter, quarter), quarter)].astype(jnp.float32)
    for h in range(2):
        total = total + dot(spread(grid_rows, srcx_ref[h, blocks:]), nback_in[h])
    dec[...] = total
    for h in range(2):
        wait_in(back_in.at[h, pl.ds(0, n - 1)], BACK1 if h else BACK)
        total = dec[...]
        for j in range(blocks):
            rows = back_in[h, j * (CHUNK // HALF):(j + 1) * (CHUNK // HALF)].reshape(CHUNK, quarter)
            total = total + dot(spread(grid_rows, srcx_ref[h, j:j + 1]), rows)
        dec[...] = total

    @pl.when(me < owners)
    def _():
        wait_in(hot_in.at[pl.ds(0, owners - 1)], HOT)
        hot_in[pl.ds(me, 1)] = hot_out[...].reshape(1, OWN, quarter)

    @pl.when(me >= owners)
    def _():
        wait_in(hot_in, HOT)

    hot_rows = pick_turned(hot_in[...].reshape(mesh_rows, quarter), hot_dst).astype(bf)
    back = lax.dot_general(spread(grid_rows, hot_src), hot_rows, (((1,), (1,)), ((), ())), preferred_element_type=jnp.float32)
    out_ref[...] = (dec[...] + back).astype(bf)

    wait_out(dst_ref.at[pl.ds(0, n - 1)], DST)
    wait_out(base_out.at[pl.ds(0, n - 1)], BASE)
    wait_out(near_out.at[pl.ds(0, 2 * REACH * span)], NEAR)

    @pl.when(me < owners)
    def _():
        wait_out(emb_out.at[pl.ds(0, owners - 1)], EMB)
        wait_out(part_out.at[pl.ds(0, owners - 1)], PART)
        wait_out(back_out.at[0, pl.ds(0, n - 1)], HOT)

    @pl.when(me >= owners)
    def _():
        wait_out(emb_out, EMB)
        wait_out(part_out, PART)

    to_core(base_in.at[core], base_in.at[core], FWDB).wait_send()
    to_core(near_in.at[core], near_in.at[core], FWDN).wait_send()
    for copy in (send, send2, send3, send4):
        copy.wait_send()
    for h in range(2):
        wait_out(back_out.at[h, pl.ds(0, n - 1)], BACK1 if h else BACK)
    wait_out(nback_out.at[:, pl.ds(0, 2 * REACH * span)], NBACK)


def cap_near(capacity):
    return (capacity - KEEP) // 2


def lay_out(table, take, mark):
    high = jnp.floor(table * (1.0 / 32.0))
    low = table - 32.0 * high
    dot = functools.partial(jnp.dot, preferred_element_type=jnp.float32)
    moved = 32.0 * dot(high.astype(jnp.bfloat16), take) + dot(low.astype(jnp.bfloat16), take)
    group = mark.shape[0]
    moved = moved.reshape(table.shape[0] // group, group, take.shape[1])
    return (moved * mark[None]).sum(axis=1).astype(jnp.int32) - 1


def base_layout(capacity, h):
    shape = (capacity, CHUNK)
    lane = lax.broadcasted_iota(jnp.int32, shape, 1)
    slot = lax.broadcasted_iota(jnp.int32, shape, 0)
    take = jnp.where(slot == h * HALF + (lane & (HALF - 1)), 1.0, 0.0).astype(jnp.bfloat16)
    group = CHUNK // HALF
    lane = lax.broadcasted_iota(jnp.int32, (group, CHUNK), 1)
    row = lax.broadcasted_iota(jnp.int32, (group, CHUNK), 0)
    return take, jnp.where(row * HALF <= lane, 1.0, 0.0) * jnp.where(lane < row * HALF + HALF, 1.0, 0.0)


def near_layout(capacity, h):
    span = cap_near(capacity)
    count = 2 * REACH + 1
    shape = (capacity, NEAR_ROWS)
    lane = lax.broadcasted_iota(jnp.int32, shape, 1)
    slot = lax.broadcasted_iota(jnp.int32, shape, 0)
    within = lane
    for i in range(1, count + 1):
        within = within - jnp.where(lane >= i * span, span, 0)
    take = jnp.where(slot == KEEP + h * span + within, 1.0, 0.0).astype(jnp.bfloat16)
    lane = lax.broadcasted_iota(jnp.int32, (8, NEAR_ROWS), 1)
    row = lax.broadcasted_iota(jnp.int32, (8, NEAR_ROWS), 0)
    inside = jnp.where(row * span <= lane, 1.0, 0.0) * jnp.where(lane < row * span + span, 1.0, 0.0)
    return take, inside * jnp.where(row < count, 1.0, 0.0)


def compact(hot, grid_state, w_src, bias_src, mesh_embed, w_node, w_dec, slot_src, slot_dst, slot_count):
    n = lax.axis_size("graph")
    capacity = slot_src.shape[2]
    grid_rows, width = grid_state.shape
    mesh_rows, half = mesh_embed.shape
    quarter = width // 2
    owners = mesh_rows // OWN
    bf, f32 = jnp.bfloat16, jnp.float32
    vm = pltpu.VMEM
    return pl.pallas_call(
        functools.partial(step_kernel, n),
        out_shape=jax.ShapeDtypeStruct((grid_rows, quarter), bf),
        in_specs=[pl.BlockSpec(memory_space=pltpu.SMEM)] + [pl.BlockSpec(memory_space=pl.ANY)] * 9,
        out_specs=pl.BlockSpec(memory_space=vm),
        scratch_shapes=[
            vm((grid_rows, width), bf), vm(w_src.shape, bf), vm((1, half), f32), vm((mesh_rows, half), bf), vm(w_node.shape, bf),
            vm(w_dec.shape, bf), vm(slot_src.shape, jnp.int32), vm(slot_dst.shape, jnp.int32), vm(slot_count.shape, jnp.int32),
            vm((n, capacity), f32), vm((n, capacity), f32),
            vm((2, n * HALF // CHUNK + 1, CHUNK), jnp.int32), vm((2, n * HALF // CHUNK + 1, CHUNK), jnp.int32),
            vm((n, HALF, width), bf), vm((NEAR_ROWS, width), bf),
            vm((2, n, HALF, width), bf), vm((2, NEAR_ROWS, width), bf),
            vm((n, 1, capacity), jnp.int32), vm((n, OWN, quarter), bf), vm((owners, OWN, quarter), bf), vm((mesh_rows, quarter), f32),
            vm((owners, OWN, half), bf), vm((n, OWN, half), bf),
            vm((mesh_rows, half), f32),
            vm((mesh_rows, half), f32), vm((mesh_rows, half), f32),
            vm((mesh_rows, quarter), f32), vm((mesh_rows, quarter), f32), vm((mesh_rows, quarter), bf),
            vm((2, n, HALF, quarter), bf), vm((2, NEAR_ROWS, quarter), bf),
            vm((2, n, HALF, quarter), bf), vm((2, NEAR_ROWS, quarter), bf),
            vm((OWN, quarter), bf), vm((owners, OWN, quarter), bf),
            vm((grid_rows, quarter), f32),
            vm((OWN, half), f32), vm((OWN, half), f32), vm((OWN, quarter), f32), vm((OWN, quarter), f32),
            pltpu.SemaphoreType.DMA((9,)), pltpu.SemaphoreType.DMA((SEMS,)), pltpu.SemaphoreType.DMA((SEMS,)),
        ],
        compiler_params=pltpu.CompilerParams(collective_id=0, has_side_effects=True, vmem_limit_bytes=48 * 1024 * 1024),
    )(hot, grid_state, w_src, bias_src[None, :], mesh_embed, w_node, w_dec, slot_src, slot_dst, slot_count)


def on_device(grid_state, w_src, bias_src, mesh_embed, w_node, w_dec, slot_src, slot_dst, slot_count):
    args = (grid_state, w_src, bias_src, mesh_embed, w_node, w_dec, slot_src, slot_dst, slot_count)
    n = slot_count.shape[0]
    apart = jnp.abs(jnp.arange(n)[:, None] - jnp.arange(n)[None, :])
    far = jnp.minimum(apart, n - apart) > REACH
    over = far & (slot_count > KEEP)
    column = jnp.broadcast_to(jnp.arange(n, dtype=jnp.int32)[None, :], (n, n))
    last = jnp.max(jnp.where(over, column, 0))
    first = jnp.min(jnp.where(over, column, n))
    fits = last <= first
    hot = last.reshape(1)
    return lax.cond(fits, lambda: compact(hot, *args), lambda: dense(*args))


def solution(mesh):
    placed = (
        P(("member", "graph"), None),
        P(None, "chan"),
        P("chan"),
        P("graph", "chan"),
        P("chan", None),
        P("chan", None),
        P("graph", None, None),
        P(None, "graph", None),
        P(),
    )
    return jax.shard_map(
        on_device,
        mesh=mesh,
        in_specs=placed,
        out_specs=P(("member", "graph"), "chan"),
        check_vma=False,
    )
```

```python
import functools
import math

import jax
import jax.numpy as jnp
from jax import lax
from jax.experimental import pallas as pl
from jax.experimental.pallas import tpu as pltpu
from jax.sharding import PartitionSpec as P

MESH_ID = pl.DeviceIdType.MESH
KEEP = 32
HALF = KEEP // 2
GROUP = 7
SEMS = 16
REACH = 2
OWN = 16
NEAR_ROWS = 256
CHUNK = 256

def split_up(value, dim, count):
    lengths = value.shape
    parts = value.reshape(*lengths[:dim], count, lengths[dim] // count, *lengths[dim + 1 :])
    return jnp.moveaxis(parts, dim, 0)


def sum_at_owner(value, axis, dim):
    parts = split_up(value, dim, lax.axis_size(axis))
    arrived = lax.all_to_all(parts, axis, split_axis=0, concat_axis=0, tiled=True)
    return arrived.sum(axis=0)


def edge_network(source_rows, w_src, bias_src):
    return jax.nn.silu(
        jnp.dot(source_rows, w_src, preferred_element_type=jnp.float32) + bias_src
    ).astype(jnp.bfloat16)


def segment_rows(values, indices, usable, row_count):
    slot_total = values.shape[0]
    width = values.shape[1]
    block_len = math.gcd(slot_total, 2048)
    block_count = slot_total // block_len
    targets = jnp.where(usable, indices, -1).reshape(block_count, block_len)
    pieces = values.reshape(block_count, block_len, width)
    row_ids = jnp.arange(row_count, dtype=jnp.int32)

    def add_block(summed, scan_item):
        row_target, piece_vals = scan_item
        one_hot = (row_ids[:, None] == row_target[None, :]).astype(jnp.bfloat16)
        return (summed + jnp.dot(one_hot, piece_vals, preferred_element_type=jnp.float32), None)

    result, unused = lax.scan(
        add_block, jnp.zeros((row_count, width), jnp.float32), (targets, pieces)
    )
    return result


def dense(
    grid_state, w_src, bias_src, mesh_embed, w_node, w_dec, slot_src, slot_dst, slot_count
):
    peers = lax.axis_size("graph")
    own_index = lax.axis_index("graph")
    core_index = lax.axis_index("chan")
    capacity = slot_src.shape[2]
    positions = jnp.arange(capacity, dtype=jnp.int32)
    grid_rows = grid_state.shape[0]
    mesh_rows = mesh_embed.shape[0]
    sent_counts = lax.dynamic_slice_in_dim(slot_count, own_index, 1, 0)[0]
    recv_counts = lax.dynamic_slice_in_dim(slot_count, own_index, 1, 1)[:, 0]
    half_slots = capacity // 2
    chosen = lax.dynamic_slice_in_dim(slot_src[0], core_index * half_slots, half_slots, 1)
    picked = jnp.take(grid_state, chosen.reshape(-1), axis=0).reshape(
        peers, half_slots, grid_state.shape[1]
    )
    arrived = lax.all_to_all(picked, "graph", split_axis=0, concat_axis=0, tiled=True)
    partner = lax.ppermute(arrived, "chan", [(0, 1), (1, 0)])
    joined = jnp.where(
        core_index == 0,
        jnp.concatenate([arrived, partner], axis=1),
        jnp.concatenate([partner, arrived], axis=1),
    )
    messages = edge_network(joined.reshape(peers * capacity, grid_state.shape[1]), w_src, bias_src)
    arrive_ok = (positions[None, :] < recv_counts[:, None]).reshape(-1)
    dst_rows = slot_dst[:, 0, :].reshape(-1)
    aggregate = segment_rows(messages, dst_rows, arrive_ok, mesh_rows)
    partial_hidden = jnp.dot(
        aggregate.astype(jnp.bfloat16), w_node, preferred_element_type=jnp.float32
    )
    hidden_pre = sum_at_owner(partial_hidden, "chan", 1)
    latent = (mesh_embed.astype(jnp.float32) + jax.nn.silu(hidden_pre)).astype(jnp.bfloat16)
    partial_proj = jnp.dot(latent, w_dec, preferred_element_type=jnp.float32)
    projected = sum_at_owner(partial_proj, "chan", 1).astype(jnp.bfloat16)
    returned = jnp.take(projected, dst_rows, axis=0).reshape(peers, capacity, projected.shape[1])
    came_back = lax.all_to_all(returned, "graph", split_axis=0, concat_axis=0, tiled=True).reshape(
        peers * capacity, projected.shape[1]
    )
    send_ok = (positions[None, :] < sent_counts[:, None]).reshape(-1)
    decoded = segment_rows(came_back, slot_src[0].reshape(-1), send_ok, grid_rows)
    width_half = decoded.shape[1]
    own_cols = lax.dynamic_slice_in_dim(grid_state, core_index * width_half, width_half, 1)
    return (own_cols.astype(jnp.float32) + decoded).astype(jnp.bfloat16)


def torus(n):
    wide = 1 << (n.bit_length() // 2)
    return n // wide, wide


def visit_order(n):
    tall, wide = torus(n)
    offsets = [(r, c) for r in range(tall) for c in range(wide)][1:]
    offsets.sort(key=lambda o: min(o[0], tall - o[0]) + min(o[1], wide - o[1]))
    return [offsets[i // 2] if i % 2 == 0 else offsets[-1 - i // 2] for i in range(n - 1)]


def silu(v):
    h = 0.5 * v
    return h + h * jnp.tanh(h)


def pick_turned(table, idx):
    rows = table.shape[0]
    hot = jnp.where(
        lax.broadcasted_iota(jnp.int32, (rows, idx.shape[1]), 0) == idx, 1.0, 0.0
    ).astype(jnp.bfloat16)
    return lax.dot_general(table, hot, (((0,), (0,)), ((), ())), preferred_element_type=jnp.float32)


def spread(rows, idx):
    return jnp.where(
        lax.broadcasted_iota(jnp.int32, (rows, idx.shape[1]), 0) == idx, 1.0, 0.0
    ).astype(jnp.bfloat16)


def step_kernel(
    n, hot_ref, grid_hbm, wsrc_hbm, bias_hbm, embed_hbm, wnode_hbm, wdec_hbm, src_hbm, dst_hbm, count_hbm, out_ref,
    grid_ref, wsrc_ref, bias_ref, embed_ref, wnode_ref, wdec_ref, src_ref, dst_ref, count_ref,
    src_live, dst_live, srcx_ref, dstx_ref,
    base_out, near_out, base_in, near_in, dst_in, emb_in, emb_out, emb_half, part_out, part_in,
    acc, hid_out, hid_in, prj_out, prj_in, prj_bf, back_out, nback_out, back_in, nback_in, hot_out, hot_in, dec,
    hhid_out, hhid_in, hprj_out, hprj_in,
    lsem, ssem, rsem,
):
    me = lax.axis_index("graph")
    core = lax.axis_index("chan")
    other = 1 - core
    grid_rows = grid_ref.shape[0]
    mesh_rows = embed_ref.shape[0]
    owners = mesh_rows // OWN
    span = cap_near(dst_ref.shape[2])
    used = (2 * REACH + 1) * span
    half = hid_out.shape[1]
    quarter = prj_out.shape[1]
    bf = jnp.bfloat16
    dot = functools.partial(jnp.dot, preferred_element_type=jnp.float32)

    pairs = (
        (src_hbm, src_ref), (dst_hbm, dst_ref), (count_hbm, count_ref), (grid_hbm, grid_ref), (embed_hbm, embed_ref),
        (wdec_hbm, wdec_ref), (wsrc_hbm, wsrc_ref), (bias_hbm, bias_ref), (wnode_hbm, wnode_ref),
    )
    SRC, DSTS, COUNT, GRID, EMBED, WDEC, WSRC, BIAS, WNODE = (
        pltpu.make_async_copy(x, y, lsem.at[i]) for i, (x, y) in enumerate(pairs))
    for copy in (SRC, DSTS, COUNT, GRID, EMBED, WDEC, WSRC, BIAS, WNODE):
        copy.start()

    tall, wide = torus(n)
    codes = [r * 2 * wide + c for r, c in visit_order(n)]
    groups = [codes[i:i + GROUP] for i in range(0, n - 1, GROUP)]
    spot = 2 * wide * (me // wide) + lax.rem(me, wide) + core * (2 * wide * tall + wide)
    turn = 1 - 2 * core

    def each_peer(visit):
        @pl.loop(0, len(groups))
        def _(g):
            for part in (range(0, 4), range(4, GROUP)):
                packed = jnp.int32(0)
                for i, group in enumerate(groups):
                    packed = jnp.where(g == i, sum(group[k] << (7 * j) for j, k in enumerate(part)), packed)
                for j in range(len(part)):
                    code = lax.shift_right_logical(packed, jnp.int32(7 * j)) & 127
                    at = spot + turn * code
                    visit((lax.shift_right_logical(at, jnp.int32(1)) & ((tall - 1) * wide)) + (at & (wide - 1)))

    barrier = pltpu.get_barrier_semaphore()
    each_peer(lambda peer: pl.semaphore_signal(barrier, inc=1, device_id={"graph": peer}, device_id_type=MESH_ID))
    pl.semaphore_signal(barrier, inc=1, device_id={"chan": other}, device_id_type=MESH_ID)

    def to_graph(src, dst, k, peer):
        return pltpu.make_async_remote_copy(
            src_ref=src, dst_ref=dst, send_sem=ssem.at[k], recv_sem=rsem.at[k],
            device_id={"graph": peer}, device_id_type=MESH_ID)

    def to_core(src, dst, k):
        return pltpu.make_async_remote_copy(
            src_ref=src, dst_ref=dst, send_sem=ssem.at[k], recv_sem=rsem.at[k],
            device_id={"chan": other}, device_id_type=MESH_ID)

    def wait_in(ref, k):
        to_graph(ref, ref, k, me).wait_recv()

    def wait_out(ref, k):
        to_graph(ref, ref, k, me).wait_send()

    DST, EMB, BASE, NEAR, PART, FWDB, FWDN, HID, PRJ, BACK, NBACK, HOT, PRJ0, BACK1, HIDH, PRJH = range(SEMS)

    blocks = (n * HALF) // CHUNK
    capacity = dst_ref.shape[2]
    SRC.wait()
    DSTS.wait()
    COUNT.wait()
    with jax.named_scope("index"):
        hot = hot_ref[0]
        ids = lax.broadcasted_iota(jnp.int32, (n, n), 0)
        cols = lax.broadcasted_iota(jnp.int32, (n, n), 1)
        counts = count_ref[...]
        sent = jnp.where(ids == me, counts, 0).sum(axis=0, keepdims=True)
        sent = jnp.where(ids == cols, sent, 0).sum(axis=1, keepdims=True)
        came = jnp.where(cols == me, counts, 0).sum(axis=1, keepdims=True)
        pos = lax.broadcasted_iota(jnp.int32, (n, capacity), 1)
        src_all = jnp.where(pos < sent, src_ref[0] + 1, 0).astype(jnp.float32)
        src_live[...] = src_all
        came = jnp.where(me == hot, 0, came)
        dst_all = jnp.where(pos < came, dst_ref[:, 0, :] + 1, 0).astype(jnp.float32)
        dst_live[...] = dst_all
        rows_id = lax.broadcasted_iota(jnp.int32, (n, capacity), 0)
        src_all = jnp.where(rows_id == hot, 0.0, src_all)
        near_id = lax.broadcasted_iota(jnp.int32, (8, capacity), 0)
        near_src = jnp.zeros((8, capacity), jnp.float32)
        near_dst = jnp.zeros((8, capacity), jnp.float32)
        for o in range(-REACH, REACH + 1):
            to = lax.rem(me + o + n, n)
            row = jnp.where(to == hot, 0.0, src_live[pl.ds(to, 1)])
            near_src = jnp.where(near_id == o + REACH, row, near_src)
            near_dst = jnp.where(near_id == o + REACH, dst_live[pl.ds(lax.rem(me - o + n, n), 1)], near_dst)
        for h in range(2):
            base = base_layout(capacity, h)
            srcx_ref[h, 0:blocks] = lay_out(src_all, *base)
            dstx_ref[h, 0:blocks] = lay_out(dst_all, *base)
            near = near_layout(capacity, h)
            srcx_ref[h, blocks:] = lay_out(near_src, *near)[:, 0:CHUNK]
            dstx_ref[h, blocks:] = lay_out(near_dst, *near)[:, 0:CHUNK]

    GRID.wait()

    for j in range(blocks):
        rows = pick_turned(grid_ref[...], srcx_ref[core, j:j + 1]).T.astype(bf)
        base_out[j * (CHUNK // HALF):(j + 1) * (CHUNK // HALF)] = rows.reshape(CHUNK // HALF, HALF, rows.shape[1])

    near_out[...] = pick_turned(grid_ref[...], srcx_ref[core, blocks:]).T.astype(bf)
    near_in[core, used:, :] = jnp.zeros((NEAR_ROWS - used, near_in.shape[2]), bf)

    pl.semaphore_wait(barrier, n)
    each_peer(lambda peer: to_graph(dst_ref.at[peer], dst_in.at[me], DST, peer).start())
    for o in range(-REACH, REACH + 1):
        rows = pl.ds((o + REACH) * span, span)
        if o == 0:
            near_in[core, (o + REACH) * span:(o + REACH + 1) * span] = near_out[(o + REACH) * span:(o + REACH + 1) * span]
        else:
            to_graph(near_out.at[rows], near_in.at[core, rows], NEAR, lax.rem(me + o + n, n)).start()
    each_peer(lambda peer: to_graph(base_out.at[peer], base_in.at[core, me], BASE, peer).start())
    base_in[core, pl.ds(me, 1)] = base_out[pl.ds(me, 1)]
    dst_in[pl.ds(me, 1)] = dst_ref[pl.ds(me, 1)]

    EMBED.wait()
    WDEC.wait()
    w_other = wdec_ref[:, pl.ds(pl.multiple_of(other * quarter, quarter), quarter)]
    w_own = wdec_ref[:, pl.ds(pl.multiple_of(core * quarter, quarter), quarter)]
    prj_out[...] = dot(embed_ref[...], w_other)
    send0 = to_core(prj_out, emb_half, PRJ0)
    send0.start()
    WSRC.wait()
    BIAS.wait()
    hot_src = src_live[pl.ds(hot, 1)].astype(jnp.int32) - 1
    msgs = silu(dot(pick_turned(grid_ref[...], hot_src).T.astype(bf), wsrc_ref[...]) + bias_ref[...]).astype(bf)
    emb_own = dot(embed_ref[...], w_own)
    send0.wait_recv()
    emb_out[...] = (emb_own + emb_half[...]).astype(bf).reshape(owners, OWN, quarter)

    wait_in(dst_in.at[pl.ds(0, n - 1)], DST)
    hot_dst = jnp.where(hot_src >= 0, dst_in[hot], -1)
    part_out[...] = dot(spread(mesh_rows, hot_dst), msgs).astype(bf).reshape(owners, OWN, half)

    def to_owner(copy_to):
        def visit(peer):
            @pl.when(peer < owners)
            def _():
                copy_to(peer).start()
        return visit

    each_peer(to_owner(lambda peer: to_graph(part_out.at[peer], part_in.at[me], PART, peer)))
    each_peer(to_owner(lambda peer: to_graph(emb_out.at[peer], emb_in.at[me], EMB, peer)))

    wait_in(base_in.at[core, pl.ds(0, n - 1)], BASE)
    to_core(base_in.at[core], base_in.at[core], FWDB).start()
    wait_in(near_in.at[core, pl.ds(0, 2 * REACH * span)], NEAR)
    to_core(near_in.at[core], near_in.at[core], FWDN).start()
    def share(rows, idx):
        m = silu(dot(rows, wsrc_ref[...]) + bias_ref[...]).astype(bf)
        return dot(spread(mesh_rows, idx), m)

    def half_sum(h):
        total = share(near_in[h], dstx_ref[h, blocks:])
        for j in range(blocks):
            rows = base_in[h, j * (CHUNK // HALF):(j + 1) * (CHUNK // HALF)].reshape(CHUNK, base_in.shape[3])
            total = total + share(rows, dstx_ref[h, j:j + 1])
        return total

    acc[...] = half_sum(core)
    to_core(base_in.at[other], base_in.at[other], FWDB).wait_recv()
    to_core(near_in.at[other], near_in.at[other], FWDN).wait_recv()

    WNODE.wait()
    n_other = wnode_ref[:, pl.ds(pl.multiple_of(other * half, half), half)]
    n_own = wnode_ref[:, pl.ds(pl.multiple_of(core * half, half), half)]
    agg = (acc[...] + half_sum(other)).astype(bf)
    hid_out[...] = dot(agg, n_other)
    send = to_core(hid_out, hid_in, HID)
    send.start()
    own = dot(agg, n_own)
    send0.wait_send()
    send.wait_recv()
    lat = (embed_ref[...].astype(jnp.float32) + silu(own + hid_in[...])).astype(bf)
    prj_out[...] = dot(lat, w_other)
    send2 = to_core(prj_out, prj_in, PRJ)
    send2.start()
    own_p = dot(lat, w_own)

    send2.wait_recv()
    prj_bf[...] = (own_p + prj_in[...]).astype(bf)
    for h in range(2):
        nback_out[h] = pick_turned(prj_bf[...], dstx_ref[h, blocks:]).T.astype(bf)
        nback_in[h, used:, :] = jnp.zeros((NEAR_ROWS - used, quarter), bf)
        for o in range(-REACH, REACH + 1):
            a = (o + REACH) * span
            if o == 0:
                nback_in[h, a:a + span] = nback_out[h, a:a + span]
            else:
                to_graph(nback_out.at[h, pl.ds(a, span)], nback_in.at[h, pl.ds(a, span)], NBACK, lax.rem(me - o + n, n)).start()

    for h in range(2):
        for j in range(blocks):
            rows = pick_turned(prj_bf[...], dstx_ref[h, j:j + 1]).T.astype(bf)
            back_out[h, j * (CHUNK // HALF):(j + 1) * (CHUNK // HALF)] = rows.reshape(CHUNK // HALF, HALF, quarter)
        back_in[h, pl.ds(me, 1)] = back_out[h, pl.ds(me, 1)]
        if h == 0:
            each_peer(lambda peer: to_graph(back_out.at[0, peer], back_in.at[0, me], BACK, peer).start())

    @pl.when(me < owners)
    def _():
        wait_in(part_in.at[pl.ds(0, n - 1)], PART)
        part_in[pl.ds(me, 1)] = part_out[pl.ds(me, 1)]

    hot_agg = part_in[...].astype(jnp.float32).sum(axis=0).astype(bf)
    hhid_out[...] = dot(hot_agg, n_other)
    send3 = to_core(hhid_out, hhid_in, HIDH)
    send3.start()
    hot_own = dot(hot_agg, n_own)

    send3.wait_recv()
    hot_lat = silu(hot_own + hhid_in[...]).astype(bf)
    hprj_out[...] = dot(hot_lat, w_other)
    send4 = to_core(hprj_out, hprj_in, PRJH)
    send4.start()
    hot_prj = dot(hot_lat, w_own)

    @pl.when(me < owners)
    def _():
        wait_in(emb_in.at[pl.ds(0, n - 1)], EMB)
        emb_in[pl.ds(me, 1)] = emb_out[pl.ds(me, 1)]

    send4.wait_recv()
    hot_out[...] = (hot_prj + hprj_in[...] + emb_in[hot].astype(jnp.float32)).astype(bf)

    def send_rest(peer):
        @pl.when(me < owners)
        def _():
            to_graph(hot_out, hot_in.at[me], HOT, peer).start()

        to_graph(back_out.at[1, peer], back_in.at[1, me], BACK1, peer).start()

    each_peer(send_rest)

    wait_in(nback_in.at[:, pl.ds(0, 2 * REACH * span)], NBACK)
    total = grid_ref[:, pl.ds(pl.multiple_of(core * quarter, quarter), quarter)].astype(jnp.float32)
    for h in range(2):
        total = total + dot(spread(grid_rows, srcx_ref[h, blocks:]), nback_in[h])
    dec[...] = total
    for h in range(2):
        wait_in(back_in.at[h, pl.ds(0, n - 1)], BACK1 if h else BACK)
        total = dec[...]
        for j in range(blocks):
            rows = back_in[h, j * (CHUNK // HALF):(j + 1) * (CHUNK // HALF)].reshape(CHUNK, quarter)
            total = total + dot(spread(grid_rows, srcx_ref[h, j:j + 1]), rows)
        dec[...] = total

    @pl.when(me < owners)
    def _():
        wait_in(hot_in.at[pl.ds(0, owners - 1)], HOT)
        hot_in[pl.ds(me, 1)] = hot_out[...].reshape(1, OWN, quarter)

    @pl.when(me >= owners)
    def _():
        wait_in(hot_in, HOT)

    hot_rows = pick_turned(hot_in[...].reshape(mesh_rows, quarter), hot_dst).astype(bf)
    back = lax.dot_general(spread(grid_rows, hot_src), hot_rows, (((1,), (1,)), ((), ())), preferred_element_type=jnp.float32)
    out_ref[...] = (dec[...] + back).astype(bf)

    wait_out(dst_ref.at[pl.ds(0, n - 1)], DST)
    wait_out(base_out.at[pl.ds(0, n - 1)], BASE)
    wait_out(near_out.at[pl.ds(0, 2 * REACH * span)], NEAR)

    @pl.when(me < owners)
    def _():
        wait_out(emb_out.at[pl.ds(0, owners - 1)], EMB)
        wait_out(part_out.at[pl.ds(0, owners - 1)], PART)
        wait_out(back_out.at[0, pl.ds(0, n - 1)], HOT)

    @pl.when(me >= owners)
    def _():
        wait_out(emb_out, EMB)
        wait_out(part_out, PART)

    to_core(base_in.at[core], base_in.at[core], FWDB).wait_send()
    to_core(near_in.at[core], near_in.at[core], FWDN).wait_send()
    for copy in (send, send2, send3, send4):
        copy.wait_send()
    for h in range(2):
        wait_out(back_out.at[h, pl.ds(0, n - 1)], BACK1 if h else BACK)
    wait_out(nback_out.at[:, pl.ds(0, 2 * REACH * span)], NBACK)


def cap_near(capacity):
    return (capacity - KEEP) // 2


def lay_out(table, take, mark):
    high = jnp.floor(table * (1.0 / 32.0))
    low = table - 32.0 * high
    dot = functools.partial(jnp.dot, preferred_element_type=jnp.float32)
    moved = 32.0 * dot(high.astype(jnp.bfloat16), take) + dot(low.astype(jnp.bfloat16), take)
    group = mark.shape[0]
    moved = moved.reshape(table.shape[0] // group, group, take.shape[1])
    return (moved * mark[None]).sum(axis=1).astype(jnp.int32) - 1


def base_layout(capacity, h):
    shape = (capacity, CHUNK)
    lane = lax.broadcasted_iota(jnp.int32, shape, 1)
    slot = lax.broadcasted_iota(jnp.int32, shape, 0)
    take = jnp.where(slot == h * HALF + (lane & (HALF - 1)), 1.0, 0.0).astype(jnp.bfloat16)
    group = CHUNK // HALF
    lane = lax.broadcasted_iota(jnp.int32, (group, CHUNK), 1)
    row = lax.broadcasted_iota(jnp.int32, (group, CHUNK), 0)
    return take, jnp.where(row * HALF <= lane, 1.0, 0.0) * jnp.where(lane < row * HALF + HALF, 1.0, 0.0)


def near_layout(capacity, h):
    span = cap_near(capacity)
    count = 2 * REACH + 1
    shape = (capacity, NEAR_ROWS)
    lane = lax.broadcasted_iota(jnp.int32, shape, 1)
    slot = lax.broadcasted_iota(jnp.int32, shape, 0)
    within = lane
    for i in range(1, count + 1):
        within = within - jnp.where(lane >= i * span, span, 0)
    take = jnp.where(slot == KEEP + h * span + within, 1.0, 0.0).astype(jnp.bfloat16)
    lane = lax.broadcasted_iota(jnp.int32, (8, NEAR_ROWS), 1)
    row = lax.broadcasted_iota(jnp.int32, (8, NEAR_ROWS), 0)
    inside = jnp.where(row * span <= lane, 1.0, 0.0) * jnp.where(lane < row * span + span, 1.0, 0.0)
    return take, inside * jnp.where(row < count, 1.0, 0.0)


def compact(hot, grid_state, w_src, bias_src, mesh_embed, w_node, w_dec, slot_src, slot_dst, slot_count):
    n = lax.axis_size("graph")
    capacity = slot_src.shape[2]
    grid_rows, width = grid_state.shape
    mesh_rows, half = mesh_embed.shape
    quarter = width // 2
    owners = mesh_rows // OWN
    bf, f32 = jnp.bfloat16, jnp.float32
    vm = pltpu.VMEM
    return pl.pallas_call(
        functools.partial(step_kernel, n),
        out_shape=jax.ShapeDtypeStruct((grid_rows, quarter), bf),
        in_specs=[pl.BlockSpec(memory_space=pltpu.SMEM)] + [pl.BlockSpec(memory_space=pl.ANY)] * 9,
        out_specs=pl.BlockSpec(memory_space=vm),
        scratch_shapes=[
            vm((grid_rows, width), bf), vm(w_src.shape, bf), vm((1, half), f32), vm((mesh_rows, half), bf), vm(w_node.shape, bf),
            vm(w_dec.shape, bf), vm(slot_src.shape, jnp.int32), vm(slot_dst.shape, jnp.int32), vm(slot_count.shape, jnp.int32),
            vm((n, capacity), f32), vm((n, capacity), f32),
            vm((2, n * HALF // CHUNK + 1, CHUNK), jnp.int32), vm((2, n * HALF // CHUNK + 1, CHUNK), jnp.int32),
            vm((n, HALF, width), bf), vm((NEAR_ROWS, width), bf),
            vm((2, n, HALF, width), bf), vm((2, NEAR_ROWS, width), bf),
            vm((n, 1, capacity), jnp.int32), vm((n, OWN, quarter), bf), vm((owners, OWN, quarter), bf), vm((mesh_rows, quarter), f32),
            vm((owners, OWN, half), bf), vm((n, OWN, half), bf),
            vm((mesh_rows, half), f32),
            vm((mesh_rows, half), f32), vm((mesh_rows, half), f32),
            vm((mesh_rows, quarter), f32), vm((mesh_rows, quarter), f32), vm((mesh_rows, quarter), bf),
            vm((2, n, HALF, quarter), bf), vm((2, NEAR_ROWS, quarter), bf),
            vm((2, n, HALF, quarter), bf), vm((2, NEAR_ROWS, quarter), bf),
            vm((OWN, quarter), bf), vm((owners, OWN, quarter), bf),
            vm((grid_rows, quarter), f32),
            vm((OWN, half), f32), vm((OWN, half), f32), vm((OWN, quarter), f32), vm((OWN, quarter), f32),
            pltpu.SemaphoreType.DMA((9,)), pltpu.SemaphoreType.DMA((SEMS,)), pltpu.SemaphoreType.DMA((SEMS,)),
        ],
        compiler_params=pltpu.CompilerParams(collective_id=0, has_side_effects=True, vmem_limit_bytes=48 * 1024 * 1024),
    )(hot, grid_state, w_src, bias_src[None, :], mesh_embed, w_node, w_dec, slot_src, slot_dst, slot_count)


def on_device(grid_state, w_src, bias_src, mesh_embed, w_node, w_dec, slot_src, slot_dst, slot_count):
    args = (grid_state, w_src, bias_src, mesh_embed, w_node, w_dec, slot_src, slot_dst, slot_count)
    n = slot_count.shape[0]
    apart = jnp.abs(jnp.arange(n)[:, None] - jnp.arange(n)[None, :])
    far = jnp.minimum(apart, n - apart) > REACH
    over = far & (slot_count > KEEP)
    column = jnp.broadcast_to(jnp.arange(n, dtype=jnp.int32)[None, :], (n, n))
    last = jnp.max(jnp.where(over, column, 0))
    first = jnp.min(jnp.where(over, column, n))
    fits = last <= first
    hot = last.reshape(1)
    return lax.cond(fits, lambda: compact(hot, *args), lambda: dense(*args))


def solution(mesh):
    placed = (
        P(("member", "graph"), None),
        P(None, "chan"),
        P("chan"),
        P("graph", "chan"),
        P("chan", None),
        P("chan", None),
        P("graph", None, None),
        P(None, "graph", None),
        P(),
    )
    return jax.shard_map(
        on_device,
        mesh=mesh,
        in_specs=placed,
        out_specs=P(("member", "graph"), "chan"),
        check_vma=False,
    )
```

```python
import functools
import math

import jax
import jax.numpy as jnp
from jax import lax
from jax.experimental import pallas as pl
from jax.experimental.pallas import tpu as pltpu
from jax.sharding import PartitionSpec as P

MESH_ID = pl.DeviceIdType.MESH
KEEP = 32
HALF = KEEP // 2
GROUP = 7
SEMS = 16
REACH = 2
OWN = 16
NEAR_ROWS = 256
CHUNK = 256

def split_up(value, dim, count):
    lengths = value.shape
    parts = value.reshape(*lengths[:dim], count, lengths[dim] // count, *lengths[dim + 1 :])
    return jnp.moveaxis(parts, dim, 0)


def sum_at_owner(value, axis, dim):
    parts = split_up(value, dim, lax.axis_size(axis))
    arrived = lax.all_to_all(parts, axis, split_axis=0, concat_axis=0, tiled=True)
    return arrived.sum(axis=0)


def edge_network(source_rows, w_src, bias_src):
    return jax.nn.silu(
        jnp.dot(source_rows, w_src, preferred_element_type=jnp.float32) + bias_src
    ).astype(jnp.bfloat16)


def segment_rows(values, indices, usable, row_count):
    slot_total = values.shape[0]
    width = values.shape[1]
    block_len = math.gcd(slot_total, 2048)
    block_count = slot_total // block_len
    targets = jnp.where(usable, indices, -1).reshape(block_count, block_len)
    pieces = values.reshape(block_count, block_len, width)
    row_ids = jnp.arange(row_count, dtype=jnp.int32)

    def add_block(summed, scan_item):
        row_target, piece_vals = scan_item
        one_hot = (row_ids[:, None] == row_target[None, :]).astype(jnp.bfloat16)
        return (summed + jnp.dot(one_hot, piece_vals, preferred_element_type=jnp.float32), None)

    result, unused = lax.scan(
        add_block, jnp.zeros((row_count, width), jnp.float32), (targets, pieces)
    )
    return result


def dense(
    grid_state, w_src, bias_src, mesh_embed, w_node, w_dec, slot_src, slot_dst, slot_count
):
    peers = lax.axis_size("graph")
    own_index = lax.axis_index("graph")
    core_index = lax.axis_index("chan")
    capacity = slot_src.shape[2]
    positions = jnp.arange(capacity, dtype=jnp.int32)
    grid_rows = grid_state.shape[0]
    mesh_rows = mesh_embed.shape[0]
    sent_counts = lax.dynamic_slice_in_dim(slot_count, own_index, 1, 0)[0]
    recv_counts = lax.dynamic_slice_in_dim(slot_count, own_index, 1, 1)[:, 0]
    half_slots = capacity // 2
    chosen = lax.dynamic_slice_in_dim(slot_src[0], core_index * half_slots, half_slots, 1)
    picked = jnp.take(grid_state, chosen.reshape(-1), axis=0).reshape(
        peers, half_slots, grid_state.shape[1]
    )
    arrived = lax.all_to_all(picked, "graph", split_axis=0, concat_axis=0, tiled=True)
    partner = lax.ppermute(arrived, "chan", [(0, 1), (1, 0)])
    joined = jnp.where(
        core_index == 0,
        jnp.concatenate([arrived, partner], axis=1),
        jnp.concatenate([partner, arrived], axis=1),
    )
    messages = edge_network(joined.reshape(peers * capacity, grid_state.shape[1]), w_src, bias_src)
    arrive_ok = (positions[None, :] < recv_counts[:, None]).reshape(-1)
    dst_rows = slot_dst[:, 0, :].reshape(-1)
    aggregate = segment_rows(messages, dst_rows, arrive_ok, mesh_rows)
    partial_hidden = jnp.dot(
        aggregate.astype(jnp.bfloat16), w_node, preferred_element_type=jnp.float32
    )
    hidden_pre = sum_at_owner(partial_hidden, "chan", 1)
    latent = (mesh_embed.astype(jnp.float32) + jax.nn.silu(hidden_pre)).astype(jnp.bfloat16)
    partial_proj = jnp.dot(latent, w_dec, preferred_element_type=jnp.float32)
    projected = sum_at_owner(partial_proj, "chan", 1).astype(jnp.bfloat16)
    returned = jnp.take(projected, dst_rows, axis=0).reshape(peers, capacity, projected.shape[1])
    came_back = lax.all_to_all(returned, "graph", split_axis=0, concat_axis=0, tiled=True).reshape(
        peers * capacity, projected.shape[1]
    )
    send_ok = (positions[None, :] < sent_counts[:, None]).reshape(-1)
    decoded = segment_rows(came_back, slot_src[0].reshape(-1), send_ok, grid_rows)
    width_half = decoded.shape[1]
    own_cols = lax.dynamic_slice_in_dim(grid_state, core_index * width_half, width_half, 1)
    return (own_cols.astype(jnp.float32) + decoded).astype(jnp.bfloat16)


def torus(n):
    wide = 1 << (n.bit_length() // 2)
    return n // wide, wide


def visit_order(n):
    tall, wide = torus(n)
    offsets = [(r, c) for r in range(tall) for c in range(wide)][1:]
    offsets.sort(key=lambda o: min(o[0], tall - o[0]) + min(o[1], wide - o[1]))
    return [offsets[i // 2] if i % 2 == 0 else offsets[-1 - i // 2] for i in range(n - 1)]


def silu(v):
    h = 0.5 * v
    return h + h * jnp.tanh(h)


def pick_turned(table, idx):
    rows = table.shape[0]
    hot = jnp.where(
        lax.broadcasted_iota(jnp.int32, (rows, idx.shape[1]), 0) == idx, 1.0, 0.0
    ).astype(jnp.bfloat16)
    return lax.dot_general(table, hot, (((0,), (0,)), ((), ())), preferred_element_type=jnp.float32)


def spread(rows, idx):
    return jnp.where(
        lax.broadcasted_iota(jnp.int32, (rows, idx.shape[1]), 0) == idx, 1.0, 0.0
    ).astype(jnp.bfloat16)


def step_kernel(
    n, hot_ref, grid_hbm, wsrc_hbm, bias_hbm, embed_hbm, wnode_hbm, wdec_hbm, src_hbm, dst_hbm, count_hbm, out_ref,
    grid_ref, wsrc_ref, bias_ref, embed_ref, wnode_ref, wdec_ref, src_ref, dst_ref, count_ref,
    src_live, dst_live, srcx_ref, dstx_ref,
    base_out, near_out, base_in, near_in, dst_in, emb_in, emb_out, emb_half, part_out, part_in,
    acc, hid_out, hid_in, prj_out, prj_in, prj_bf, back_out, nback_out, back_in, nback_in, hot_out, hot_in, dec,
    hhid_out, hhid_in, hprj_out, hprj_in,
    lsem, ssem, rsem,
):
    me = lax.axis_index("graph")
    core = lax.axis_index("chan")
    other = 1 - core
    grid_rows = grid_ref.shape[0]
    mesh_rows = embed_ref.shape[0]
    owners = mesh_rows // OWN
    span = cap_near(dst_ref.shape[2])
    used = (2 * REACH + 1) * span
    half = hid_out.shape[1]
    quarter = prj_out.shape[1]
    bf = jnp.bfloat16
    dot = functools.partial(jnp.dot, preferred_element_type=jnp.float32)

    pairs = (
        (src_hbm, src_ref), (dst_hbm, dst_ref), (count_hbm, count_ref), (grid_hbm, grid_ref), (embed_hbm, embed_ref),
        (wdec_hbm, wdec_ref), (wsrc_hbm, wsrc_ref), (bias_hbm, bias_ref), (wnode_hbm, wnode_ref),
    )
    SRC, DSTS, COUNT, GRID, EMBED, WDEC, WSRC, BIAS, WNODE = (
        pltpu.make_async_copy(x, y, lsem.at[i]) for i, (x, y) in enumerate(pairs))
    for copy in (SRC, DSTS, COUNT, GRID, EMBED, WDEC, WSRC, BIAS, WNODE):
        copy.start()

    tall, wide = torus(n)
    codes = [r * 2 * wide + c for r, c in visit_order(n)]
    groups = [codes[i:i + GROUP] for i in range(0, n - 1, GROUP)]
    spot = 2 * wide * (me // wide) + lax.rem(me, wide) + core * (2 * wide * tall + wide)
    turn = 1 - 2 * core

    def each_peer(visit):
        @pl.loop(0, len(groups))
        def _(g):
            for part in (range(0, 4), range(4, GROUP)):
                packed = jnp.int32(0)
                for i, group in enumerate(groups):
                    packed = jnp.where(g == i, sum(group[k] << (7 * j) for j, k in enumerate(part)), packed)
                for j in range(len(part)):
                    code = lax.shift_right_logical(packed, jnp.int32(7 * j)) & 127
                    at = spot + turn * code
                    visit((lax.shift_right_logical(at, jnp.int32(1)) & ((tall - 1) * wide)) + (at & (wide - 1)))

    per_row = owners // tall

    def seat(shard):
        r = lax.shift_right_logical(shard, jnp.int32(wide.bit_length() - 1))
        rank = (shard + 3 * r) & (wide - 1)
        return rank < per_row, r * per_row + rank

    mine, my_block = seat(me)
    barrier = pltpu.get_barrier_semaphore()
    each_peer(lambda peer: pl.semaphore_signal(barrier, inc=1, device_id={"graph": peer}, device_id_type=MESH_ID))
    pl.semaphore_signal(barrier, inc=1, device_id={"chan": other}, device_id_type=MESH_ID)

    def to_graph(src, dst, k, peer):
        return pltpu.make_async_remote_copy(
            src_ref=src, dst_ref=dst, send_sem=ssem.at[k], recv_sem=rsem.at[k],
            device_id={"graph": peer}, device_id_type=MESH_ID)

    def to_core(src, dst, k):
        return pltpu.make_async_remote_copy(
            src_ref=src, dst_ref=dst, send_sem=ssem.at[k], recv_sem=rsem.at[k],
            device_id={"chan": other}, device_id_type=MESH_ID)

    def wait_in(ref, k):
        to_graph(ref, ref, k, me).wait_recv()

    def wait_out(ref, k):
        to_graph(ref, ref, k, me).wait_send()

    DST, EMB, BASE, NEAR, PART, FWDB, FWDN, HID, PRJ, BACK, NBACK, HOT, PRJ0, BACK1, HIDH, PRJH = range(SEMS)

    blocks = (n * HALF) // CHUNK
    capacity = dst_ref.shape[2]
    SRC.wait()
    DSTS.wait()
    COUNT.wait()
    with jax.named_scope("index"):
        hot = hot_ref[0]
        ids = lax.broadcasted_iota(jnp.int32, (n, n), 0)
        cols = lax.broadcasted_iota(jnp.int32, (n, n), 1)
        counts = count_ref[...]
        sent = jnp.where(ids == me, counts, 0).sum(axis=0, keepdims=True)
        sent = jnp.where(ids == cols, sent, 0).sum(axis=1, keepdims=True)
        came = jnp.where(cols == me, counts, 0).sum(axis=1, keepdims=True)
        pos = lax.broadcasted_iota(jnp.int32, (n, capacity), 1)
        src_all = jnp.where(pos < sent, src_ref[0] + 1, 0).astype(jnp.float32)
        src_live[...] = src_all
        came = jnp.where(me == hot, 0, came)
        dst_all = jnp.where(pos < came, dst_ref[:, 0, :] + 1, 0).astype(jnp.float32)
        dst_live[...] = dst_all
        rows_id = lax.broadcasted_iota(jnp.int32, (n, capacity), 0)
        src_all = jnp.where(rows_id == hot, 0.0, src_all)
        near_id = lax.broadcasted_iota(jnp.int32, (8, capacity), 0)
        near_src = jnp.zeros((8, capacity), jnp.float32)
        near_dst = jnp.zeros((8, capacity), jnp.float32)
        for o in range(-REACH, REACH + 1):
            to = lax.rem(me + o + n, n)
            row = jnp.where(to == hot, 0.0, src_live[pl.ds(to, 1)])
            near_src = jnp.where(near_id == o + REACH, row, near_src)
            near_dst = jnp.where(near_id == o + REACH, dst_live[pl.ds(lax.rem(me - o + n, n), 1)], near_dst)
        for h in range(2):
            base = base_layout(capacity, h)
            srcx_ref[h, 0:blocks] = lay_out(src_all, *base)
            dstx_ref[h, 0:blocks] = lay_out(dst_all, *base)
            near = near_layout(capacity, h)
            srcx_ref[h, blocks:] = lay_out(near_src, *near)[:, 0:CHUNK]
            dstx_ref[h, blocks:] = lay_out(near_dst, *near)[:, 0:CHUNK]

    GRID.wait()

    for j in range(blocks):
        rows = pick_turned(grid_ref[...], srcx_ref[core, j:j + 1]).T.astype(bf)
        base_out[j * (CHUNK // HALF):(j + 1) * (CHUNK // HALF)] = rows.reshape(CHUNK // HALF, HALF, rows.shape[1])

    near_out[...] = pick_turned(grid_ref[...], srcx_ref[core, blocks:]).T.astype(bf)
    near_in[core, used:, :] = jnp.zeros((NEAR_ROWS - used, near_in.shape[2]), bf)

    pl.semaphore_wait(barrier, n)
    each_peer(lambda peer: to_graph(dst_ref.at[peer], dst_in.at[me], DST, peer).start())
    for o in range(-REACH, REACH + 1):
        rows = pl.ds((o + REACH) * span, span)
        if o == 0:
            near_in[core, (o + REACH) * span:(o + REACH + 1) * span] = near_out[(o + REACH) * span:(o + REACH + 1) * span]
        else:
            to_graph(near_out.at[rows], near_in.at[core, rows], NEAR, lax.rem(me + o + n, n)).start()
    each_peer(lambda peer: to_graph(base_out.at[peer], base_in.at[core, me], BASE, peer).start())
    base_in[core, pl.ds(me, 1)] = base_out[pl.ds(me, 1)]
    dst_in[pl.ds(me, 1)] = dst_ref[pl.ds(me, 1)]

    EMBED.wait()
    WDEC.wait()
    w_other = wdec_ref[:, pl.ds(pl.multiple_of(other * quarter, quarter), quarter)]
    w_own = wdec_ref[:, pl.ds(pl.multiple_of(core * quarter, quarter), quarter)]
    prj_out[...] = dot(embed_ref[...], w_other)
    send0 = to_core(prj_out, emb_half, PRJ0)
    send0.start()
    WSRC.wait()
    BIAS.wait()
    hot_src = src_live[pl.ds(hot, 1)].astype(jnp.int32) - 1
    msgs = silu(dot(pick_turned(grid_ref[...], hot_src).T.astype(bf), wsrc_ref[...]) + bias_ref[...]).astype(bf)
    emb_own = dot(embed_ref[...], w_own)
    send0.wait_recv()
    emb_out[...] = (emb_own + emb_half[...]).astype(bf).reshape(owners, OWN, quarter)

    wait_in(dst_in.at[pl.ds(0, n - 1)], DST)
    hot_dst = jnp.where(hot_src >= 0, dst_in[hot], -1)
    part_out[...] = dot(spread(mesh_rows, hot_dst), msgs).astype(bf).reshape(owners, OWN, half)

    def to_owner(copy_to):
        def visit(peer):
            owns, block = seat(peer)

            @pl.when(owns)
            def _():
                copy_to(peer, block).start()
        return visit

    each_peer(to_owner(lambda peer, block: to_graph(part_out.at[block], part_in.at[me], PART, peer)))
    each_peer(to_owner(lambda peer, block: to_graph(emb_out.at[block], emb_in.at[me], EMB, peer)))

    wait_in(base_in.at[core, pl.ds(0, n - 1)], BASE)
    to_core(base_in.at[core], base_in.at[core], FWDB).start()
    wait_in(near_in.at[core, pl.ds(0, 2 * REACH * span)], NEAR)
    to_core(near_in.at[core], near_in.at[core], FWDN).start()
    def share(rows, idx):
        m = silu(dot(rows, wsrc_ref[...]) + bias_ref[...]).astype(bf)
        return dot(spread(mesh_rows, idx), m)

    def half_sum(h):
        total = share(near_in[h], dstx_ref[h, blocks:])
        for j in range(blocks):
            rows = base_in[h, j * (CHUNK // HALF):(j + 1) * (CHUNK // HALF)].reshape(CHUNK, base_in.shape[3])
            total = total + share(rows, dstx_ref[h, j:j + 1])
        return total

    acc[...] = half_sum(core)
    to_core(base_in.at[other], base_in.at[other], FWDB).wait_recv()
    to_core(near_in.at[other], near_in.at[other], FWDN).wait_recv()

    WNODE.wait()
    n_other = wnode_ref[:, pl.ds(pl.multiple_of(other * half, half), half)]
    n_own = wnode_ref[:, pl.ds(pl.multiple_of(core * half, half), half)]
    agg = (acc[...] + half_sum(other)).astype(bf)
    hid_out[...] = dot(agg, n_other)
    send = to_core(hid_out, hid_in, HID)
    send.start()
    own = dot(agg, n_own)
    send0.wait_send()
    send.wait_recv()
    lat = (embed_ref[...].astype(jnp.float32) + silu(own + hid_in[...])).astype(bf)
    prj_out[...] = dot(lat, w_other)
    send2 = to_core(prj_out, prj_in, PRJ)
    send2.start()
    own_p = dot(lat, w_own)

    send2.wait_recv()
    prj_bf[...] = (own_p + prj_in[...]).astype(bf)
    for h in range(2):
        nback_out[h] = pick_turned(prj_bf[...], dstx_ref[h, blocks:]).T.astype(bf)
        nback_in[h, used:, :] = jnp.zeros((NEAR_ROWS - used, quarter), bf)
        for o in range(-REACH, REACH + 1):
            a = (o + REACH) * span
            if o == 0:
                nback_in[h, a:a + span] = nback_out[h, a:a + span]
            else:
                to_graph(nback_out.at[h, pl.ds(a, span)], nback_in.at[h, pl.ds(a, span)], NBACK, lax.rem(me - o + n, n)).start()

    for h in range(2):
        for j in range(blocks):
            rows = pick_turned(prj_bf[...], dstx_ref[h, j:j + 1]).T.astype(bf)
            back_out[h, j * (CHUNK // HALF):(j + 1) * (CHUNK // HALF)] = rows.reshape(CHUNK // HALF, HALF, quarter)
        back_in[h, pl.ds(me, 1)] = back_out[h, pl.ds(me, 1)]
        each_peer(lambda peer, h=h: to_graph(back_out.at[h, peer], back_in.at[h, me], BACK1 if h else BACK, peer).start())

    @pl.when(mine)
    def _():
        wait_in(part_in.at[pl.ds(0, n - 1)], PART)
        part_in[pl.ds(me, 1)] = part_out[pl.ds(my_block, 1)]

    hot_agg = part_in[...].astype(jnp.float32).sum(axis=0).astype(bf)
    hhid_out[...] = dot(hot_agg, n_other)
    send3 = to_core(hhid_out, hhid_in, HIDH)
    send3.start()
    hot_own = dot(hot_agg, n_own)

    send3.wait_recv()
    hot_lat = silu(hot_own + hhid_in[...]).astype(bf)
    hprj_out[...] = dot(hot_lat, w_other)
    send4 = to_core(hprj_out, hprj_in, PRJH)
    send4.start()
    hot_prj = dot(hot_lat, w_own)

    @pl.when(mine)
    def _():
        wait_in(emb_in.at[pl.ds(0, n - 1)], EMB)
        emb_in[pl.ds(me, 1)] = emb_out[pl.ds(my_block, 1)]

    send4.wait_recv()
    hot_out[...] = (hot_prj + hprj_in[...] + emb_in[hot].astype(jnp.float32)).astype(bf)

    @pl.when(mine)
    def _():
        each_peer(lambda peer: to_graph(hot_out, hot_in.at[my_block], HOT, peer).start())

    wait_in(nback_in.at[:, pl.ds(0, 2 * REACH * span)], NBACK)
    total = grid_ref[:, pl.ds(pl.multiple_of(core * quarter, quarter), quarter)].astype(jnp.float32)
    for h in range(2):
        total = total + dot(spread(grid_rows, srcx_ref[h, blocks:]), nback_in[h])
    dec[...] = total
    for h in range(2):
        wait_in(back_in.at[h, pl.ds(0, n - 1)], BACK1 if h else BACK)
        total = dec[...]
        for j in range(blocks):
            rows = back_in[h, j * (CHUNK // HALF):(j + 1) * (CHUNK // HALF)].reshape(CHUNK, quarter)
            total = total + dot(spread(grid_rows, srcx_ref[h, j:j + 1]), rows)
        dec[...] = total

    @pl.when(mine)
    def _():
        wait_in(hot_in.at[pl.ds(0, owners - 1)], HOT)
        hot_in[pl.ds(my_block, 1)] = hot_out[...].reshape(1, OWN, quarter)

    @pl.when(jnp.logical_not(mine))
    def _():
        wait_in(hot_in, HOT)

    hot_rows = pick_turned(hot_in[...].reshape(mesh_rows, quarter), hot_dst).astype(bf)
    back = lax.dot_general(spread(grid_rows, hot_src), hot_rows, (((1,), (1,)), ((), ())), preferred_element_type=jnp.float32)
    out_ref[...] = (dec[...] + back).astype(bf)

    wait_out(dst_ref.at[pl.ds(0, n - 1)], DST)
    wait_out(base_out.at[pl.ds(0, n - 1)], BASE)
    wait_out(near_out.at[pl.ds(0, 2 * REACH * span)], NEAR)

    @pl.when(mine)
    def _():
        wait_out(emb_out.at[pl.ds(0, owners - 1)], EMB)
        wait_out(part_out.at[pl.ds(0, owners - 1)], PART)
        wait_out(back_out.at[0, pl.ds(0, n - 1)], HOT)

    @pl.when(jnp.logical_not(mine))
    def _():
        wait_out(emb_out, EMB)
        wait_out(part_out, PART)

    to_core(base_in.at[core], base_in.at[core], FWDB).wait_send()
    to_core(near_in.at[core], near_in.at[core], FWDN).wait_send()
    for copy in (send, send2, send3, send4):
        copy.wait_send()
    for h in range(2):
        wait_out(back_out.at[h, pl.ds(0, n - 1)], BACK1 if h else BACK)
    wait_out(nback_out.at[:, pl.ds(0, 2 * REACH * span)], NBACK)


def cap_near(capacity):
    return (capacity - KEEP) // 2


def lay_out(table, take, mark):
    high = jnp.floor(table * (1.0 / 32.0))
    low = table - 32.0 * high
    dot = functools.partial(jnp.dot, preferred_element_type=jnp.float32)
    moved = 32.0 * dot(high.astype(jnp.bfloat16), take) + dot(low.astype(jnp.bfloat16), take)
    group = mark.shape[0]
    moved = moved.reshape(table.shape[0] // group, group, take.shape[1])
    return (moved * mark[None]).sum(axis=1).astype(jnp.int32) - 1


def base_layout(capacity, h):
    shape = (capacity, CHUNK)
    lane = lax.broadcasted_iota(jnp.int32, shape, 1)
    slot = lax.broadcasted_iota(jnp.int32, shape, 0)
    take = jnp.where(slot == h * HALF + (lane & (HALF - 1)), 1.0, 0.0).astype(jnp.bfloat16)
    group = CHUNK // HALF
    lane = lax.broadcasted_iota(jnp.int32, (group, CHUNK), 1)
    row = lax.broadcasted_iota(jnp.int32, (group, CHUNK), 0)
    return take, jnp.where(row * HALF <= lane, 1.0, 0.0) * jnp.where(lane < row * HALF + HALF, 1.0, 0.0)


def near_layout(capacity, h):
    span = cap_near(capacity)
    count = 2 * REACH + 1
    shape = (capacity, NEAR_ROWS)
    lane = lax.broadcasted_iota(jnp.int32, shape, 1)
    slot = lax.broadcasted_iota(jnp.int32, shape, 0)
    within = lane
    for i in range(1, count + 1):
        within = within - jnp.where(lane >= i * span, span, 0)
    take = jnp.where(slot == KEEP + h * span + within, 1.0, 0.0).astype(jnp.bfloat16)
    lane = lax.broadcasted_iota(jnp.int32, (8, NEAR_ROWS), 1)
    row = lax.broadcasted_iota(jnp.int32, (8, NEAR_ROWS), 0)
    inside = jnp.where(row * span <= lane, 1.0, 0.0) * jnp.where(lane < row * span + span, 1.0, 0.0)
    return take, inside * jnp.where(row < count, 1.0, 0.0)


def compact(hot, grid_state, w_src, bias_src, mesh_embed, w_node, w_dec, slot_src, slot_dst, slot_count):
    n = lax.axis_size("graph")
    capacity = slot_src.shape[2]
    grid_rows, width = grid_state.shape
    mesh_rows, half = mesh_embed.shape
    quarter = width // 2
    owners = mesh_rows // OWN
    bf, f32 = jnp.bfloat16, jnp.float32
    vm = pltpu.VMEM
    return pl.pallas_call(
        functools.partial(step_kernel, n),
        out_shape=jax.ShapeDtypeStruct((grid_rows, quarter), bf),
        in_specs=[pl.BlockSpec(memory_space=pltpu.SMEM)] + [pl.BlockSpec(memory_space=pl.ANY)] * 9,
        out_specs=pl.BlockSpec(memory_space=vm),
        scratch_shapes=[
            vm((grid_rows, width), bf), vm(w_src.shape, bf), vm((1, half), f32), vm((mesh_rows, half), bf), vm(w_node.shape, bf),
            vm(w_dec.shape, bf), vm(slot_src.shape, jnp.int32), vm(slot_dst.shape, jnp.int32), vm(slot_count.shape, jnp.int32),
            vm((n, capacity), f32), vm((n, capacity), f32),
            vm((2, n * HALF // CHUNK + 1, CHUNK), jnp.int32), vm((2, n * HALF // CHUNK + 1, CHUNK), jnp.int32),
            vm((n, HALF, width), bf), vm((NEAR_ROWS, width), bf),
            vm((2, n, HALF, width), bf), vm((2, NEAR_ROWS, width), bf),
            vm((n, 1, capacity), jnp.int32), vm((n, OWN, quarter), bf), vm((owners, OWN, quarter), bf), vm((mesh_rows, quarter), f32),
            vm((owners, OWN, half), bf), vm((n, OWN, half), bf),
            vm((mesh_rows, half), f32),
            vm((mesh_rows, half), f32), vm((mesh_rows, half), f32),
            vm((mesh_rows, quarter), f32), vm((mesh_rows, quarter), f32), vm((mesh_rows, quarter), bf),
            vm((2, n, HALF, quarter), bf), vm((2, NEAR_ROWS, quarter), bf),
            vm((2, n, HALF, quarter), bf), vm((2, NEAR_ROWS, quarter), bf),
            vm((OWN, quarter), bf), vm((owners, OWN, quarter), bf),
            vm((grid_rows, quarter), f32),
            vm((OWN, half), f32), vm((OWN, half), f32), vm((OWN, quarter), f32), vm((OWN, quarter), f32),
            pltpu.SemaphoreType.DMA((9,)), pltpu.SemaphoreType.DMA((SEMS,)), pltpu.SemaphoreType.DMA((SEMS,)),
        ],
        compiler_params=pltpu.CompilerParams(collective_id=0, has_side_effects=True, vmem_limit_bytes=48 * 1024 * 1024),
    )(hot, grid_state, w_src, bias_src[None, :], mesh_embed, w_node, w_dec, slot_src, slot_dst, slot_count)


def on_device(grid_state, w_src, bias_src, mesh_embed, w_node, w_dec, slot_src, slot_dst, slot_count):
    args = (grid_state, w_src, bias_src, mesh_embed, w_node, w_dec, slot_src, slot_dst, slot_count)
    n = slot_count.shape[0]
    apart = jnp.abs(jnp.arange(n)[:, None] - jnp.arange(n)[None, :])
    far = jnp.minimum(apart, n - apart) > REACH
    over = far & (slot_count > KEEP)
    column = jnp.broadcast_to(jnp.arange(n, dtype=jnp.int32)[None, :], (n, n))
    last = jnp.max(jnp.where(over, column, 0))
    first = jnp.min(jnp.where(over, column, n))
    fits = last <= first
    hot = last.reshape(1)
    return lax.cond(fits, lambda: compact(hot, *args), lambda: dense(*args))


def solution(mesh):
    placed = (
        P(("member", "graph"), None),
        P(None, "chan"),
        P("chan"),
        P("graph", "chan"),
        P("chan", None),
        P("chan", None),
        P("graph", None, None),
        P(None, "graph", None),
        P(),
    )
    return jax.shard_map(
        on_device,
        mesh=mesh,
        in_specs=placed,
        out_specs=P(("member", "graph"), "chan"),
        check_vma=False,
    )
```

```python
import functools
import math

import jax
import jax.numpy as jnp
from jax import lax
from jax.experimental import pallas as pl
from jax.experimental.pallas import tpu as pltpu
from jax.sharding import PartitionSpec as P

MESH_ID = pl.DeviceIdType.MESH
KEEP = 32
HALF = KEEP // 2
GROUP = 7
SEMS = 15
REACH = 2
OWN = 16
NEAR_ROWS = 256
CHUNK = 256

def split_up(value, dim, count):
    lengths = value.shape
    parts = value.reshape(*lengths[:dim], count, lengths[dim] // count, *lengths[dim + 1 :])
    return jnp.moveaxis(parts, dim, 0)


def sum_at_owner(value, axis, dim):
    parts = split_up(value, dim, lax.axis_size(axis))
    arrived = lax.all_to_all(parts, axis, split_axis=0, concat_axis=0, tiled=True)
    return arrived.sum(axis=0)


def edge_network(source_rows, w_src, bias_src):
    return jax.nn.silu(
        jnp.dot(source_rows, w_src, preferred_element_type=jnp.float32) + bias_src
    ).astype(jnp.bfloat16)


def segment_rows(values, indices, usable, row_count):
    slot_total = values.shape[0]
    width = values.shape[1]
    block_len = math.gcd(slot_total, 2048)
    block_count = slot_total // block_len
    targets = jnp.where(usable, indices, -1).reshape(block_count, block_len)
    pieces = values.reshape(block_count, block_len, width)
    row_ids = jnp.arange(row_count, dtype=jnp.int32)

    def add_block(summed, scan_item):
        row_target, piece_vals = scan_item
        one_hot = (row_ids[:, None] == row_target[None, :]).astype(jnp.bfloat16)
        return (summed + jnp.dot(one_hot, piece_vals, preferred_element_type=jnp.float32), None)

    result, unused = lax.scan(
        add_block, jnp.zeros((row_count, width), jnp.float32), (targets, pieces)
    )
    return result


def dense(
    grid_state, w_src, bias_src, mesh_embed, w_node, w_dec, slot_src, slot_dst, slot_count
):
    peers = lax.axis_size("graph")
    own_index = lax.axis_index("graph")
    core_index = lax.axis_index("chan")
    capacity = slot_src.shape[2]
    positions = jnp.arange(capacity, dtype=jnp.int32)
    grid_rows = grid_state.shape[0]
    mesh_rows = mesh_embed.shape[0]
    sent_counts = lax.dynamic_slice_in_dim(slot_count, own_index, 1, 0)[0]
    recv_counts = lax.dynamic_slice_in_dim(slot_count, own_index, 1, 1)[:, 0]
    half_slots = capacity // 2
    chosen = lax.dynamic_slice_in_dim(slot_src[0], core_index * half_slots, half_slots, 1)
    picked = jnp.take(grid_state, chosen.reshape(-1), axis=0).reshape(
        peers, half_slots, grid_state.shape[1]
    )
    arrived = lax.all_to_all(picked, "graph", split_axis=0, concat_axis=0, tiled=True)
    partner = lax.ppermute(arrived, "chan", [(0, 1), (1, 0)])
    joined = jnp.where(
        core_index == 0,
        jnp.concatenate([arrived, partner], axis=1),
        jnp.concatenate([partner, arrived], axis=1),
    )
    messages = edge_network(joined.reshape(peers * capacity, grid_state.shape[1]), w_src, bias_src)
    arrive_ok = (positions[None, :] < recv_counts[:, None]).reshape(-1)
    dst_rows = slot_dst[:, 0, :].reshape(-1)
    aggregate = segment_rows(messages, dst_rows, arrive_ok, mesh_rows)
    partial_hidden = jnp.dot(
        aggregate.astype(jnp.bfloat16), w_node, preferred_element_type=jnp.float32
    )
    hidden_pre = sum_at_owner(partial_hidden, "chan", 1)
    latent = (mesh_embed.astype(jnp.float32) + jax.nn.silu(hidden_pre)).astype(jnp.bfloat16)
    partial_proj = jnp.dot(latent, w_dec, preferred_element_type=jnp.float32)
    projected = sum_at_owner(partial_proj, "chan", 1).astype(jnp.bfloat16)
    returned = jnp.take(projected, dst_rows, axis=0).reshape(peers, capacity, projected.shape[1])
    came_back = lax.all_to_all(returned, "graph", split_axis=0, concat_axis=0, tiled=True).reshape(
        peers * capacity, projected.shape[1]
    )
    send_ok = (positions[None, :] < sent_counts[:, None]).reshape(-1)
    decoded = segment_rows(came_back, slot_src[0].reshape(-1), send_ok, grid_rows)
    width_half = decoded.shape[1]
    own_cols = lax.dynamic_slice_in_dim(grid_state, core_index * width_half, width_half, 1)
    return (own_cols.astype(jnp.float32) + decoded).astype(jnp.bfloat16)


def torus(n):
    wide = 1 << (n.bit_length() // 2)
    return n // wide, wide


def visit_order(n):
    tall, wide = torus(n)
    offsets = [(r, c) for r in range(tall) for c in range(wide)][1:]
    offsets.sort(key=lambda o: min(o[0], tall - o[0]) + min(o[1], wide - o[1]))
    return [offsets[i // 2] if i % 2 == 0 else offsets[-1 - i // 2] for i in range(n - 1)]


def silu(v):
    h = 0.5 * v
    return h + h * jnp.tanh(h)


def pick_turned(table, idx):
    rows = table.shape[0]
    hot = jnp.where(
        lax.broadcasted_iota(jnp.int32, (rows, idx.shape[1]), 0) == idx, 1.0, 0.0
    ).astype(jnp.bfloat16)
    return lax.dot_general(table, hot, (((0,), (0,)), ((), ())), preferred_element_type=jnp.float32)


def spread(rows, idx):
    return jnp.where(
        lax.broadcasted_iota(jnp.int32, (rows, idx.shape[1]), 0) == idx, 1.0, 0.0
    ).astype(jnp.bfloat16)


def step_kernel(
    n, hot_ref, grid_hbm, wsrc_hbm, bias_hbm, embed_hbm, wnode_hbm, wdec_hbm, src_hbm, dst_hbm, count_hbm, out_ref,
    grid_ref, wsrc_ref, bias_ref, embed_ref, wnode_ref, wdec_ref, src_ref, dst_ref, count_ref,
    src_live, dst_live, srcx_ref, dstx_ref,
    base_out, near_out, base_in, near_in, dst_in, emb_in, emb_out, emb_half, part_out, part_in,
    acc, hid_out, hid_in, prj_out, prj_in, prj_bf, back_out, nback_out, back_in, nback_in, hot_out, hot_in, dec,
    hhid_out, hhid_in, hprj_out, hprj_in,
    lsem, ssem, rsem,
):
    me = lax.axis_index("graph")
    core = lax.axis_index("chan")
    other = 1 - core
    grid_rows = grid_ref.shape[0]
    mesh_rows = embed_ref.shape[0]
    owners = mesh_rows // OWN
    span = cap_near(dst_ref.shape[2])
    used = (2 * REACH + 1) * span
    half = hid_out.shape[1]
    quarter = prj_out.shape[1]
    bf = jnp.bfloat16
    dot = functools.partial(jnp.dot, preferred_element_type=jnp.float32)

    pairs = (
        (src_hbm, src_ref), (dst_hbm, dst_ref), (count_hbm, count_ref), (grid_hbm, grid_ref), (embed_hbm, embed_ref),
        (wdec_hbm, wdec_ref), (wsrc_hbm, wsrc_ref), (bias_hbm, bias_ref), (wnode_hbm, wnode_ref),
    )
    SRC, DSTS, COUNT, GRID, EMBED, WDEC, WSRC, BIAS, WNODE = (
        pltpu.make_async_copy(x, y, lsem.at[i]) for i, (x, y) in enumerate(pairs))
    for copy in (SRC, DSTS, COUNT, GRID, EMBED, WDEC, WSRC, BIAS, WNODE):
        copy.start()

    tall, wide = torus(n)
    codes = [r * 2 * wide + c for r, c in visit_order(n)]
    groups = [codes[i:i + GROUP] for i in range(0, n - 1, GROUP)]
    spot = 2 * wide * (me // wide) + lax.rem(me, wide) + core * (2 * wide * tall + wide)
    turn = 1 - 2 * core

    def each_peer(visit):
        @pl.loop(0, len(groups))
        def _(g):
            for part in (range(0, 4), range(4, GROUP)):
                packed = jnp.int32(0)
                for i, group in enumerate(groups):
                    packed = jnp.where(g == i, sum(group[k] << (7 * j) for j, k in enumerate(part)), packed)
                for j in range(len(part)):
                    code = lax.shift_right_logical(packed, jnp.int32(7 * j)) & 127
                    at = spot + turn * code
                    visit((lax.shift_right_logical(at, jnp.int32(1)) & ((tall - 1) * wide)) + (at & (wide - 1)))

    per_row = owners // tall

    def seat(shard):
        r = lax.shift_right_logical(shard, jnp.int32(wide.bit_length() - 1))
        rank = (shard + 3 * r) & (wide - 1)
        return rank < per_row, r * per_row + rank

    mine, my_block = seat(me)
    barrier = pltpu.get_barrier_semaphore()
    each_peer(lambda peer: pl.semaphore_signal(barrier, inc=1, device_id={"graph": peer}, device_id_type=MESH_ID))
    pl.semaphore_signal(barrier, inc=1, device_id={"chan": other}, device_id_type=MESH_ID)

    def to_graph(src, dst, k, peer):
        return pltpu.make_async_remote_copy(
            src_ref=src, dst_ref=dst, send_sem=ssem.at[k], recv_sem=rsem.at[k],
            device_id={"graph": peer}, device_id_type=MESH_ID)

    def to_core(src, dst, k):
        return pltpu.make_async_remote_copy(
            src_ref=src, dst_ref=dst, send_sem=ssem.at[k], recv_sem=rsem.at[k],
            device_id={"chan": other}, device_id_type=MESH_ID)

    def wait_in(ref, k):
        to_graph(ref, ref, k, me).wait_recv()

    def wait_out(ref, k):
        to_graph(ref, ref, k, me).wait_send()

    DST, EMB, BASE, NEAR, PART, FWDB, FWDN, HID, PRJ, BACK, NBACK, HOT, PRJ0, HIDH, PRJH = range(SEMS)

    blocks = (n * HALF) // CHUNK
    capacity = dst_ref.shape[2]
    SRC.wait()
    DSTS.wait()
    COUNT.wait()
    with jax.named_scope("index"):
        hot = hot_ref[0]
        ids = lax.broadcasted_iota(jnp.int32, (n, n), 0)
        cols = lax.broadcasted_iota(jnp.int32, (n, n), 1)
        counts = count_ref[...]
        sent = jnp.where(ids == me, counts, 0).sum(axis=0, keepdims=True)
        sent = jnp.where(ids == cols, sent, 0).sum(axis=1, keepdims=True)
        came = jnp.where(cols == me, counts, 0).sum(axis=1, keepdims=True)
        pos = lax.broadcasted_iota(jnp.int32, (n, capacity), 1)
        src_all = jnp.where(pos < sent, src_ref[0] + 1, 0).astype(jnp.float32)
        src_live[...] = src_all
        came = jnp.where(me == hot, 0, came)
        dst_all = jnp.where(pos < came, dst_ref[:, 0, :] + 1, 0).astype(jnp.float32)
        dst_live[...] = dst_all
        rows_id = lax.broadcasted_iota(jnp.int32, (n, capacity), 0)
        src_all = jnp.where(rows_id == hot, 0.0, src_all)
        near_id = lax.broadcasted_iota(jnp.int32, (8, capacity), 0)
        near_src = jnp.zeros((8, capacity), jnp.float32)
        near_dst = jnp.zeros((8, capacity), jnp.float32)
        for o in range(-REACH, REACH + 1):
            to = lax.rem(me + o + n, n)
            row = jnp.where(to == hot, 0.0, src_live[pl.ds(to, 1)])
            near_src = jnp.where(near_id == o + REACH, row, near_src)
            near_dst = jnp.where(near_id == o + REACH, dst_live[pl.ds(lax.rem(me - o + n, n), 1)], near_dst)
        for h in range(2):
            base = base_layout(capacity, h)
            srcx_ref[h, 0:blocks] = lay_out(src_all, *base)
            dstx_ref[h, 0:blocks] = lay_out(dst_all, *base)
            near = near_layout(capacity, h)
            srcx_ref[h, blocks:] = lay_out(near_src, *near)[:, 0:CHUNK]
            dstx_ref[h, blocks:] = lay_out(near_dst, *near)[:, 0:CHUNK]

    GRID.wait()

    for j in range(blocks):
        rows = pick_turned(grid_ref[...], srcx_ref[core, j:j + 1]).T.astype(bf)
        base_out[j * (CHUNK // HALF):(j + 1) * (CHUNK // HALF)] = rows.reshape(CHUNK // HALF, HALF, rows.shape[1])

    near_out[...] = pick_turned(grid_ref[...], srcx_ref[core, blocks:]).T.astype(bf)
    near_in[core, used:, :] = jnp.zeros((NEAR_ROWS - used, near_in.shape[2]), bf)

    pl.semaphore_wait(barrier, n)
    each_peer(lambda peer: to_graph(dst_ref.at[peer], dst_in.at[me], DST, peer).start())
    for o in range(-REACH, REACH + 1):
        rows = pl.ds((o + REACH) * span, span)
        if o == 0:
            near_in[core, (o + REACH) * span:(o + REACH + 1) * span] = near_out[(o + REACH) * span:(o + REACH + 1) * span]
        else:
            to_graph(near_out.at[rows], near_in.at[core, rows], NEAR, lax.rem(me + o + n, n)).start()
    each_peer(lambda peer: to_graph(base_out.at[peer], base_in.at[core, me], BASE, peer).start())
    base_in[core, pl.ds(me, 1)] = base_out[pl.ds(me, 1)]
    dst_in[pl.ds(me, 1)] = dst_ref[pl.ds(me, 1)]

    EMBED.wait()
    WDEC.wait()
    w_other = wdec_ref[:, pl.ds(pl.multiple_of(other * quarter, quarter), quarter)]
    w_own = wdec_ref[:, pl.ds(pl.multiple_of(core * quarter, quarter), quarter)]
    prj_out[...] = dot(embed_ref[...], w_other).astype(bf)
    send0 = to_core(prj_out, emb_half, PRJ0)
    send0.start()
    WSRC.wait()
    BIAS.wait()
    hot_src = src_live[pl.ds(hot, 1)].astype(jnp.int32) - 1
    msgs = silu(dot(pick_turned(grid_ref[...], hot_src).T.astype(bf), wsrc_ref[...]) + bias_ref[...]).astype(bf)
    emb_own = dot(embed_ref[...], w_own)
    send0.wait_recv()
    emb_out[...] = (emb_own + emb_half[...].astype(jnp.float32)).astype(bf).reshape(owners, OWN, quarter)

    wait_in(dst_in.at[pl.ds(0, n - 1)], DST)
    hot_dst = jnp.where(hot_src >= 0, dst_in[hot], -1)
    part_out[...] = dot(spread(mesh_rows, hot_dst), msgs).astype(bf).reshape(owners, OWN, half)

    def to_owner(copy_to):
        def visit(peer):
            owns, block = seat(peer)

            @pl.when(owns)
            def _():
                copy_to(peer, block).start()
        return visit

    each_peer(to_owner(lambda peer, block: to_graph(part_out.at[block], part_in.at[me], PART, peer)))
    each_peer(to_owner(lambda peer, block: to_graph(emb_out.at[block], emb_in.at[me], EMB, peer)))

    wait_in(base_in.at[core, pl.ds(0, n - 1)], BASE)
    to_core(base_in.at[core], base_in.at[core], FWDB).start()
    wait_in(near_in.at[core, pl.ds(0, 2 * REACH * span)], NEAR)
    to_core(near_in.at[core], near_in.at[core], FWDN).start()
    def share(rows, idx):
        m = silu(dot(rows, wsrc_ref[...]) + bias_ref[...]).astype(bf)
        return dot(spread(mesh_rows, idx), m)

    def half_sum(h):
        total = share(near_in[h], dstx_ref[h, blocks:])
        for j in range(blocks):
            rows = base_in[h, j * (CHUNK // HALF):(j + 1) * (CHUNK // HALF)].reshape(CHUNK, base_in.shape[3])
            total = total + share(rows, dstx_ref[h, j:j + 1])
        return total

    acc[...] = half_sum(core)
    to_core(base_in.at[other], base_in.at[other], FWDB).wait_recv()
    to_core(near_in.at[other], near_in.at[other], FWDN).wait_recv()

    WNODE.wait()
    n_other = wnode_ref[:, pl.ds(pl.multiple_of(other * half, half), half)]
    n_own = wnode_ref[:, pl.ds(pl.multiple_of(core * half, half), half)]
    agg = (acc[...] + half_sum(other)).astype(bf)
    hid_out[...] = dot(agg, n_other).astype(bf)
    send = to_core(hid_out, hid_in, HID)
    send.start()
    own = dot(agg, n_own)
    send0.wait_send()
    send.wait_recv()
    lat = (embed_ref[...].astype(jnp.float32) + silu(own + hid_in[...].astype(jnp.float32))).astype(bf)
    prj_out[...] = dot(lat, w_other).astype(bf)
    send2 = to_core(prj_out, prj_in, PRJ)
    send2.start()
    own_p = dot(lat, w_own)

    send2.wait_recv()
    prj_bf[...] = (own_p + prj_in[...].astype(jnp.float32)).astype(bf)
    for h in range(2):
        for j in range(blocks):
            rows = pick_turned(prj_bf[...], dstx_ref[h, j:j + 1]).T.astype(bf)
            back_out[h, j * (CHUNK // HALF):(j + 1) * (CHUNK // HALF)] = rows.reshape(CHUNK // HALF, HALF, quarter)
        back_in[h, pl.ds(me, 1)] = back_out[h, pl.ds(me, 1)]

    each_peer(lambda peer: to_graph(back_out.at[:, peer], back_in.at[:, me], BACK, peer).start())
    for h in range(2):
        nback_out[h] = pick_turned(prj_bf[...], dstx_ref[h, blocks:]).T.astype(bf)
        nback_in[h, used:, :] = jnp.zeros((NEAR_ROWS - used, quarter), bf)
        for o in range(-REACH, REACH + 1):
            a = (o + REACH) * span
            if o == 0:
                nback_in[h, a:a + span] = nback_out[h, a:a + span]
            else:
                to_graph(nback_out.at[h, pl.ds(a, span)], nback_in.at[h, pl.ds(a, span)], NBACK, lax.rem(me - o + n, n)).start()

    @pl.when(mine)
    def _():
        wait_in(part_in.at[pl.ds(0, n - 1)], PART)
        part_in[pl.ds(me, 1)] = part_out[pl.ds(my_block, 1)]

    hot_agg = part_in[...].astype(jnp.float32).sum(axis=0).astype(bf)
    hhid_out[...] = dot(hot_agg, n_other)
    send3 = to_core(hhid_out, hhid_in, HIDH)
    send3.start()
    hot_own = dot(hot_agg, n_own)

    send3.wait_recv()
    hot_lat = silu(hot_own + hhid_in[...]).astype(bf)
    hprj_out[...] = dot(hot_lat, w_other)
    send4 = to_core(hprj_out, hprj_in, PRJH)
    send4.start()
    hot_prj = dot(hot_lat, w_own)

    @pl.when(mine)
    def _():
        wait_in(emb_in.at[pl.ds(0, n - 1)], EMB)
        emb_in[pl.ds(me, 1)] = emb_out[pl.ds(my_block, 1)]

    send4.wait_recv()
    hot_out[...] = (hot_prj + hprj_in[...] + emb_in[hot].astype(jnp.float32)).astype(bf)

    @pl.when(mine)
    def _():
        each_peer(lambda peer: to_graph(hot_out, hot_in.at[my_block], HOT, peer).start())

    wait_in(nback_in.at[:, pl.ds(0, 2 * REACH * span)], NBACK)
    total = grid_ref[:, pl.ds(pl.multiple_of(core * quarter, quarter), quarter)].astype(jnp.float32)
    for h in range(2):
        total = total + dot(spread(grid_rows, srcx_ref[h, blocks:]), nback_in[h])
    dec[...] = total
    wait_in(back_in.at[:, pl.ds(0, n - 1)], BACK)
    total = dec[...]
    for h in range(2):
        for j in range(blocks):
            rows = back_in[h, j * (CHUNK // HALF):(j + 1) * (CHUNK // HALF)].reshape(CHUNK, quarter)
            total = total + dot(spread(grid_rows, srcx_ref[h, j:j + 1]), rows)
    dec[...] = total

    @pl.when(mine)
    def _():
        wait_in(hot_in.at[pl.ds(0, owners - 1)], HOT)
        hot_in[pl.ds(my_block, 1)] = hot_out[...].reshape(1, OWN, quarter)

    @pl.when(jnp.logical_not(mine))
    def _():
        wait_in(hot_in, HOT)

    hot_rows = pick_turned(hot_in[...].reshape(mesh_rows, quarter), hot_dst).astype(bf)
    back = lax.dot_general(spread(grid_rows, hot_src), hot_rows, (((1,), (1,)), ((), ())), preferred_element_type=jnp.float32)
    out_ref[...] = (dec[...] + back).astype(bf)

    wait_out(dst_ref.at[pl.ds(0, n - 1)], DST)
    wait_out(base_out.at[pl.ds(0, n - 1)], BASE)
    wait_out(near_out.at[pl.ds(0, 2 * REACH * span)], NEAR)

    @pl.when(mine)
    def _():
        wait_out(emb_out.at[pl.ds(0, owners - 1)], EMB)
        wait_out(part_out.at[pl.ds(0, owners - 1)], PART)
        wait_out(back_out.at[0, pl.ds(0, n - 1)], HOT)

    @pl.when(jnp.logical_not(mine))
    def _():
        wait_out(emb_out, EMB)
        wait_out(part_out, PART)

    to_core(base_in.at[core], base_in.at[core], FWDB).wait_send()
    to_core(near_in.at[core], near_in.at[core], FWDN).wait_send()
    for copy in (send, send2, send3, send4):
        copy.wait_send()
    wait_out(back_out.at[:, pl.ds(0, n - 1)], BACK)
    wait_out(nback_out.at[:, pl.ds(0, 2 * REACH * span)], NBACK)


def cap_near(capacity):
    return (capacity - KEEP) // 2


def lay_out(table, take, mark):
    high = jnp.floor(table * (1.0 / 32.0))
    low = table - 32.0 * high
    dot = functools.partial(jnp.dot, preferred_element_type=jnp.float32)
    moved = 32.0 * dot(high.astype(jnp.bfloat16), take) + dot(low.astype(jnp.bfloat16), take)
    group = mark.shape[0]
    moved = moved.reshape(table.shape[0] // group, group, take.shape[1])
    return (moved * mark[None]).sum(axis=1).astype(jnp.int32) - 1


def base_layout(capacity, h):
    shape = (capacity, CHUNK)
    lane = lax.broadcasted_iota(jnp.int32, shape, 1)
    slot = lax.broadcasted_iota(jnp.int32, shape, 0)
    take = jnp.where(slot == h * HALF + (lane & (HALF - 1)), 1.0, 0.0).astype(jnp.bfloat16)
    group = CHUNK // HALF
    lane = lax.broadcasted_iota(jnp.int32, (group, CHUNK), 1)
    row = lax.broadcasted_iota(jnp.int32, (group, CHUNK), 0)
    return take, jnp.where(row * HALF <= lane, 1.0, 0.0) * jnp.where(lane < row * HALF + HALF, 1.0, 0.0)


def near_layout(capacity, h):
    span = cap_near(capacity)
    count = 2 * REACH + 1
    shape = (capacity, NEAR_ROWS)
    lane = lax.broadcasted_iota(jnp.int32, shape, 1)
    slot = lax.broadcasted_iota(jnp.int32, shape, 0)
    within = lane
    for i in range(1, count + 1):
        within = within - jnp.where(lane >= i * span, span, 0)
    take = jnp.where(slot == KEEP + h * span + within, 1.0, 0.0).astype(jnp.bfloat16)
    lane = lax.broadcasted_iota(jnp.int32, (8, NEAR_ROWS), 1)
    row = lax.broadcasted_iota(jnp.int32, (8, NEAR_ROWS), 0)
    inside = jnp.where(row * span <= lane, 1.0, 0.0) * jnp.where(lane < row * span + span, 1.0, 0.0)
    return take, inside * jnp.where(row < count, 1.0, 0.0)


def compact(hot, grid_state, w_src, bias_src, mesh_embed, w_node, w_dec, slot_src, slot_dst, slot_count):
    n = lax.axis_size("graph")
    capacity = slot_src.shape[2]
    grid_rows, width = grid_state.shape
    mesh_rows, half = mesh_embed.shape
    quarter = width // 2
    owners = mesh_rows // OWN
    bf, f32 = jnp.bfloat16, jnp.float32
    vm = pltpu.VMEM
    return pl.pallas_call(
        functools.partial(step_kernel, n),
        out_shape=jax.ShapeDtypeStruct((grid_rows, quarter), bf),
        in_specs=[pl.BlockSpec(memory_space=pltpu.SMEM)] + [pl.BlockSpec(memory_space=pl.ANY)] * 9,
        out_specs=pl.BlockSpec(memory_space=vm),
        scratch_shapes=[
            vm((grid_rows, width), bf), vm(w_src.shape, bf), vm((1, half), f32), vm((mesh_rows, half), bf), vm(w_node.shape, bf),
            vm(w_dec.shape, bf), vm(slot_src.shape, jnp.int32), vm(slot_dst.shape, jnp.int32), vm(slot_count.shape, jnp.int32),
            vm((n, capacity), f32), vm((n, capacity), f32),
            vm((2, n * HALF // CHUNK + 1, CHUNK), jnp.int32), vm((2, n * HALF // CHUNK + 1, CHUNK), jnp.int32),
            vm((n, HALF, width), bf), vm((NEAR_ROWS, width), bf),
            vm((2, n, HALF, width), bf), vm((2, NEAR_ROWS, width), bf),
            vm((n, 1, capacity), jnp.int32), vm((n, OWN, quarter), bf), vm((owners, OWN, quarter), bf), vm((mesh_rows, quarter), bf),
            vm((owners, OWN, half), bf), vm((n, OWN, half), bf),
            vm((mesh_rows, half), f32),
            vm((mesh_rows, half), bf), vm((mesh_rows, half), bf),
            vm((mesh_rows, quarter), bf), vm((mesh_rows, quarter), bf), vm((mesh_rows, quarter), bf),
            vm((2, n, HALF, quarter), bf), vm((2, NEAR_ROWS, quarter), bf),
            vm((2, n, HALF, quarter), bf), vm((2, NEAR_ROWS, quarter), bf),
            vm((OWN, quarter), bf), vm((owners, OWN, quarter), bf),
            vm((grid_rows, quarter), f32),
            vm((OWN, half), f32), vm((OWN, half), f32), vm((OWN, quarter), f32), vm((OWN, quarter), f32),
            pltpu.SemaphoreType.DMA((9,)), pltpu.SemaphoreType.DMA((SEMS,)), pltpu.SemaphoreType.DMA((SEMS,)),
        ],
        compiler_params=pltpu.CompilerParams(collective_id=0, has_side_effects=True, vmem_limit_bytes=48 * 1024 * 1024),
    )(hot, grid_state, w_src, bias_src[None, :], mesh_embed, w_node, w_dec, slot_src, slot_dst, slot_count)


def on_device(grid_state, w_src, bias_src, mesh_embed, w_node, w_dec, slot_src, slot_dst, slot_count):
    args = (grid_state, w_src, bias_src, mesh_embed, w_node, w_dec, slot_src, slot_dst, slot_count)
    n = slot_count.shape[0]
    apart = jnp.abs(jnp.arange(n)[:, None] - jnp.arange(n)[None, :])
    far = jnp.minimum(apart, n - apart) > REACH
    over = far & (slot_count > KEEP)
    column = jnp.broadcast_to(jnp.arange(n, dtype=jnp.int32)[None, :], (n, n))
    last = jnp.max(jnp.where(over, column, 0))
    first = jnp.min(jnp.where(over, column, n))
    fits = last <= first
    hot = last.reshape(1)
    return lax.cond(fits, lambda: compact(hot, *args), lambda: dense(*args))


def solution(mesh):
    placed = (
        P(("member", "graph"), None),
        P(None, "chan"),
        P("chan"),
        P("graph", "chan"),
        P("chan", None),
        P("chan", None),
        P("graph", None, None),
        P(None, "graph", None),
        P(),
    )
    return jax.shard_map(
        on_device,
        mesh=mesh,
        in_specs=placed,
        out_specs=P(("member", "graph"), "chan"),
        check_vma=False,
    )
```

```python
import functools
import math

import jax
import jax.numpy as jnp
from jax import lax
from jax.experimental import pallas as pl
from jax.experimental.pallas import tpu as pltpu
from jax.sharding import PartitionSpec as P

MESH_ID = pl.DeviceIdType.MESH
KEEP = 32
HALF = KEEP // 2
GROUP = 7
SEMS = 15
REACH = 2
OWN = 16
NEAR_ROWS = 256
CHUNK = 256

def split_up(value, dim, count):
    lengths = value.shape
    parts = value.reshape(*lengths[:dim], count, lengths[dim] // count, *lengths[dim + 1 :])
    return jnp.moveaxis(parts, dim, 0)


def sum_at_owner(value, axis, dim):
    parts = split_up(value, dim, lax.axis_size(axis))
    arrived = lax.all_to_all(parts, axis, split_axis=0, concat_axis=0, tiled=True)
    return arrived.sum(axis=0)


def edge_network(source_rows, w_src, bias_src):
    return jax.nn.silu(
        jnp.dot(source_rows, w_src, preferred_element_type=jnp.float32) + bias_src
    ).astype(jnp.bfloat16)


def segment_rows(values, indices, usable, row_count):
    slot_total = values.shape[0]
    width = values.shape[1]
    block_len = math.gcd(slot_total, 2048)
    block_count = slot_total // block_len
    targets = jnp.where(usable, indices, -1).reshape(block_count, block_len)
    pieces = values.reshape(block_count, block_len, width)
    row_ids = jnp.arange(row_count, dtype=jnp.int32)

    def add_block(summed, scan_item):
        row_target, piece_vals = scan_item
        one_hot = (row_ids[:, None] == row_target[None, :]).astype(jnp.bfloat16)
        return (summed + jnp.dot(one_hot, piece_vals, preferred_element_type=jnp.float32), None)

    result, unused = lax.scan(
        add_block, jnp.zeros((row_count, width), jnp.float32), (targets, pieces)
    )
    return result


def dense(
    grid_state, w_src, bias_src, mesh_embed, w_node, w_dec, slot_src, slot_dst, slot_count
):
    peers = lax.axis_size("graph")
    own_index = lax.axis_index("graph")
    core_index = lax.axis_index("chan")
    capacity = slot_src.shape[2]
    positions = jnp.arange(capacity, dtype=jnp.int32)
    grid_rows = grid_state.shape[0]
    mesh_rows = mesh_embed.shape[0]
    sent_counts = lax.dynamic_slice_in_dim(slot_count, own_index, 1, 0)[0]
    recv_counts = lax.dynamic_slice_in_dim(slot_count, own_index, 1, 1)[:, 0]
    half_slots = capacity // 2
    chosen = lax.dynamic_slice_in_dim(slot_src[0], core_index * half_slots, half_slots, 1)
    picked = jnp.take(grid_state, chosen.reshape(-1), axis=0).reshape(
        peers, half_slots, grid_state.shape[1]
    )
    arrived = lax.all_to_all(picked, "graph", split_axis=0, concat_axis=0, tiled=True)
    partner = lax.ppermute(arrived, "chan", [(0, 1), (1, 0)])
    joined = jnp.where(
        core_index == 0,
        jnp.concatenate([arrived, partner], axis=1),
        jnp.concatenate([partner, arrived], axis=1),
    )
    messages = edge_network(joined.reshape(peers * capacity, grid_state.shape[1]), w_src, bias_src)
    arrive_ok = (positions[None, :] < recv_counts[:, None]).reshape(-1)
    dst_rows = slot_dst[:, 0, :].reshape(-1)
    aggregate = segment_rows(messages, dst_rows, arrive_ok, mesh_rows)
    partial_hidden = jnp.dot(
        aggregate.astype(jnp.bfloat16), w_node, preferred_element_type=jnp.float32
    )
    hidden_pre = sum_at_owner(partial_hidden, "chan", 1)
    latent = (mesh_embed.astype(jnp.float32) + jax.nn.silu(hidden_pre)).astype(jnp.bfloat16)
    partial_proj = jnp.dot(latent, w_dec, preferred_element_type=jnp.float32)
    projected = sum_at_owner(partial_proj, "chan", 1).astype(jnp.bfloat16)
    returned = jnp.take(projected, dst_rows, axis=0).reshape(peers, capacity, projected.shape[1])
    came_back = lax.all_to_all(returned, "graph", split_axis=0, concat_axis=0, tiled=True).reshape(
        peers * capacity, projected.shape[1]
    )
    send_ok = (positions[None, :] < sent_counts[:, None]).reshape(-1)
    decoded = segment_rows(came_back, slot_src[0].reshape(-1), send_ok, grid_rows)
    width_half = decoded.shape[1]
    own_cols = lax.dynamic_slice_in_dim(grid_state, core_index * width_half, width_half, 1)
    return (own_cols.astype(jnp.float32) + decoded).astype(jnp.bfloat16)


def torus(n):
    wide = 1 << (n.bit_length() // 2)
    return n // wide, wide


def visit_order(n):
    tall, wide = torus(n)
    offsets = [(r, c) for r in range(tall) for c in range(wide)][1:]
    offsets.sort(key=lambda o: min(o[0], tall - o[0]) + min(o[1], wide - o[1]))
    return [offsets[i // 2] if i % 2 == 0 else offsets[-1 - i // 2] for i in range(n - 1)]


def silu(v):
    h = 0.5 * v
    return h + h * jnp.tanh(h)


def pick_turned(table, idx):
    rows = table.shape[0]
    hot = jnp.where(
        lax.broadcasted_iota(jnp.int32, (rows, idx.shape[1]), 0) == idx, 1.0, 0.0
    ).astype(jnp.bfloat16)
    return lax.dot_general(table, hot, (((0,), (0,)), ((), ())), preferred_element_type=jnp.float32)


def spread(rows, idx):
    return jnp.where(
        lax.broadcasted_iota(jnp.int32, (rows, idx.shape[1]), 0) == idx, 1.0, 0.0
    ).astype(jnp.bfloat16)


def step_kernel(
    n, grid_hbm, wsrc_hbm, bias_hbm, embed_hbm, wnode_hbm, wdec_hbm, src_hbm, dst_hbm, count_hbm, out_ref, fits_ref,
    grid_ref, wsrc_ref, bias_ref, embed_ref, wnode_ref, wdec_ref, src_ref, dst_ref, count_ref,
    src_live, dst_live, srcx_ref, dstx_ref,
    base_out, near_out, base_in, near_in, dst_in, emb_in, emb_out, emb_half, part_out, part_in,
    acc, hid_out, hid_in, prj_out, prj_in, prj_bf, back_out, nback_out, back_in, nback_in, hot_out, hot_in, dec,
    hhid_out, hhid_in, hprj_out, hprj_in, hot_to, hot_from,
    lsem, ssem, rsem,
):
    me = lax.axis_index("graph")
    core = lax.axis_index("chan")
    other = 1 - core
    grid_rows = grid_ref.shape[0]
    mesh_rows = embed_ref.shape[0]
    owners = mesh_rows // OWN
    span = cap_near(dst_ref.shape[2])
    used = (2 * REACH + 1) * span
    half = hid_out.shape[1]
    quarter = prj_out.shape[1]
    bf = jnp.bfloat16
    dot = functools.partial(jnp.dot, preferred_element_type=jnp.float32)

    pairs = (
        (src_hbm, src_ref), (dst_hbm, dst_ref), (count_hbm, count_ref), (grid_hbm, grid_ref), (embed_hbm, embed_ref),
        (wdec_hbm, wdec_ref), (wsrc_hbm, wsrc_ref), (bias_hbm, bias_ref), (wnode_hbm, wnode_ref),
    )
    SRC, DSTS, COUNT, GRID, EMBED, WDEC, WSRC, BIAS, WNODE = (
        pltpu.make_async_copy(x, y, lsem.at[i]) for i, (x, y) in enumerate(pairs))
    for copy in (SRC, DSTS, COUNT, GRID, EMBED, WDEC, WSRC, BIAS, WNODE):
        copy.start()

    tall, wide = torus(n)
    codes = [r * 2 * wide + c for r, c in visit_order(n)]
    groups = [codes[i:i + GROUP] for i in range(0, n - 1, GROUP)]
    spot = 2 * wide * (me // wide) + lax.rem(me, wide) + core * (2 * wide * tall + wide)
    turn = 1 - 2 * core

    def each_peer(visit):
        @pl.loop(0, len(groups))
        def _(g):
            for part in (range(0, 4), range(4, GROUP)):
                packed = jnp.int32(0)
                for i, group in enumerate(groups):
                    packed = jnp.where(g == i, sum(group[k] << (7 * j) for j, k in enumerate(part)), packed)
                for j in range(len(part)):
                    code = lax.shift_right_logical(packed, jnp.int32(7 * j)) & 127
                    at = spot + turn * code
                    visit((lax.shift_right_logical(at, jnp.int32(1)) & ((tall - 1) * wide)) + (at & (wide - 1)))

    per_row = owners // tall

    def seat(shard):
        r = lax.shift_right_logical(shard, jnp.int32(wide.bit_length() - 1))
        rank = (shard + 3 * r) & (wide - 1)
        return rank < per_row, r * per_row + rank

    mine, my_block = seat(me)
    barrier = pltpu.get_barrier_semaphore()
    each_peer(lambda peer: pl.semaphore_signal(barrier, inc=1, device_id={"graph": peer}, device_id_type=MESH_ID))
    pl.semaphore_signal(barrier, inc=1, device_id={"chan": other}, device_id_type=MESH_ID)

    def to_graph(src, dst, k, peer):
        return pltpu.make_async_remote_copy(
            src_ref=src, dst_ref=dst, send_sem=ssem.at[k], recv_sem=rsem.at[k],
            device_id={"graph": peer}, device_id_type=MESH_ID)

    def to_core(src, dst, k):
        return pltpu.make_async_remote_copy(
            src_ref=src, dst_ref=dst, send_sem=ssem.at[k], recv_sem=rsem.at[k],
            device_id={"chan": other}, device_id_type=MESH_ID)

    def wait_in(ref, k):
        to_graph(ref, ref, k, me).wait_recv()

    def wait_out(ref, k):
        to_graph(ref, ref, k, me).wait_send()

    DST, EMB, BASE, NEAR, PART, FWDB, FWDN, HID, PRJ, BACK, NBACK, HOT, PRJ0, HIDH, PRJH = range(SEMS)

    blocks = (n * HALF) // CHUNK
    capacity = dst_ref.shape[2]
    SRC.wait()
    DSTS.wait()
    COUNT.wait()
    with jax.named_scope("index"):
        ids = lax.broadcasted_iota(jnp.int32, (n, n), 0)
        cols = lax.broadcasted_iota(jnp.int32, (n, n), 1)
        counts = count_ref[...]
        apart = jnp.abs(ids - cols)
        far_counts = jnp.where(jnp.minimum(apart, n - apart) > REACH, counts, 0)
        hot = jnp.max(jnp.where(far_counts > KEEP, cols, 0))
        first = jnp.min(jnp.where(far_counts > KEEP, cols, n))
        fits_ref[0] = jnp.where(hot <= first, 1, 0)
        sent = jnp.where(ids == me, counts, 0).sum(axis=0, keepdims=True)
        sent = jnp.where(ids == cols, sent, 0).sum(axis=1, keepdims=True)
        came = jnp.where(cols == me, counts, 0).sum(axis=1, keepdims=True)
        pos = lax.broadcasted_iota(jnp.int32, (n, capacity), 1)
        src_all = jnp.where(pos < sent, src_ref[0] + 1, 0).astype(jnp.float32)
        src_live[...] = src_all
        came = jnp.where(me == hot, 0, came)
        dst_all = jnp.where(pos < came, dst_ref[:, 0, :] + 1, 0).astype(jnp.float32)
        dst_live[...] = dst_all
        rows_id = lax.broadcasted_iota(jnp.int32, (n, capacity), 0)
        src_all = jnp.where(rows_id == hot, 0.0, src_all)
        near_id = lax.broadcasted_iota(jnp.int32, (8, capacity), 0)
        near_src = jnp.zeros((8, capacity), jnp.float32)
        near_dst = jnp.zeros((8, capacity), jnp.float32)
        for o in range(-REACH, REACH + 1):
            to = lax.rem(me + o + n, n)
            row = jnp.where(to == hot, 0.0, src_live[pl.ds(to, 1)])
            near_src = jnp.where(near_id == o + REACH, row, near_src)
            near_dst = jnp.where(near_id == o + REACH, dst_live[pl.ds(lax.rem(me - o + n, n), 1)], near_dst)
        for h in range(2):
            base = base_layout(capacity, h)
            srcx_ref[h, 0:blocks] = lay_out(src_all, *base)
            dstx_ref[h, 0:blocks] = lay_out(dst_all, *base)
            near = near_layout(capacity, h)
            srcx_ref[h, blocks:] = lay_out(near_src, *near)[:, 0:CHUNK]
            dstx_ref[h, blocks:] = lay_out(near_dst, *near)[:, 0:CHUNK]

    GRID.wait()

    for j in range(blocks):
        rows = pick_turned(grid_ref[...], srcx_ref[core, j:j + 1]).T.astype(bf)
        base_out[j * (CHUNK // HALF):(j + 1) * (CHUNK // HALF)] = rows.reshape(CHUNK // HALF, HALF, rows.shape[1])

    near_out[...] = pick_turned(grid_ref[...], srcx_ref[core, blocks:]).T.astype(bf)
    near_in[core, used:, :] = jnp.zeros((NEAR_ROWS - used, near_in.shape[2]), bf)

    pl.semaphore_wait(barrier, n)
    each_peer(lambda peer: to_graph(dst_ref.at[peer], dst_in.at[me], DST, peer).start())
    for o in range(-REACH, REACH + 1):
        rows = pl.ds((o + REACH) * span, span)
        if o == 0:
            near_in[core, (o + REACH) * span:(o + REACH + 1) * span] = near_out[(o + REACH) * span:(o + REACH + 1) * span]
        else:
            to_graph(near_out.at[rows], near_in.at[core, rows], NEAR, lax.rem(me + o + n, n)).start()
    each_peer(lambda peer: to_graph(base_out.at[peer], base_in.at[core, me], BASE, peer).start())
    base_in[core, pl.ds(me, 1)] = base_out[pl.ds(me, 1)]
    dst_in[pl.ds(me, 1)] = dst_ref[pl.ds(me, 1)]

    EMBED.wait()
    WDEC.wait()
    w_other = wdec_ref[:, pl.ds(pl.multiple_of(other * quarter, quarter), quarter)]
    w_own = wdec_ref[:, pl.ds(pl.multiple_of(core * quarter, quarter), quarter)]
    prj_out[...] = dot(embed_ref[...], w_other).astype(bf)
    send0 = to_core(prj_out, emb_half, PRJ0)
    send0.start()
    WSRC.wait()
    BIAS.wait()
    hot_src = src_live[pl.ds(hot, 1)].astype(jnp.int32) - 1
    msgs = silu(dot(pick_turned(grid_ref[...], hot_src).T.astype(bf), wsrc_ref[...]) + bias_ref[...]).astype(bf)
    emb_own = dot(embed_ref[...], w_own)
    send0.wait_recv()
    emb_out[...] = (emb_own + emb_half[...].astype(jnp.float32)).astype(bf).reshape(owners, OWN, quarter)

    wait_in(dst_in.at[pl.ds(0, n - 1)], DST)
    hot_dst = jnp.where(hot_src >= 0, dst_in[hot], -1)
    part_out[...] = dot(spread(mesh_rows, hot_dst), msgs).astype(bf).reshape(owners, OWN, half)

    def to_owner(copy_to):
        def visit(peer):
            owns, block = seat(peer)

            @pl.when(owns)
            def _():
                copy_to(peer, block).start()
        return visit

    each_peer(to_owner(lambda peer, block: to_graph(part_out.at[block], part_in.at[me], PART, peer)))
    each_peer(to_owner(lambda peer, block: to_graph(emb_out.at[block], emb_in.at[me], EMB, peer)))

    wait_in(base_in.at[core, pl.ds(0, n - 1)], BASE)
    to_core(base_in.at[core], base_in.at[core], FWDB).start()
    wait_in(near_in.at[core, pl.ds(0, 2 * REACH * span)], NEAR)
    to_core(near_in.at[core], near_in.at[core], FWDN).start()
    def share(rows, idx):
        m = silu(dot(rows, wsrc_ref[...]) + bias_ref[...]).astype(bf)
        return dot(spread(mesh_rows, idx), m)

    def half_sum(h):
        total = share(near_in[h], dstx_ref[h, blocks:])
        for j in range(blocks):
            rows = base_in[h, j * (CHUNK // HALF):(j + 1) * (CHUNK // HALF)].reshape(CHUNK, base_in.shape[3])
            total = total + share(rows, dstx_ref[h, j:j + 1])
        return total

    acc[...] = half_sum(core)
    to_core(base_in.at[other], base_in.at[other], FWDB).wait_recv()
    to_core(near_in.at[other], near_in.at[other], FWDN).wait_recv()

    WNODE.wait()
    n_other = wnode_ref[:, pl.ds(pl.multiple_of(other * half, half), half)]
    n_own = wnode_ref[:, pl.ds(pl.multiple_of(core * half, half), half)]
    agg = (acc[...] + half_sum(other)).astype(bf)
    hid_out[...] = dot(agg, n_other).astype(bf)
    send = to_core(hid_out, hid_in, HID)
    send.start()
    own = dot(agg, n_own)
    send0.wait_send()
    send.wait_recv()
    lat = (embed_ref[...].astype(jnp.float32) + silu(own + hid_in[...].astype(jnp.float32))).astype(bf)
    prj_out[...] = dot(lat, w_other).astype(bf)
    send2 = to_core(prj_out, prj_in, PRJ)
    send2.start()
    own_p = dot(lat, w_own)

    send2.wait_recv()
    prj_bf[...] = (own_p + prj_in[...].astype(jnp.float32)).astype(bf)
    for h in range(2):
        for j in range(blocks):
            rows = pick_turned(prj_bf[...], dstx_ref[h, j:j + 1]).T.astype(bf)
            back_out[h, j * (CHUNK // HALF):(j + 1) * (CHUNK // HALF)] = rows.reshape(CHUNK // HALF, HALF, quarter)
        back_in[h, pl.ds(me, 1)] = back_out[h, pl.ds(me, 1)]

    each_peer(lambda peer: to_graph(back_out.at[:, peer], back_in.at[:, me], BACK, peer).start())
    for h in range(2):
        nback_out[h] = pick_turned(prj_bf[...], dstx_ref[h, blocks:]).T.astype(bf)
        nback_in[h, used:, :] = jnp.zeros((NEAR_ROWS - used, quarter), bf)
        for o in range(-REACH, REACH + 1):
            a = (o + REACH) * span
            if o == 0:
                nback_in[h, a:a + span] = nback_out[h, a:a + span]
            else:
                to_graph(nback_out.at[h, pl.ds(a, span)], nback_in.at[h, pl.ds(a, span)], NBACK, lax.rem(me - o + n, n)).start()

    @pl.when(mine)
    def _():
        wait_in(part_in.at[pl.ds(0, n - 1)], PART)
        part_in[pl.ds(me, 1)] = part_out[pl.ds(my_block, 1)]

    hot_agg = part_in[...].astype(jnp.float32).sum(axis=0).astype(bf)
    hhid_out[...] = dot(hot_agg, n_other)
    send3 = to_core(hhid_out, hhid_in, HIDH)
    send3.start()
    hot_own = dot(hot_agg, n_own)

    send3.wait_recv()
    hot_lat = silu(hot_own + hhid_in[...]).astype(bf)
    hprj_out[...] = dot(hot_lat, w_other)
    send4 = to_core(hprj_out, hprj_in, PRJH)
    send4.start()
    hot_prj = dot(hot_lat, w_own)

    @pl.when(mine)
    def _():
        wait_in(emb_in.at[pl.ds(0, n - 1)], EMB)
        emb_in[pl.ds(me, 1)] = emb_out[pl.ds(my_block, 1)]

    send4.wait_recv()
    hot_out[...] = (hot_prj + hprj_in[...] + emb_in[hot].astype(jnp.float32)).astype(bf)

    @pl.when(mine)
    def _():
        each_peer(lambda peer: to_graph(hot_out, hot_in.at[my_block], HOT, peer).start())

    wait_in(nback_in.at[:, pl.ds(0, 2 * REACH * span)], NBACK)
    total = grid_ref[:, pl.ds(pl.multiple_of(core * quarter, quarter), quarter)].astype(jnp.float32)
    for h in range(2):
        total = total + dot(spread(grid_rows, srcx_ref[h, blocks:]), nback_in[h])
    dec[...] = total
    wait_in(back_in.at[:, pl.ds(0, n - 1)], BACK)
    total = dec[...]
    for h in range(2):
        for j in range(blocks):
            rows = back_in[h, j * (CHUNK // HALF):(j + 1) * (CHUNK // HALF)].reshape(CHUNK, quarter)
            total = total + dot(spread(grid_rows, srcx_ref[h, j:j + 1]), rows)
    dec[...] = total

    hot_to[...] = spread(grid_rows, hot_src)
    hot_from[...] = spread(mesh_rows, hot_dst)

    @pl.when(mine)
    def _():
        wait_in(hot_in.at[pl.ds(0, owners - 1)], HOT)
        hot_in[pl.ds(my_block, 1)] = hot_out[...].reshape(1, OWN, quarter)

    @pl.when(jnp.logical_not(mine))
    def _():
        wait_in(hot_in, HOT)

    hot_rows = lax.dot_general(
        hot_in[...].reshape(mesh_rows, quarter), hot_from[...], (((0,), (0,)), ((), ())), preferred_element_type=jnp.float32
    ).astype(bf)
    back = lax.dot_general(hot_to[...], hot_rows, (((1,), (1,)), ((), ())), preferred_element_type=jnp.float32)
    out_ref[...] = (dec[...] + back).astype(bf)

    wait_out(dst_ref.at[pl.ds(0, n - 1)], DST)
    wait_out(base_out.at[pl.ds(0, n - 1)], BASE)
    wait_out(near_out.at[pl.ds(0, 2 * REACH * span)], NEAR)

    @pl.when(mine)
    def _():
        wait_out(emb_out.at[pl.ds(0, owners - 1)], EMB)
        wait_out(part_out.at[pl.ds(0, owners - 1)], PART)
        wait_out(back_out.at[0, pl.ds(0, n - 1)], HOT)

    @pl.when(jnp.logical_not(mine))
    def _():
        wait_out(emb_out, EMB)
        wait_out(part_out, PART)

    to_core(base_in.at[core], base_in.at[core], FWDB).wait_send()
    to_core(near_in.at[core], near_in.at[core], FWDN).wait_send()
    for copy in (send, send2, send3, send4):
        copy.wait_send()
    wait_out(back_out.at[:, pl.ds(0, n - 1)], BACK)
    wait_out(nback_out.at[:, pl.ds(0, 2 * REACH * span)], NBACK)


def cap_near(capacity):
    return (capacity - KEEP) // 2


def lay_out(table, take, mark):
    high = jnp.floor(table * (1.0 / 32.0))
    low = table - 32.0 * high
    dot = functools.partial(jnp.dot, preferred_element_type=jnp.float32)
    moved = 32.0 * dot(high.astype(jnp.bfloat16), take) + dot(low.astype(jnp.bfloat16), take)
    group = mark.shape[0]
    moved = moved.reshape(table.shape[0] // group, group, take.shape[1])
    return (moved * mark[None]).sum(axis=1).astype(jnp.int32) - 1


def base_layout(capacity, h):
    shape = (capacity, CHUNK)
    lane = lax.broadcasted_iota(jnp.int32, shape, 1)
    slot = lax.broadcasted_iota(jnp.int32, shape, 0)
    take = jnp.where(slot == h * HALF + (lane & (HALF - 1)), 1.0, 0.0).astype(jnp.bfloat16)
    group = CHUNK // HALF
    lane = lax.broadcasted_iota(jnp.int32, (group, CHUNK), 1)
    row = lax.broadcasted_iota(jnp.int32, (group, CHUNK), 0)
    return take, jnp.where(row * HALF <= lane, 1.0, 0.0) * jnp.where(lane < row * HALF + HALF, 1.0, 0.0)


def near_layout(capacity, h):
    span = cap_near(capacity)
    count = 2 * REACH + 1
    shape = (capacity, NEAR_ROWS)
    lane = lax.broadcasted_iota(jnp.int32, shape, 1)
    slot = lax.broadcasted_iota(jnp.int32, shape, 0)
    within = lane
    for i in range(1, count + 1):
        within = within - jnp.where(lane >= i * span, span, 0)
    take = jnp.where(slot == KEEP + h * span + within, 1.0, 0.0).astype(jnp.bfloat16)
    lane = lax.broadcasted_iota(jnp.int32, (8, NEAR_ROWS), 1)
    row = lax.broadcasted_iota(jnp.int32, (8, NEAR_ROWS), 0)
    inside = jnp.where(row * span <= lane, 1.0, 0.0) * jnp.where(lane < row * span + span, 1.0, 0.0)
    return take, inside * jnp.where(row < count, 1.0, 0.0)


def compact(grid_state, w_src, bias_src, mesh_embed, w_node, w_dec, slot_src, slot_dst, slot_count):
    n = lax.axis_size("graph")
    capacity = slot_src.shape[2]
    grid_rows, width = grid_state.shape
    mesh_rows, half = mesh_embed.shape
    quarter = width // 2
    owners = mesh_rows // OWN
    bf, f32 = jnp.bfloat16, jnp.float32
    vm = pltpu.VMEM
    return pl.pallas_call(
        functools.partial(step_kernel, n),
        out_shape=(jax.ShapeDtypeStruct((grid_rows, quarter), bf), jax.ShapeDtypeStruct((1,), jnp.int32)),
        in_specs=[pl.BlockSpec(memory_space=pl.ANY)] * 9,
        out_specs=(pl.BlockSpec(memory_space=vm), pl.BlockSpec(memory_space=pltpu.SMEM)),
        scratch_shapes=[
            vm((grid_rows, width), bf), vm(w_src.shape, bf), vm((1, half), f32), vm((mesh_rows, half), bf), vm(w_node.shape, bf),
            vm(w_dec.shape, bf), vm(slot_src.shape, jnp.int32), vm(slot_dst.shape, jnp.int32), vm(slot_count.shape, jnp.int32),
            vm((n, capacity), f32), vm((n, capacity), f32),
            vm((2, n * HALF // CHUNK + 1, CHUNK), jnp.int32), vm((2, n * HALF // CHUNK + 1, CHUNK), jnp.int32),
            vm((n, HALF, width), bf), vm((NEAR_ROWS, width), bf),
            vm((2, n, HALF, width), bf), vm((2, NEAR_ROWS, width), bf),
            vm((n, 1, capacity), jnp.int32), vm((n, OWN, quarter), bf), vm((owners, OWN, quarter), bf), vm((mesh_rows, quarter), bf),
            vm((owners, OWN, half), bf), vm((n, OWN, half), bf),
            vm((mesh_rows, half), f32),
            vm((mesh_rows, half), bf), vm((mesh_rows, half), bf),
            vm((mesh_rows, quarter), bf), vm((mesh_rows, quarter), bf), vm((mesh_rows, quarter), bf),
            vm((2, n, HALF, quarter), bf), vm((2, NEAR_ROWS, quarter), bf),
            vm((2, n, HALF, quarter), bf), vm((2, NEAR_ROWS, quarter), bf),
            vm((OWN, quarter), bf), vm((owners, OWN, quarter), bf),
            vm((grid_rows, quarter), f32),
            vm((OWN, half), f32), vm((OWN, half), f32), vm((OWN, quarter), f32), vm((OWN, quarter), f32),
            vm((grid_rows, capacity), bf), vm((mesh_rows, capacity), bf),
            pltpu.SemaphoreType.DMA((9,)), pltpu.SemaphoreType.DMA((SEMS,)), pltpu.SemaphoreType.DMA((SEMS,)),
        ],
        compiler_params=pltpu.CompilerParams(collective_id=0, has_side_effects=True, vmem_limit_bytes=48 * 1024 * 1024),
    )(grid_state, w_src, bias_src[None, :], mesh_embed, w_node, w_dec, slot_src, slot_dst, slot_count)


def on_device(grid_state, w_src, bias_src, mesh_embed, w_node, w_dec, slot_src, slot_dst, slot_count):
    args = (grid_state, w_src, bias_src, mesh_embed, w_node, w_dec, slot_src, slot_dst, slot_count)
    result, fits = compact(*args)
    return lax.cond(fits[0] > 0, lambda: result, lambda: dense(*args))


def solution(mesh):
    placed = (
        P(("member", "graph"), None),
        P(None, "chan"),
        P("chan"),
        P("graph", "chan"),
        P("chan", None),
        P("chan", None),
        P("graph", None, None),
        P(None, "graph", None),
        P(),
    )
    return jax.shard_map(
        on_device,
        mesh=mesh,
        in_specs=placed,
        out_specs=P(("member", "graph"), "chan"),
        check_vma=False,
    )
```

```python
import functools
import math

import jax
import jax.numpy as jnp
from jax import lax
from jax.experimental import pallas as pl
from jax.experimental.pallas import tpu as pltpu
from jax.sharding import PartitionSpec as P

MESH_ID = pl.DeviceIdType.MESH
KEEP = 32
HALF = KEEP // 2
GROUP = 7
SEMS = 17
REACH = 2
OWN = 16
NEAR_ROWS = 256
CHUNK = 256

def split_up(value, dim, count):
    lengths = value.shape
    parts = value.reshape(*lengths[:dim], count, lengths[dim] // count, *lengths[dim + 1 :])
    return jnp.moveaxis(parts, dim, 0)


def sum_at_owner(value, axis, dim):
    parts = split_up(value, dim, lax.axis_size(axis))
    arrived = lax.all_to_all(parts, axis, split_axis=0, concat_axis=0, tiled=True)
    return arrived.sum(axis=0)


def edge_network(source_rows, w_src, bias_src):
    return jax.nn.silu(
        jnp.dot(source_rows, w_src, preferred_element_type=jnp.float32) + bias_src
    ).astype(jnp.bfloat16)


def segment_rows(values, indices, usable, row_count):
    slot_total = values.shape[0]
    width = values.shape[1]
    block_len = math.gcd(slot_total, 2048)
    block_count = slot_total // block_len
    targets = jnp.where(usable, indices, -1).reshape(block_count, block_len)
    pieces = values.reshape(block_count, block_len, width)
    row_ids = jnp.arange(row_count, dtype=jnp.int32)

    def add_block(summed, scan_item):
        row_target, piece_vals = scan_item
        one_hot = (row_ids[:, None] == row_target[None, :]).astype(jnp.bfloat16)
        return (summed + jnp.dot(one_hot, piece_vals, preferred_element_type=jnp.float32), None)

    result, unused = lax.scan(
        add_block, jnp.zeros((row_count, width), jnp.float32), (targets, pieces)
    )
    return result


def dense(
    grid_state, w_src, bias_src, mesh_embed, w_node, w_dec, slot_src, slot_dst, slot_count
):
    peers = lax.axis_size("graph")
    own_index = lax.axis_index("graph")
    core_index = lax.axis_index("chan")
    capacity = slot_src.shape[2]
    positions = jnp.arange(capacity, dtype=jnp.int32)
    grid_rows = grid_state.shape[0]
    mesh_rows = mesh_embed.shape[0]
    sent_counts = lax.dynamic_slice_in_dim(slot_count, own_index, 1, 0)[0]
    recv_counts = lax.dynamic_slice_in_dim(slot_count, own_index, 1, 1)[:, 0]
    half_slots = capacity // 2
    chosen = lax.dynamic_slice_in_dim(slot_src[0], core_index * half_slots, half_slots, 1)
    picked = jnp.take(grid_state, chosen.reshape(-1), axis=0).reshape(
        peers, half_slots, grid_state.shape[1]
    )
    arrived = lax.all_to_all(picked, "graph", split_axis=0, concat_axis=0, tiled=True)
    partner = lax.ppermute(arrived, "chan", [(0, 1), (1, 0)])
    joined = jnp.where(
        core_index == 0,
        jnp.concatenate([arrived, partner], axis=1),
        jnp.concatenate([partner, arrived], axis=1),
    )
    messages = edge_network(joined.reshape(peers * capacity, grid_state.shape[1]), w_src, bias_src)
    arrive_ok = (positions[None, :] < recv_counts[:, None]).reshape(-1)
    dst_rows = slot_dst[:, 0, :].reshape(-1)
    aggregate = segment_rows(messages, dst_rows, arrive_ok, mesh_rows)
    partial_hidden = jnp.dot(
        aggregate.astype(jnp.bfloat16), w_node, preferred_element_type=jnp.float32
    )
    hidden_pre = sum_at_owner(partial_hidden, "chan", 1)
    latent = (mesh_embed.astype(jnp.float32) + jax.nn.silu(hidden_pre)).astype(jnp.bfloat16)
    partial_proj = jnp.dot(latent, w_dec, preferred_element_type=jnp.float32)
    projected = sum_at_owner(partial_proj, "chan", 1).astype(jnp.bfloat16)
    returned = jnp.take(projected, dst_rows, axis=0).reshape(peers, capacity, projected.shape[1])
    came_back = lax.all_to_all(returned, "graph", split_axis=0, concat_axis=0, tiled=True).reshape(
        peers * capacity, projected.shape[1]
    )
    send_ok = (positions[None, :] < sent_counts[:, None]).reshape(-1)
    decoded = segment_rows(came_back, slot_src[0].reshape(-1), send_ok, grid_rows)
    width_half = decoded.shape[1]
    own_cols = lax.dynamic_slice_in_dim(grid_state, core_index * width_half, width_half, 1)
    return (own_cols.astype(jnp.float32) + decoded).astype(jnp.bfloat16)


def torus(n):
    wide = 1 << (n.bit_length() // 2)
    return n // wide, wide


def visit_order(n):
    tall, wide = torus(n)
    offsets = [(r, c) for r in range(tall) for c in range(wide)][1:]
    offsets.sort(key=lambda o: min(o[0], tall - o[0]) + min(o[1], wide - o[1]))
    return [offsets[i // 2] if i % 2 == 0 else offsets[-1 - i // 2] for i in range(n - 1)]


def silu(v):
    h = 0.5 * v
    return h + h * jnp.tanh(h)


def pick_turned(table, idx):
    rows = table.shape[0]
    hot = jnp.where(
        lax.broadcasted_iota(jnp.int32, (rows, idx.shape[1]), 0) == idx, 1.0, 0.0
    ).astype(jnp.bfloat16)
    return lax.dot_general(table, hot, (((0,), (0,)), ((), ())), preferred_element_type=jnp.float32)


def spread(rows, idx):
    return jnp.where(
        lax.broadcasted_iota(jnp.int32, (rows, idx.shape[1]), 0) == idx, 1.0, 0.0
    ).astype(jnp.bfloat16)


def step_kernel(
    n, grid_hbm, wsrc_hbm, bias_hbm, embed_hbm, wnode_hbm, wdec_hbm, src_hbm, dst_hbm, count_hbm, out_ref, fits_ref,
    grid_ref, wsrc_ref, bias_ref, embed_ref, wnode_ref, wdec_ref, src_ref, dst_ref, count_ref,
    src_live, dst_live, srcx_ref, dstx_ref,
    base_out, near_out, base_in, near_in, dst_in, emb_in, emb_out, emb_half, part_out, part_in,
    acc, hid_out, hid_in, prj_out, prj_in, prj_bf, back_out, nback_out, back_in, nback_in, hot_out, hot_in, dec,
    hhid_out, hhid_in, hprj_out, hprj_in, hot_to, hot_from,
    lsem, ssem, rsem,
):
    me = lax.axis_index("graph")
    core = lax.axis_index("chan")
    other = 1 - core
    grid_rows = grid_ref.shape[0]
    mesh_rows = embed_ref.shape[0]
    owners = mesh_rows // OWN
    span = cap_near(dst_ref.shape[2])
    used = (2 * REACH + 1) * span
    half = hid_out.shape[1]
    quarter = prj_out.shape[1]
    bf = jnp.bfloat16
    dot = functools.partial(jnp.dot, preferred_element_type=jnp.float32)

    pairs = (
        (src_hbm, src_ref), (dst_hbm, dst_ref), (count_hbm, count_ref), (grid_hbm, grid_ref), (embed_hbm, embed_ref),
        (wdec_hbm, wdec_ref), (wsrc_hbm, wsrc_ref), (bias_hbm, bias_ref), (wnode_hbm, wnode_ref),
    )
    SRC, DSTS, COUNT, GRID, EMBED, WDEC, WSRC, BIAS, WNODE = (
        pltpu.make_async_copy(x, y, lsem.at[i]) for i, (x, y) in enumerate(pairs))
    for copy in (SRC, DSTS, COUNT, GRID, EMBED, WDEC, WSRC, BIAS, WNODE):
        copy.start()

    tall, wide = torus(n)
    codes = [r * 2 * wide + c for r, c in visit_order(n)]
    groups = [codes[i:i + GROUP] for i in range(0, n - 1, GROUP)]
    spot = 2 * wide * (me // wide) + lax.rem(me, wide) + core * (2 * wide * tall + wide)
    turn = 1 - 2 * core

    def each_peer(visit):
        @pl.loop(0, len(groups))
        def _(g):
            for part in (range(0, 4), range(4, GROUP)):
                packed = jnp.int32(0)
                for i, group in enumerate(groups):
                    packed = jnp.where(g == i, sum(group[k] << (7 * j) for j, k in enumerate(part)), packed)
                for j in range(len(part)):
                    code = lax.shift_right_logical(packed, jnp.int32(7 * j)) & 127
                    at = spot + turn * code
                    visit((lax.shift_right_logical(at, jnp.int32(1)) & ((tall - 1) * wide)) + (at & (wide - 1)))

    per_row = owners // tall

    def seat(shard):
        r = lax.shift_right_logical(shard, jnp.int32(wide.bit_length() - 1))
        rank = (shard + 3 * r) & (wide - 1)
        return rank < per_row, r * per_row + rank

    mine, my_block = seat(me)
    barrier = pltpu.get_barrier_semaphore()
    each_peer(lambda peer: pl.semaphore_signal(barrier, inc=1, device_id={"graph": peer}, device_id_type=MESH_ID))
    pl.semaphore_signal(barrier, inc=1, device_id={"chan": other}, device_id_type=MESH_ID)

    def to_graph(src, dst, k, peer):
        return pltpu.make_async_remote_copy(
            src_ref=src, dst_ref=dst, send_sem=ssem.at[k], recv_sem=rsem.at[k],
            device_id={"graph": peer}, device_id_type=MESH_ID)

    def to_core(src, dst, k):
        return pltpu.make_async_remote_copy(
            src_ref=src, dst_ref=dst, send_sem=ssem.at[k], recv_sem=rsem.at[k],
            device_id={"chan": other}, device_id_type=MESH_ID)

    def wait_in(ref, k):
        to_graph(ref, ref, k, me).wait_recv()

    def wait_out(ref, k):
        to_graph(ref, ref, k, me).wait_send()

    DST, EMB, BASE, NEAR, PART, FWDB, FWDN, HID, PRJ, BACK, NBACK, HOT, PRJ0, HIDH, PRJH, HID1, PRJ1 = range(SEMS)

    blocks = (n * HALF) // CHUNK
    capacity = dst_ref.shape[2]
    SRC.wait()
    DSTS.wait()
    COUNT.wait()
    with jax.named_scope("index"):
        ids = lax.broadcasted_iota(jnp.int32, (n, n), 0)
        cols = lax.broadcasted_iota(jnp.int32, (n, n), 1)
        counts = count_ref[...]
        apart = jnp.abs(ids - cols)
        far_counts = jnp.where(jnp.minimum(apart, n - apart) > REACH, counts, 0)
        hot = jnp.max(jnp.where(far_counts > KEEP, cols, 0))
        first = jnp.min(jnp.where(far_counts > KEEP, cols, n))
        fits_ref[0] = jnp.where(hot <= first, 1, 0)
        sent = jnp.where(ids == me, counts, 0).sum(axis=0, keepdims=True)
        sent = jnp.where(ids == cols, sent, 0).sum(axis=1, keepdims=True)
        came = jnp.where(cols == me, counts, 0).sum(axis=1, keepdims=True)
        pos = lax.broadcasted_iota(jnp.int32, (n, capacity), 1)
        src_all = jnp.where(pos < sent, src_ref[0] + 1, 0).astype(jnp.float32)
        src_live[...] = src_all
        came = jnp.where(me == hot, 0, came)
        dst_all = jnp.where(pos < came, dst_ref[:, 0, :] + 1, 0).astype(jnp.float32)
        dst_live[...] = dst_all
        rows_id = lax.broadcasted_iota(jnp.int32, (n, capacity), 0)
        src_all = jnp.where(rows_id == hot, 0.0, src_all)
        near_id = lax.broadcasted_iota(jnp.int32, (8, capacity), 0)
        near_src = jnp.zeros((8, capacity), jnp.float32)
        near_dst = jnp.zeros((8, capacity), jnp.float32)
        for o in range(-REACH, REACH + 1):
            to = lax.rem(me + o + n, n)
            row = jnp.where(to == hot, 0.0, src_live[pl.ds(to, 1)])
            near_src = jnp.where(near_id == o + REACH, row, near_src)
            near_dst = jnp.where(near_id == o + REACH, dst_live[pl.ds(lax.rem(me - o + n, n), 1)], near_dst)
        for h in range(2):
            base = base_layout(capacity, h)
            srcx_ref[h, 0:blocks] = lay_out(src_all, *base)
            dstx_ref[h, 0:blocks] = lay_out(dst_all, *base)
            near = near_layout(capacity, h)
            srcx_ref[h, blocks:] = lay_out(near_src, *near)[:, 0:CHUNK]
            dstx_ref[h, blocks:] = lay_out(near_dst, *near)[:, 0:CHUNK]

    GRID.wait()

    for j in range(blocks):
        rows = pick_turned(grid_ref[...], srcx_ref[core, j:j + 1]).T.astype(bf)
        base_out[j * (CHUNK // HALF):(j + 1) * (CHUNK // HALF)] = rows.reshape(CHUNK // HALF, HALF, rows.shape[1])

    near_out[...] = pick_turned(grid_ref[...], srcx_ref[core, blocks:]).T.astype(bf)
    near_in[core, used:, :] = jnp.zeros((NEAR_ROWS - used, near_in.shape[2]), bf)

    pl.semaphore_wait(barrier, n)
    each_peer(lambda peer: to_graph(dst_ref.at[peer], dst_in.at[me], DST, peer).start())
    for o in range(-REACH, REACH + 1):
        rows = pl.ds((o + REACH) * span, span)
        if o == 0:
            near_in[core, (o + REACH) * span:(o + REACH + 1) * span] = near_out[(o + REACH) * span:(o + REACH + 1) * span]
        else:
            to_graph(near_out.at[rows], near_in.at[core, rows], NEAR, lax.rem(me + o + n, n)).start()
    each_peer(lambda peer: to_graph(base_out.at[peer], base_in.at[core, me], BASE, peer).start())
    base_in[core, pl.ds(me, 1)] = base_out[pl.ds(me, 1)]
    dst_in[pl.ds(me, 1)] = dst_ref[pl.ds(me, 1)]

    EMBED.wait()
    WDEC.wait()
    w_other = wdec_ref[:, pl.ds(pl.multiple_of(other * quarter, quarter), quarter)]
    w_own = wdec_ref[:, pl.ds(pl.multiple_of(core * quarter, quarter), quarter)]
    prj_out[...] = dot(embed_ref[...], w_other).astype(bf)
    send0 = to_core(prj_out, emb_half, PRJ0)
    send0.start()
    WSRC.wait()
    BIAS.wait()
    hot_src = src_live[pl.ds(hot, 1)].astype(jnp.int32) - 1
    msgs = silu(dot(pick_turned(grid_ref[...], hot_src).T.astype(bf), wsrc_ref[...]) + bias_ref[...]).astype(bf)
    emb_own = dot(embed_ref[...], w_own)
    send0.wait_recv()
    emb_out[...] = (emb_own + emb_half[...].astype(jnp.float32)).astype(bf).reshape(owners, OWN, quarter)

    wait_in(dst_in.at[pl.ds(0, n - 1)], DST)
    hot_dst = jnp.where(hot_src >= 0, dst_in[hot], -1)
    part_out[...] = dot(spread(mesh_rows, hot_dst), msgs).astype(bf).reshape(owners, OWN, half)

    def to_owner(copy_to):
        def visit(peer):
            owns, block = seat(peer)

            @pl.when(owns)
            def _():
                copy_to(peer, block).start()
        return visit

    each_peer(to_owner(lambda peer, block: to_graph(part_out.at[block], part_in.at[me], PART, peer)))

    wait_in(base_in.at[core, pl.ds(0, n - 1)], BASE)
    to_core(base_in.at[core], base_in.at[core], FWDB).start()
    wait_in(near_in.at[core, pl.ds(0, 2 * REACH * span)], NEAR)
    to_core(near_in.at[core], near_in.at[core], FWDN).start()
    each_peer(to_owner(lambda peer, block: to_graph(emb_out.at[block], emb_in.at[me], EMB, peer)))

    def share(rows, idx):
        m = silu(dot(rows, wsrc_ref[...]) + bias_ref[...]).astype(bf)
        return dot(spread(mesh_rows, idx), m)

    def half_sum(h):
        total = share(near_in[h], dstx_ref[h, blocks:])
        for j in range(blocks):
            rows = base_in[h, j * (CHUNK // HALF):(j + 1) * (CHUNK // HALF)].reshape(CHUNK, base_in.shape[3])
            total = total + share(rows, dstx_ref[h, j:j + 1])
        return total

    acc[...] = half_sum(core)
    to_core(base_in.at[other], base_in.at[other], FWDB).wait_recv()
    to_core(near_in.at[other], near_in.at[other], FWDN).wait_recv()

    WNODE.wait()
    n_other = wnode_ref[:, pl.ds(pl.multiple_of(other * half, half), half)]
    n_own = wnode_ref[:, pl.ds(pl.multiple_of(core * half, half), half)]
    agg = (acc[...] + half_sum(other)).astype(bf)
    middle = mesh_rows // 2
    spans = (slice(0, middle), slice(middle, mesh_rows))
    sends, own, own_p = [], [], []
    for part, k in zip(spans, (HID, HID1)):
        hid_out[part] = dot(agg[part], n_other).astype(bf)
        sends.append(to_core(hid_out.at[part], hid_in.at[part], k))
        sends[-1].start()
    for part in spans:
        own.append(dot(agg[part], n_own))
    send0.wait_send()
    for i, (part, k) in enumerate(zip(spans, (PRJ, PRJ1))):
        sends[i].wait_recv()
        lat = (embed_ref[part].astype(jnp.float32) + silu(own[i] + hid_in[part].astype(jnp.float32))).astype(bf)
        prj_out[part] = dot(lat, w_other).astype(bf)
        sends.append(to_core(prj_out.at[part], prj_in.at[part], k))
        sends[-1].start()
        own_p.append(dot(lat, w_own))
    for i, part in enumerate(spans):
        sends[2 + i].wait_recv()
        prj_bf[part] = (own_p[i] + prj_in[part].astype(jnp.float32)).astype(bf)
    for h in range(2):
        for j in range(blocks):
            rows = pick_turned(prj_bf[...], dstx_ref[h, j:j + 1]).T.astype(bf)
            back_out[h, j * (CHUNK // HALF):(j + 1) * (CHUNK // HALF)] = rows.reshape(CHUNK // HALF, HALF, quarter)
        back_in[h, pl.ds(me, 1)] = back_out[h, pl.ds(me, 1)]

    each_peer(lambda peer: to_graph(back_out.at[:, peer], back_in.at[:, me], BACK, peer).start())
    @pl.when(mine)
    def _():
        wait_in(part_in.at[pl.ds(0, n - 1)], PART)
        part_in[pl.ds(me, 1)] = part_out[pl.ds(my_block, 1)]

    hot_agg = part_in[...].astype(jnp.float32).sum(axis=0).astype(bf)
    hhid_out[...] = dot(hot_agg, n_other)
    send3 = to_core(hhid_out, hhid_in, HIDH)
    send3.start()
    hot_own = dot(hot_agg, n_own)

    send3.wait_recv()
    hot_lat = silu(hot_own + hhid_in[...]).astype(bf)
    hprj_out[...] = dot(hot_lat, w_other)
    send4 = to_core(hprj_out, hprj_in, PRJH)
    send4.start()
    hot_prj = dot(hot_lat, w_own)

    @pl.when(mine)
    def _():
        wait_in(emb_in.at[pl.ds(0, n - 1)], EMB)
        emb_in[pl.ds(me, 1)] = emb_out[pl.ds(my_block, 1)]

    send4.wait_recv()
    hot_out[...] = (hot_prj + hprj_in[...] + emb_in[hot].astype(jnp.float32)).astype(bf)

    @pl.when(mine)
    def _():
        each_peer(lambda peer: to_graph(hot_out, hot_in.at[my_block], HOT, peer).start())

    for h in range(2):
        nback_out[h] = pick_turned(prj_bf[...], dstx_ref[h, blocks:]).T.astype(bf)
        nback_in[h, used:, :] = jnp.zeros((NEAR_ROWS - used, quarter), bf)
        for o in range(-REACH, REACH + 1):
            a = (o + REACH) * span
            if o == 0:
                nback_in[h, a:a + span] = nback_out[h, a:a + span]
            else:
                to_graph(nback_out.at[h, pl.ds(a, span)], nback_in.at[h, pl.ds(a, span)], NBACK, lax.rem(me - o + n, n)).start()

    wait_in(nback_in.at[:, pl.ds(0, 2 * REACH * span)], NBACK)
    total = grid_ref[:, pl.ds(pl.multiple_of(core * quarter, quarter), quarter)].astype(jnp.float32)
    for h in range(2):
        total = total + dot(spread(grid_rows, srcx_ref[h, blocks:]), nback_in[h])
    dec[...] = total
    wait_in(back_in.at[:, pl.ds(0, n - 1)], BACK)
    total = dec[...]
    for h in range(2):
        for j in range(blocks):
            rows = back_in[h, j * (CHUNK // HALF):(j + 1) * (CHUNK // HALF)].reshape(CHUNK, quarter)
            total = total + dot(spread(grid_rows, srcx_ref[h, j:j + 1]), rows)
    dec[...] = total

    hot_to[...] = spread(grid_rows, hot_src)
    hot_from[...] = spread(mesh_rows, hot_dst)

    @pl.when(mine)
    def _():
        wait_in(hot_in.at[pl.ds(0, owners - 1)], HOT)
        hot_in[pl.ds(my_block, 1)] = hot_out[...].reshape(1, OWN, quarter)

    @pl.when(jnp.logical_not(mine))
    def _():
        wait_in(hot_in, HOT)

    hot_rows = lax.dot_general(
        hot_in[...].reshape(mesh_rows, quarter), hot_from[...], (((0,), (0,)), ((), ())), preferred_element_type=jnp.float32
    ).astype(bf)
    back = lax.dot_general(hot_to[...], hot_rows, (((1,), (1,)), ((), ())), preferred_element_type=jnp.float32)
    out_ref[...] = (dec[...] + back).astype(bf)

    wait_out(dst_ref.at[pl.ds(0, n - 1)], DST)
    wait_out(base_out.at[pl.ds(0, n - 1)], BASE)
    wait_out(near_out.at[pl.ds(0, 2 * REACH * span)], NEAR)

    @pl.when(mine)
    def _():
        wait_out(emb_out.at[pl.ds(0, owners - 1)], EMB)
        wait_out(part_out.at[pl.ds(0, owners - 1)], PART)
        wait_out(back_out.at[0, pl.ds(0, n - 1)], HOT)

    @pl.when(jnp.logical_not(mine))
    def _():
        wait_out(emb_out, EMB)
        wait_out(part_out, PART)

    to_core(base_in.at[core], base_in.at[core], FWDB).wait_send()
    to_core(near_in.at[core], near_in.at[core], FWDN).wait_send()
    for copy in (*sends, send3, send4):
        copy.wait_send()
    wait_out(back_out.at[:, pl.ds(0, n - 1)], BACK)
    wait_out(nback_out.at[:, pl.ds(0, 2 * REACH * span)], NBACK)


def cap_near(capacity):
    return (capacity - KEEP) // 2


def lay_out(table, take, mark):
    high = jnp.floor(table * (1.0 / 32.0))
    low = table - 32.0 * high
    dot = functools.partial(jnp.dot, preferred_element_type=jnp.float32)
    moved = 32.0 * dot(high.astype(jnp.bfloat16), take) + dot(low.astype(jnp.bfloat16), take)
    group = mark.shape[0]
    moved = moved.reshape(table.shape[0] // group, group, take.shape[1])
    return (moved * mark[None]).sum(axis=1).astype(jnp.int32) - 1


def base_layout(capacity, h):
    shape = (capacity, CHUNK)
    lane = lax.broadcasted_iota(jnp.int32, shape, 1)
    slot = lax.broadcasted_iota(jnp.int32, shape, 0)
    take = jnp.where(slot == h * HALF + (lane & (HALF - 1)), 1.0, 0.0).astype(jnp.bfloat16)
    group = CHUNK // HALF
    lane = lax.broadcasted_iota(jnp.int32, (group, CHUNK), 1)
    row = lax.broadcasted_iota(jnp.int32, (group, CHUNK), 0)
    return take, jnp.where(row * HALF <= lane, 1.0, 0.0) * jnp.where(lane < row * HALF + HALF, 1.0, 0.0)


def near_layout(capacity, h):
    span = cap_near(capacity)
    count = 2 * REACH + 1
    shape = (capacity, NEAR_ROWS)
    lane = lax.broadcasted_iota(jnp.int32, shape, 1)
    slot = lax.broadcasted_iota(jnp.int32, shape, 0)
    within = lane
    for i in range(1, count + 1):
        within = within - jnp.where(lane >= i * span, span, 0)
    take = jnp.where(slot == KEEP + h * span + within, 1.0, 0.0).astype(jnp.bfloat16)
    lane = lax.broadcasted_iota(jnp.int32, (8, NEAR_ROWS), 1)
    row = lax.broadcasted_iota(jnp.int32, (8, NEAR_ROWS), 0)
    inside = jnp.where(row * span <= lane, 1.0, 0.0) * jnp.where(lane < row * span + span, 1.0, 0.0)
    return take, inside * jnp.where(row < count, 1.0, 0.0)


def compact(grid_state, w_src, bias_src, mesh_embed, w_node, w_dec, slot_src, slot_dst, slot_count):
    n = lax.axis_size("graph")
    capacity = slot_src.shape[2]
    grid_rows, width = grid_state.shape
    mesh_rows, half = mesh_embed.shape
    quarter = width // 2
    owners = mesh_rows // OWN
    bf, f32 = jnp.bfloat16, jnp.float32
    vm = pltpu.VMEM
    return pl.pallas_call(
        functools.partial(step_kernel, n),
        out_shape=(jax.ShapeDtypeStruct((grid_rows, quarter), bf), jax.ShapeDtypeStruct((1,), jnp.int32)),
        in_specs=[pl.BlockSpec(memory_space=pl.ANY)] * 9,
        out_specs=(pl.BlockSpec(memory_space=vm), pl.BlockSpec(memory_space=pltpu.SMEM)),
        scratch_shapes=[
            vm((grid_rows, width), bf), vm(w_src.shape, bf), vm((1, half), f32), vm((mesh_rows, half), bf), vm(w_node.shape, bf),
            vm(w_dec.shape, bf), vm(slot_src.shape, jnp.int32), vm(slot_dst.shape, jnp.int32), vm(slot_count.shape, jnp.int32),
            vm((n, capacity), f32), vm((n, capacity), f32),
            vm((2, n * HALF // CHUNK + 1, CHUNK), jnp.int32), vm((2, n * HALF // CHUNK + 1, CHUNK), jnp.int32),
            vm((n, HALF, width), bf), vm((NEAR_ROWS, width), bf),
            vm((2, n, HALF, width), bf), vm((2, NEAR_ROWS, width), bf),
            vm((n, 1, capacity), jnp.int32), vm((n, OWN, quarter), bf), vm((owners, OWN, quarter), bf), vm((mesh_rows, quarter), bf),
            vm((owners, OWN, half), bf), vm((n, OWN, half), bf),
            vm((mesh_rows, half), f32),
            vm((mesh_rows, half), bf), vm((mesh_rows, half), bf),
            vm((mesh_rows, quarter), bf), vm((mesh_rows, quarter), bf), vm((mesh_rows, quarter), bf),
            vm((2, n, HALF, quarter), bf), vm((2, NEAR_ROWS, quarter), bf),
            vm((2, n, HALF, quarter), bf), vm((2, NEAR_ROWS, quarter), bf),
            vm((OWN, quarter), bf), vm((owners, OWN, quarter), bf),
            vm((grid_rows, quarter), f32),
            vm((OWN, half), f32), vm((OWN, half), f32), vm((OWN, quarter), f32), vm((OWN, quarter), f32),
            vm((grid_rows, capacity), bf), vm((mesh_rows, capacity), bf),
            pltpu.SemaphoreType.DMA((9,)), pltpu.SemaphoreType.DMA((SEMS,)), pltpu.SemaphoreType.DMA((SEMS,)),
        ],
        compiler_params=pltpu.CompilerParams(collective_id=0, has_side_effects=True, vmem_limit_bytes=48 * 1024 * 1024),
    )(grid_state, w_src, bias_src[None, :], mesh_embed, w_node, w_dec, slot_src, slot_dst, slot_count)


def on_device(grid_state, w_src, bias_src, mesh_embed, w_node, w_dec, slot_src, slot_dst, slot_count):
    args = (grid_state, w_src, bias_src, mesh_embed, w_node, w_dec, slot_src, slot_dst, slot_count)
    result, fits = compact(*args)
    return lax.cond(fits[0] > 0, lambda: result, lambda: dense(*args))


def solution(mesh):
    placed = (
        P(("member", "graph"), None),
        P(None, "chan"),
        P("chan"),
        P("graph", "chan"),
        P("chan", None),
        P("chan", None),
        P("graph", None, None),
        P(None, "graph", None),
        P(),
    )
    return jax.shard_map(
        on_device,
        mesh=mesh,
        in_specs=placed,
        out_specs=P(("member", "graph"), "chan"),
        check_vma=False,
    )
```

```python
import functools
import math

import jax
import jax.numpy as jnp
from jax import lax
from jax.experimental import pallas as pl
from jax.experimental.pallas import tpu as pltpu
from jax.sharding import PartitionSpec as P

MESH_ID = pl.DeviceIdType.MESH
KEEP = 32
HALF = KEEP // 2
GROUP = 7
SEMS = 17
REACH = 2
OWN = 16
NEAR_ROWS = 256
CHUNK = 256

def split_up(value, dim, count):
    lengths = value.shape
    parts = value.reshape(*lengths[:dim], count, lengths[dim] // count, *lengths[dim + 1 :])
    return jnp.moveaxis(parts, dim, 0)


def sum_at_owner(value, axis, dim):
    parts = split_up(value, dim, lax.axis_size(axis))
    arrived = lax.all_to_all(parts, axis, split_axis=0, concat_axis=0, tiled=True)
    return arrived.sum(axis=0)


def edge_network(source_rows, w_src, bias_src):
    return jax.nn.silu(
        jnp.dot(source_rows, w_src, preferred_element_type=jnp.float32) + bias_src
    ).astype(jnp.bfloat16)


def segment_rows(values, indices, usable, row_count):
    slot_total = values.shape[0]
    width = values.shape[1]
    block_len = math.gcd(slot_total, 2048)
    block_count = slot_total // block_len
    targets = jnp.where(usable, indices, -1).reshape(block_count, block_len)
    pieces = values.reshape(block_count, block_len, width)
    row_ids = jnp.arange(row_count, dtype=jnp.int32)

    def add_block(summed, scan_item):
        row_target, piece_vals = scan_item
        one_hot = (row_ids[:, None] == row_target[None, :]).astype(jnp.bfloat16)
        return (summed + jnp.dot(one_hot, piece_vals, preferred_element_type=jnp.float32), None)

    result, unused = lax.scan(
        add_block, jnp.zeros((row_count, width), jnp.float32), (targets, pieces)
    )
    return result


def dense(
    grid_state, w_src, bias_src, mesh_embed, w_node, w_dec, slot_src, slot_dst, slot_count
):
    peers = lax.axis_size("graph")
    own_index = lax.axis_index("graph")
    core_index = lax.axis_index("chan")
    capacity = slot_src.shape[2]
    positions = jnp.arange(capacity, dtype=jnp.int32)
    grid_rows = grid_state.shape[0]
    mesh_rows = mesh_embed.shape[0]
    sent_counts = lax.dynamic_slice_in_dim(slot_count, own_index, 1, 0)[0]
    recv_counts = lax.dynamic_slice_in_dim(slot_count, own_index, 1, 1)[:, 0]
    half_slots = capacity // 2
    chosen = lax.dynamic_slice_in_dim(slot_src[0], core_index * half_slots, half_slots, 1)
    picked = jnp.take(grid_state, chosen.reshape(-1), axis=0).reshape(
        peers, half_slots, grid_state.shape[1]
    )
    arrived = lax.all_to_all(picked, "graph", split_axis=0, concat_axis=0, tiled=True)
    partner = lax.ppermute(arrived, "chan", [(0, 1), (1, 0)])
    joined = jnp.where(
        core_index == 0,
        jnp.concatenate([arrived, partner], axis=1),
        jnp.concatenate([partner, arrived], axis=1),
    )
    messages = edge_network(joined.reshape(peers * capacity, grid_state.shape[1]), w_src, bias_src)
    arrive_ok = (positions[None, :] < recv_counts[:, None]).reshape(-1)
    dst_rows = slot_dst[:, 0, :].reshape(-1)
    aggregate = segment_rows(messages, dst_rows, arrive_ok, mesh_rows)
    partial_hidden = jnp.dot(
        aggregate.astype(jnp.bfloat16), w_node, preferred_element_type=jnp.float32
    )
    hidden_pre = sum_at_owner(partial_hidden, "chan", 1)
    latent = (mesh_embed.astype(jnp.float32) + jax.nn.silu(hidden_pre)).astype(jnp.bfloat16)
    partial_proj = jnp.dot(latent, w_dec, preferred_element_type=jnp.float32)
    projected = sum_at_owner(partial_proj, "chan", 1).astype(jnp.bfloat16)
    returned = jnp.take(projected, dst_rows, axis=0).reshape(peers, capacity, projected.shape[1])
    came_back = lax.all_to_all(returned, "graph", split_axis=0, concat_axis=0, tiled=True).reshape(
        peers * capacity, projected.shape[1]
    )
    send_ok = (positions[None, :] < sent_counts[:, None]).reshape(-1)
    decoded = segment_rows(came_back, slot_src[0].reshape(-1), send_ok, grid_rows)
    width_half = decoded.shape[1]
    own_cols = lax.dynamic_slice_in_dim(grid_state, core_index * width_half, width_half, 1)
    return (own_cols.astype(jnp.float32) + decoded).astype(jnp.bfloat16)


def torus(n):
    wide = 1 << (n.bit_length() // 2)
    return n // wide, wide


def visit_order(n):
    tall, wide = torus(n)
    offsets = [(r, c) for r in range(tall) for c in range(wide)][1:]
    offsets.sort(key=lambda o: min(o[0], tall - o[0]) + min(o[1], wide - o[1]))
    return [offsets[i // 2] if i % 2 == 0 else offsets[-1 - i // 2] for i in range(n - 1)]


def silu(v):
    h = 0.5 * v
    return h + h * jnp.tanh(h)


def pick_turned(table, idx):
    rows = table.shape[0]
    hot = jnp.where(
        lax.broadcasted_iota(jnp.int32, (rows, idx.shape[1]), 0) == idx, 1.0, 0.0
    ).astype(jnp.bfloat16)
    return lax.dot_general(table, hot, (((0,), (0,)), ((), ())), preferred_element_type=jnp.float32)


def spread(rows, idx):
    return jnp.where(
        lax.broadcasted_iota(jnp.int32, (rows, idx.shape[1]), 0) == idx, 1.0, 0.0
    ).astype(jnp.bfloat16)


def step_kernel(
    n, grid_hbm, wsrc_hbm, bias_hbm, embed_hbm, wnode_hbm, wdec_hbm, src_hbm, dst_hbm, count_hbm, out_ref, fits_ref,
    grid_ref, wsrc_ref, bias_ref, embed_ref, wnode_ref, wdec_ref, src_ref, dst_ref, count_ref,
    src_live, dst_live, srcx_ref, dstx_ref,
    base_out, near_out, base_in, near_in, dst_in, emb_in, emb_out, emb_half, part_out, part_in,
    acc, hid_out, hid_in, prj_out, prj_in, prj_bf, back_out, nback_out, back_in, nback_in, hot_out, hot_in, dec,
    hhid_out, hhid_in, hprj_out, hprj_in, hot_to, hot_from,
    lsem, ssem, rsem,
):
    me = lax.axis_index("graph")
    core = lax.axis_index("chan")
    other = 1 - core
    grid_rows = grid_ref.shape[0]
    mesh_rows = embed_ref.shape[0]
    owners = mesh_rows // OWN
    span = cap_near(dst_ref.shape[2])
    used = (2 * REACH + 1) * span
    half = hid_out.shape[1]
    quarter = prj_out.shape[1]
    bf = jnp.bfloat16
    dot = functools.partial(jnp.dot, preferred_element_type=jnp.float32)

    pairs = (
        (src_hbm, src_ref), (dst_hbm, dst_ref), (count_hbm, count_ref), (grid_hbm, grid_ref), (embed_hbm, embed_ref),
        (wdec_hbm, wdec_ref), (wsrc_hbm, wsrc_ref), (bias_hbm, bias_ref), (wnode_hbm, wnode_ref),
    )
    SRC, DSTS, COUNT, GRID, EMBED, WDEC, WSRC, BIAS, WNODE = (
        pltpu.make_async_copy(x, y, lsem.at[i]) for i, (x, y) in enumerate(pairs))
    for copy in (SRC, DSTS, COUNT, GRID, EMBED, WDEC, WSRC, BIAS, WNODE):
        copy.start()

    tall, wide = torus(n)
    codes = [r * 2 * wide + c for r, c in visit_order(n)]
    groups = [codes[i:i + GROUP] for i in range(0, n - 1, GROUP)]
    spot = 2 * wide * (me // wide) + lax.rem(me, wide) + core * (2 * wide * tall + wide)
    turn = 1 - 2 * core

    def each_peer(visit):
        @pl.loop(0, len(groups))
        def _(g):
            for part in (range(0, 4), range(4, GROUP)):
                packed = jnp.int32(0)
                for i, group in enumerate(groups):
                    packed = jnp.where(g == i, sum(group[k] << (7 * j) for j, k in enumerate(part)), packed)
                for j in range(len(part)):
                    code = lax.shift_right_logical(packed, jnp.int32(7 * j)) & 127
                    at = spot + turn * code
                    visit((lax.shift_right_logical(at, jnp.int32(1)) & ((tall - 1) * wide)) + (at & (wide - 1)))

    per_row = owners // tall

    def seat(shard):
        r = lax.shift_right_logical(shard, jnp.int32(wide.bit_length() - 1))
        rank = (shard + 3 * r) & (wide - 1)
        return rank < per_row, r * per_row + rank

    mine, my_block = seat(me)
    barrier = pltpu.get_barrier_semaphore()
    each_peer(lambda peer: pl.semaphore_signal(barrier, inc=1, device_id={"graph": peer}, device_id_type=MESH_ID))
    pl.semaphore_signal(barrier, inc=1, device_id={"chan": other}, device_id_type=MESH_ID)

    def to_graph(src, dst, k, peer):
        return pltpu.make_async_remote_copy(
            src_ref=src, dst_ref=dst, send_sem=ssem.at[k], recv_sem=rsem.at[k],
            device_id={"graph": peer}, device_id_type=MESH_ID)

    def to_core(src, dst, k):
        return pltpu.make_async_remote_copy(
            src_ref=src, dst_ref=dst, send_sem=ssem.at[k], recv_sem=rsem.at[k],
            device_id={"chan": other}, device_id_type=MESH_ID)

    def wait_in(ref, k):
        to_graph(ref, ref, k, me).wait_recv()

    def wait_out(ref, k):
        to_graph(ref, ref, k, me).wait_send()

    DST, EMB, BASE, NEAR, PART, FWDB, FWDN, HID, PRJ, BACK, NBACK, HOT, PRJ0, HIDH, PRJH, HID1, PRJ1 = range(SEMS)

    blocks = (n * HALF) // CHUNK
    capacity = dst_ref.shape[2]
    SRC.wait()
    DSTS.wait()
    COUNT.wait()
    with jax.named_scope("index"):
        ids = lax.broadcasted_iota(jnp.int32, (n, n), 0)
        cols = lax.broadcasted_iota(jnp.int32, (n, n), 1)
        counts = count_ref[...]
        apart = jnp.abs(ids - cols)
        far_counts = jnp.where(jnp.minimum(apart, n - apart) > REACH, counts, 0)
        hot = jnp.max(jnp.where(far_counts > KEEP, cols, 0))
        first = jnp.min(jnp.where(far_counts > KEEP, cols, n))
        fits_ref[0] = jnp.where(hot <= first, 1, 0)
        sent = jnp.where(ids == me, counts, 0).sum(axis=0, keepdims=True)
        sent = jnp.where(ids == cols, sent, 0).sum(axis=1, keepdims=True)
        came = jnp.where(cols == me, counts, 0).sum(axis=1, keepdims=True)
        pos = lax.broadcasted_iota(jnp.int32, (n, capacity), 1)
        src_all = jnp.where(pos < sent, src_ref[0] + 1, 0).astype(jnp.float32)
        src_live[...] = src_all
        came = jnp.where(me == hot, 0, came)
        dst_all = jnp.where(pos < came, dst_ref[:, 0, :] + 1, 0).astype(jnp.float32)
        dst_live[...] = dst_all
        rows_id = lax.broadcasted_iota(jnp.int32, (n, capacity), 0)
        src_all = jnp.where(rows_id == hot, 0.0, src_all)
        near_id = lax.broadcasted_iota(jnp.int32, (8, capacity), 0)
        near_src = jnp.zeros((8, capacity), jnp.float32)
        near_dst = jnp.zeros((8, capacity), jnp.float32)
        for o in range(-REACH, REACH + 1):
            to = lax.rem(me + o + n, n)
            row = jnp.where(to == hot, 0.0, src_live[pl.ds(to, 1)])
            near_src = jnp.where(near_id == o + REACH, row, near_src)
            near_dst = jnp.where(near_id == o + REACH, dst_live[pl.ds(lax.rem(me - o + n, n), 1)], near_dst)
        for h in range(2):
            base = base_layout(capacity, h)
            srcx_ref[h, 0:blocks] = lay_out(src_all, *base)
            dstx_ref[h, 0:blocks] = lay_out(dst_all, *base)
            near = near_layout(capacity, h)
            srcx_ref[h, blocks:] = lay_out(near_src, *near)[:, 0:CHUNK]
            dstx_ref[h, blocks:] = lay_out(near_dst, *near)[:, 0:CHUNK]

    GRID.wait()

    for j in range(blocks):
        rows = pick_turned(grid_ref[...], srcx_ref[core, j:j + 1]).T.astype(bf)
        base_out[j * (CHUNK // HALF):(j + 1) * (CHUNK // HALF)] = rows.reshape(CHUNK // HALF, HALF, rows.shape[1])

    near_out[...] = pick_turned(grid_ref[...], srcx_ref[core, blocks:]).T.astype(bf)
    near_in[core, used:, :] = jnp.zeros((NEAR_ROWS - used, near_in.shape[2]), bf)

    pl.semaphore_wait(barrier, n)
    each_peer(lambda peer: to_graph(dst_ref.at[peer], dst_in.at[me], DST, peer).start())
    for o in range(-REACH, REACH + 1):
        rows = pl.ds((o + REACH) * span, span)
        if o == 0:
            near_in[core, (o + REACH) * span:(o + REACH + 1) * span] = near_out[(o + REACH) * span:(o + REACH + 1) * span]
        else:
            to_graph(near_out.at[rows], near_in.at[core, rows], NEAR, lax.rem(me + o + n, n)).start()
    each_peer(lambda peer: to_graph(base_out.at[peer], base_in.at[core, me], BASE, peer).start())
    base_in[core, pl.ds(me, 1)] = base_out[pl.ds(me, 1)]
    dst_in[pl.ds(me, 1)] = dst_ref[pl.ds(me, 1)]

    EMBED.wait()
    WDEC.wait()
    w_other = wdec_ref[:, pl.ds(pl.multiple_of(other * quarter, quarter), quarter)]
    w_own = wdec_ref[:, pl.ds(pl.multiple_of(core * quarter, quarter), quarter)]
    prj_out[...] = dot(embed_ref[...], w_other).astype(bf)
    send0 = to_core(prj_out, emb_half, PRJ0)
    send0.start()
    WSRC.wait()
    BIAS.wait()
    hot_src = src_live[pl.ds(hot, 1)].astype(jnp.int32) - 1
    msgs = silu(dot(pick_turned(grid_ref[...], hot_src).T.astype(bf), wsrc_ref[...]) + bias_ref[...]).astype(bf)
    emb_own = dot(embed_ref[...], w_own)
    send0.wait_recv()
    emb_out[...] = (emb_own + emb_half[...].astype(jnp.float32)).astype(bf).reshape(owners, OWN, quarter)

    wait_in(dst_in.at[pl.ds(0, n - 1)], DST)
    hot_dst = jnp.where(hot_src >= 0, dst_in[hot], -1)
    part_out[...] = dot(spread(mesh_rows, hot_dst), msgs).astype(bf).reshape(owners, OWN, half)

    def to_owner(copy_to):
        def visit(peer):
            owns, block = seat(peer)

            @pl.when(owns)
            def _():
                copy_to(peer, block).start()
        return visit

    each_peer(to_owner(lambda peer, block: to_graph(part_out.at[block], part_in.at[me], PART, peer)))
    each_peer(to_owner(lambda peer, block: to_graph(emb_out.at[block], emb_in.at[me], EMB, peer)))

    wait_in(base_in.at[core, pl.ds(0, n - 1)], BASE)
    to_core(base_in.at[core], base_in.at[core], FWDB).start()
    wait_in(near_in.at[core, pl.ds(0, 2 * REACH * span)], NEAR)
    to_core(near_in.at[core], near_in.at[core], FWDN).start()
    def share(rows, idx):
        m = silu(dot(rows, wsrc_ref[...]) + bias_ref[...]).astype(bf)
        return dot(spread(mesh_rows, idx), m)

    def half_sum(h):
        total = share(near_in[h], dstx_ref[h, blocks:])
        for j in range(blocks):
            rows = base_in[h, j * (CHUNK // HALF):(j + 1) * (CHUNK // HALF)].reshape(CHUNK, base_in.shape[3])
            total = total + share(rows, dstx_ref[h, j:j + 1])
        return total

    acc[...] = half_sum(core)
    to_core(base_in.at[other], base_in.at[other], FWDB).wait_recv()
    to_core(near_in.at[other], near_in.at[other], FWDN).wait_recv()

    WNODE.wait()
    n_other = wnode_ref[:, pl.ds(pl.multiple_of(other * half, half), half)]
    n_own = wnode_ref[:, pl.ds(pl.multiple_of(core * half, half), half)]
    agg = (acc[...] + half_sum(other)).astype(bf)
    middle = mesh_rows // 2
    spans = (slice(0, middle), slice(middle, mesh_rows))
    sends, own, own_p = [], [], []
    for part, k in zip(spans, (HID, HID1)):
        hid_out[part] = dot(agg[part], n_other).astype(bf)
        sends.append(to_core(hid_out.at[part], hid_in.at[part], k))
        sends[-1].start()
    for part in spans:
        own.append(dot(agg[part], n_own))
    send0.wait_send()
    for i, (part, k) in enumerate(zip(spans, (PRJ, PRJ1))):
        sends[i].wait_recv()
        lat = (embed_ref[part].astype(jnp.float32) + silu(own[i] + hid_in[part].astype(jnp.float32))).astype(bf)
        prj_out[part] = dot(lat, w_other).astype(bf)
        sends.append(to_core(prj_out.at[part], prj_in.at[part], k))
        sends[-1].start()
        own_p.append(dot(lat, w_own))
    for i, part in enumerate(spans):
        sends[2 + i].wait_recv()
        prj_bf[part] = (own_p[i] + prj_in[part].astype(jnp.float32)).astype(bf)
    for h in range(2):
        for j in range(blocks):
            rows = pick_turned(prj_bf[...], dstx_ref[h, j:j + 1]).T.astype(bf)
            back_out[h, j * (CHUNK // HALF):(j + 1) * (CHUNK // HALF)] = rows.reshape(CHUNK // HALF, HALF, quarter)
        back_in[h, pl.ds(me, 1)] = back_out[h, pl.ds(me, 1)]

    each_peer(lambda peer: to_graph(back_out.at[:, peer], back_in.at[:, me], BACK, peer).start())
    @pl.when(mine)
    def _():
        wait_in(part_in.at[pl.ds(0, n - 1)], PART)
        part_in[pl.ds(me, 1)] = part_out[pl.ds(my_block, 1)]

    hot_agg = part_in[...].astype(jnp.float32).sum(axis=0).astype(bf)
    hhid_out[...] = dot(hot_agg, n_other)
    send3 = to_core(hhid_out, hhid_in, HIDH)
    send3.start()
    hot_own = dot(hot_agg, n_own)

    send3.wait_recv()
    hot_lat = silu(hot_own + hhid_in[...]).astype(bf)
    hprj_out[...] = dot(hot_lat, w_other)
    send4 = to_core(hprj_out, hprj_in, PRJH)
    send4.start()
    hot_prj = dot(hot_lat, w_own)

    @pl.when(mine)
    def _():
        wait_in(emb_in.at[pl.ds(0, n - 1)], EMB)
        emb_in[pl.ds(me, 1)] = emb_out[pl.ds(my_block, 1)]

    send4.wait_recv()
    hot_out[...] = (hot_prj + hprj_in[...] + emb_in[hot].astype(jnp.float32)).astype(bf)

    @pl.when(mine)
    def _():
        each_peer(lambda peer: to_graph(hot_out, hot_in.at[my_block], HOT, peer).start())

    for h in range(2):
        nback_out[h] = pick_turned(prj_bf[...], dstx_ref[h, blocks:]).T.astype(bf)
        nback_in[h, used:, :] = jnp.zeros((NEAR_ROWS - used, quarter), bf)
        for o in range(-REACH, REACH + 1):
            a = (o + REACH) * span
            if o == 0:
                nback_in[h, a:a + span] = nback_out[h, a:a + span]
            else:
                to_graph(nback_out.at[h, pl.ds(a, span)], nback_in.at[h, pl.ds(a, span)], NBACK, lax.rem(me - o + n, n)).start()

    wait_in(nback_in.at[:, pl.ds(0, 2 * REACH * span)], NBACK)
    total = grid_ref[:, pl.ds(pl.multiple_of(core * quarter, quarter), quarter)].astype(jnp.float32)
    for h in range(2):
        total = total + dot(spread(grid_rows, srcx_ref[h, blocks:]), nback_in[h])
    dec[...] = total
    wait_in(back_in.at[:, pl.ds(0, n - 1)], BACK)
    total = dec[...]
    for h in range(2):
        for j in range(blocks):
            rows = back_in[h, j * (CHUNK // HALF):(j + 1) * (CHUNK // HALF)].reshape(CHUNK, quarter)
            total = total + dot(spread(grid_rows, srcx_ref[h, j:j + 1]), rows)
    dec[...] = total

    hot_to[...] = spread(grid_rows, hot_src)
    hot_from[...] = spread(mesh_rows, hot_dst)

    @pl.when(mine)
    def _():
        wait_in(hot_in.at[pl.ds(0, owners - 1)], HOT)
        hot_in[pl.ds(my_block, 1)] = hot_out[...].reshape(1, OWN, quarter)

    @pl.when(jnp.logical_not(mine))
    def _():
        wait_in(hot_in, HOT)

    hot_rows = lax.dot_general(
        hot_in[...].reshape(mesh_rows, quarter), hot_from[...], (((0,), (0,)), ((), ())), preferred_element_type=jnp.float32
    ).astype(bf)
    back = lax.dot_general(hot_to[...], hot_rows, (((1,), (1,)), ((), ())), preferred_element_type=jnp.float32)
    out_ref[...] = (dec[...] + back).astype(bf)

    wait_out(dst_ref.at[pl.ds(0, n - 1)], DST)
    wait_out(base_out.at[pl.ds(0, n - 1)], BASE)
    wait_out(near_out.at[pl.ds(0, 2 * REACH * span)], NEAR)

    @pl.when(mine)
    def _():
        wait_out(emb_out.at[pl.ds(0, owners - 1)], EMB)
        wait_out(part_out.at[pl.ds(0, owners - 1)], PART)
        wait_out(back_out.at[0, pl.ds(0, n - 1)], HOT)

    @pl.when(jnp.logical_not(mine))
    def _():
        wait_out(emb_out, EMB)
        wait_out(part_out, PART)

    to_core(base_in.at[core], base_in.at[core], FWDB).wait_send()
    to_core(near_in.at[core], near_in.at[core], FWDN).wait_send()
    for copy in (*sends, send3, send4):
        copy.wait_send()
    wait_out(back_out.at[:, pl.ds(0, n - 1)], BACK)
    wait_out(nback_out.at[:, pl.ds(0, 2 * REACH * span)], NBACK)


def cap_near(capacity):
    return (capacity - KEEP) // 2


def lay_out(table, take, mark):
    high = jnp.floor(table * (1.0 / 32.0))
    low = table - 32.0 * high
    dot = functools.partial(jnp.dot, preferred_element_type=jnp.float32)
    moved = 32.0 * dot(high.astype(jnp.bfloat16), take) + dot(low.astype(jnp.bfloat16), take)
    group = mark.shape[0]
    moved = moved.reshape(table.shape[0] // group, group, take.shape[1])
    return (moved * mark[None]).sum(axis=1).astype(jnp.int32) - 1


def base_layout(capacity, h):
    shape = (capacity, CHUNK)
    lane = lax.broadcasted_iota(jnp.int32, shape, 1)
    slot = lax.broadcasted_iota(jnp.int32, shape, 0)
    take = jnp.where(slot == h * HALF + (lane & (HALF - 1)), 1.0, 0.0).astype(jnp.bfloat16)
    group = CHUNK // HALF
    lane = lax.broadcasted_iota(jnp.int32, (group, CHUNK), 1)
    row = lax.broadcasted_iota(jnp.int32, (group, CHUNK), 0)
    return take, jnp.where(row * HALF <= lane, 1.0, 0.0) * jnp.where(lane < row * HALF + HALF, 1.0, 0.0)


def near_layout(capacity, h):
    span = cap_near(capacity)
    count = 2 * REACH + 1
    shape = (capacity, NEAR_ROWS)
    lane = lax.broadcasted_iota(jnp.int32, shape, 1)
    slot = lax.broadcasted_iota(jnp.int32, shape, 0)
    within = lane
    for i in range(1, count + 1):
        within = within - jnp.where(lane >= i * span, span, 0)
    take = jnp.where(slot == KEEP + h * span + within, 1.0, 0.0).astype(jnp.bfloat16)
    lane = lax.broadcasted_iota(jnp.int32, (8, NEAR_ROWS), 1)
    row = lax.broadcasted_iota(jnp.int32, (8, NEAR_ROWS), 0)
    inside = jnp.where(row * span <= lane, 1.0, 0.0) * jnp.where(lane < row * span + span, 1.0, 0.0)
    return take, inside * jnp.where(row < count, 1.0, 0.0)


def compact(grid_state, w_src, bias_src, mesh_embed, w_node, w_dec, slot_src, slot_dst, slot_count):
    n = lax.axis_size("graph")
    capacity = slot_src.shape[2]
    grid_rows, width = grid_state.shape
    mesh_rows, half = mesh_embed.shape
    quarter = width // 2
    owners = mesh_rows // OWN
    bf, f32 = jnp.bfloat16, jnp.float32
    vm = pltpu.VMEM
    return pl.pallas_call(
        functools.partial(step_kernel, n),
        out_shape=(jax.ShapeDtypeStruct((grid_rows, quarter), bf), jax.ShapeDtypeStruct((1,), jnp.int32)),
        in_specs=[pl.BlockSpec(memory_space=pl.ANY)] * 9,
        out_specs=(pl.BlockSpec(memory_space=vm), pl.BlockSpec(memory_space=pltpu.SMEM)),
        scratch_shapes=[
            vm((grid_rows, width), bf), vm(w_src.shape, bf), vm((1, half), f32), vm((mesh_rows, half), bf), vm(w_node.shape, bf),
            vm(w_dec.shape, bf), vm(slot_src.shape, jnp.int32), vm(slot_dst.shape, jnp.int32), vm(slot_count.shape, jnp.int32),
            vm((n, capacity), f32), vm((n, capacity), f32),
            vm((2, n * HALF // CHUNK + 1, CHUNK), jnp.int32), vm((2, n * HALF // CHUNK + 1, CHUNK), jnp.int32),
            vm((n, HALF, width), bf), vm((NEAR_ROWS, width), bf),
            vm((2, n, HALF, width), bf), vm((2, NEAR_ROWS, width), bf),
            vm((n, 1, capacity), jnp.int32), vm((n, OWN, quarter), bf), vm((owners, OWN, quarter), bf), vm((mesh_rows, quarter), bf),
            vm((owners, OWN, half), bf), vm((n, OWN, half), bf),
            vm((mesh_rows, half), f32),
            vm((mesh_rows, half), bf), vm((mesh_rows, half), bf),
            vm((mesh_rows, quarter), bf), vm((mesh_rows, quarter), bf), vm((mesh_rows, quarter), bf),
            vm((2, n, HALF, quarter), bf), vm((2, NEAR_ROWS, quarter), bf),
            vm((2, n, HALF, quarter), bf), vm((2, NEAR_ROWS, quarter), bf),
            vm((OWN, quarter), bf), vm((owners, OWN, quarter), bf),
            vm((grid_rows, quarter), f32),
            vm((OWN, half), f32), vm((OWN, half), f32), vm((OWN, quarter), f32), vm((OWN, quarter), f32),
            vm((grid_rows, capacity), bf), vm((mesh_rows, capacity), bf),
            pltpu.SemaphoreType.DMA((9,)), pltpu.SemaphoreType.DMA((SEMS,)), pltpu.SemaphoreType.DMA((SEMS,)),
        ],
        compiler_params=pltpu.CompilerParams(collective_id=0, has_side_effects=True, vmem_limit_bytes=48 * 1024 * 1024),
    )(grid_state, w_src, bias_src[None, :], mesh_embed, w_node, w_dec, slot_src, slot_dst, slot_count)


def on_device(grid_state, w_src, bias_src, mesh_embed, w_node, w_dec, slot_src, slot_dst, slot_count):
    args = (grid_state, w_src, bias_src, mesh_embed, w_node, w_dec, slot_src, slot_dst, slot_count)
    result, fits = compact(*args)
    return lax.cond(fits[0] > 0, lambda: result, lambda: dense(*args))


def solution(mesh):
    placed = (
        P(("member", "graph"), None),
        P(None, "chan"),
        P("chan"),
        P("graph", "chan"),
        P("chan", None),
        P("chan", None),
        P("graph", None, None),
        P(None, "graph", None),
        P(),
    )
    return jax.shard_map(
        on_device,
        mesh=mesh,
        in_specs=placed,
        out_specs=P(("member", "graph"), "chan"),
        check_vma=False,
    )
```

```python
import functools
import math

import jax
import jax.numpy as jnp
from jax import lax
from jax.experimental import pallas as pl
from jax.experimental.pallas import tpu as pltpu
from jax.sharding import PartitionSpec as P

MESH_ID = pl.DeviceIdType.MESH
KEEP = 32
HALF = KEEP // 2
GROUP = 7
SEMS = 15
REACH = 2
OWN = 16
NEAR_ROWS = 256
CHUNK = 256

def split_up(value, dim, count):
    lengths = value.shape
    parts = value.reshape(*lengths[:dim], count, lengths[dim] // count, *lengths[dim + 1 :])
    return jnp.moveaxis(parts, dim, 0)


def sum_at_owner(value, axis, dim):
    parts = split_up(value, dim, lax.axis_size(axis))
    arrived = lax.all_to_all(parts, axis, split_axis=0, concat_axis=0, tiled=True)
    return arrived.sum(axis=0)


def edge_network(source_rows, w_src, bias_src):
    return jax.nn.silu(
        jnp.dot(source_rows, w_src, preferred_element_type=jnp.float32) + bias_src
    ).astype(jnp.bfloat16)


def segment_rows(values, indices, usable, row_count):
    slot_total = values.shape[0]
    width = values.shape[1]
    block_len = math.gcd(slot_total, 2048)
    block_count = slot_total // block_len
    targets = jnp.where(usable, indices, -1).reshape(block_count, block_len)
    pieces = values.reshape(block_count, block_len, width)
    row_ids = jnp.arange(row_count, dtype=jnp.int32)

    def add_block(summed, scan_item):
        row_target, piece_vals = scan_item
        one_hot = (row_ids[:, None] == row_target[None, :]).astype(jnp.bfloat16)
        return (summed + jnp.dot(one_hot, piece_vals, preferred_element_type=jnp.float32), None)

    result, unused = lax.scan(
        add_block, jnp.zeros((row_count, width), jnp.float32), (targets, pieces)
    )
    return result


def dense(
    grid_state, w_src, bias_src, mesh_embed, w_node, w_dec, slot_src, slot_dst, slot_count
):
    peers = lax.axis_size("graph")
    own_index = lax.axis_index("graph")
    core_index = lax.axis_index("chan")
    capacity = slot_src.shape[2]
    positions = jnp.arange(capacity, dtype=jnp.int32)
    grid_rows = grid_state.shape[0]
    mesh_rows = mesh_embed.shape[0]
    sent_counts = lax.dynamic_slice_in_dim(slot_count, own_index, 1, 0)[0]
    recv_counts = lax.dynamic_slice_in_dim(slot_count, own_index, 1, 1)[:, 0]
    half_slots = capacity // 2
    chosen = lax.dynamic_slice_in_dim(slot_src[0], core_index * half_slots, half_slots, 1)
    picked = jnp.take(grid_state, chosen.reshape(-1), axis=0).reshape(
        peers, half_slots, grid_state.shape[1]
    )
    arrived = lax.all_to_all(picked, "graph", split_axis=0, concat_axis=0, tiled=True)
    partner = lax.ppermute(arrived, "chan", [(0, 1), (1, 0)])
    joined = jnp.where(
        core_index == 0,
        jnp.concatenate([arrived, partner], axis=1),
        jnp.concatenate([partner, arrived], axis=1),
    )
    messages = edge_network(joined.reshape(peers * capacity, grid_state.shape[1]), w_src, bias_src)
    arrive_ok = (positions[None, :] < recv_counts[:, None]).reshape(-1)
    dst_rows = slot_dst[:, 0, :].reshape(-1)
    aggregate = segment_rows(messages, dst_rows, arrive_ok, mesh_rows)
    partial_hidden = jnp.dot(
        aggregate.astype(jnp.bfloat16), w_node, preferred_element_type=jnp.float32
    )
    hidden_pre = sum_at_owner(partial_hidden, "chan", 1)
    latent = (mesh_embed.astype(jnp.float32) + jax.nn.silu(hidden_pre)).astype(jnp.bfloat16)
    partial_proj = jnp.dot(latent, w_dec, preferred_element_type=jnp.float32)
    projected = sum_at_owner(partial_proj, "chan", 1).astype(jnp.bfloat16)
    returned = jnp.take(projected, dst_rows, axis=0).reshape(peers, capacity, projected.shape[1])
    came_back = lax.all_to_all(returned, "graph", split_axis=0, concat_axis=0, tiled=True).reshape(
        peers * capacity, projected.shape[1]
    )
    send_ok = (positions[None, :] < sent_counts[:, None]).reshape(-1)
    decoded = segment_rows(came_back, slot_src[0].reshape(-1), send_ok, grid_rows)
    width_half = decoded.shape[1]
    own_cols = lax.dynamic_slice_in_dim(grid_state, core_index * width_half, width_half, 1)
    return (own_cols.astype(jnp.float32) + decoded).astype(jnp.bfloat16)


def torus(n):
    wide = 1 << (n.bit_length() // 2)
    return n // wide, wide


def visit_order(n):
    tall, wide = torus(n)
    offsets = [(r, c) for r in range(tall) for c in range(wide)][1:]
    offsets.sort(key=lambda o: min(o[0], tall - o[0]) + min(o[1], wide - o[1]))
    return [offsets[i // 2] if i % 2 == 0 else offsets[-1 - i // 2] for i in range(n - 1)]


def silu(v):
    h = 0.5 * v
    return h + h * jnp.tanh(h)


def pick_turned(table, idx):
    rows = table.shape[0]
    hot = jnp.where(
        lax.broadcasted_iota(jnp.int32, (rows, idx.shape[1]), 0) == idx, 1.0, 0.0
    ).astype(jnp.bfloat16)
    return lax.dot_general(table, hot, (((0,), (0,)), ((), ())), preferred_element_type=jnp.float32)


def spread(rows, idx):
    return jnp.where(
        lax.broadcasted_iota(jnp.int32, (rows, idx.shape[1]), 0) == idx, 1.0, 0.0
    ).astype(jnp.bfloat16)


def step_kernel(
    n, grid_hbm, wsrc_hbm, bias_hbm, embed_hbm, wnode_hbm, wdec_hbm, src_hbm, dst_hbm, count_hbm, out_ref, fits_ref,
    grid_ref, wsrc_ref, bias_ref, embed_ref, wnode_ref, wdec_ref, src_ref, dst_ref, count_ref,
    src_live, dst_live, srcx_ref, dstx_ref,
    base_out, near_out, base_in, near_in, dst_in, emb_in, emb_out, emb_half, part_out, part_in,
    acc, hid_out, hid_in, prj_out, prj_in, prj_bf, back_out, nback_out, back_in, nback_in, hot_out, hot_in, dec,
    hhid_out, hhid_in, hprj_out, hprj_in, hot_to, hot_from,
    lsem, ssem, rsem,
):
    me = lax.axis_index("graph")
    core = lax.axis_index("chan")
    other = 1 - core
    grid_rows = grid_ref.shape[0]
    mesh_rows = embed_ref.shape[0]
    owners = mesh_rows // OWN
    span = cap_near(dst_ref.shape[2])
    used = (2 * REACH + 1) * span
    half = hid_out.shape[1]
    quarter = prj_out.shape[1]
    bf = jnp.bfloat16
    dot = functools.partial(jnp.dot, preferred_element_type=jnp.float32)

    pairs = (
        (src_hbm, src_ref), (dst_hbm, dst_ref), (count_hbm, count_ref), (grid_hbm, grid_ref), (embed_hbm, embed_ref),
        (wdec_hbm, wdec_ref), (wsrc_hbm, wsrc_ref), (bias_hbm, bias_ref), (wnode_hbm, wnode_ref),
    )
    SRC, DSTS, COUNT, GRID, EMBED, WDEC, WSRC, BIAS, WNODE = (
        pltpu.make_async_copy(x, y, lsem.at[i]) for i, (x, y) in enumerate(pairs))
    for copy in (SRC, DSTS, COUNT, GRID, EMBED, WDEC, WSRC, BIAS, WNODE):
        copy.start()

    tall, wide = torus(n)
    codes = [r * 2 * wide + c for r, c in visit_order(n)]
    groups = [codes[i:i + GROUP] for i in range(0, n - 1, GROUP)]
    spot = 2 * wide * (me // wide) + lax.rem(me, wide) + core * (2 * wide * tall + wide)
    turn = 1 - 2 * core

    def each_peer(visit):
        @pl.loop(0, len(groups))
        def _(g):
            for part in (range(0, 4), range(4, GROUP)):
                packed = jnp.int32(0)
                for i, group in enumerate(groups):
                    packed = jnp.where(g == i, sum(group[k] << (7 * j) for j, k in enumerate(part)), packed)
                for j in range(len(part)):
                    code = lax.shift_right_logical(packed, jnp.int32(7 * j)) & 127
                    at = spot + turn * code
                    visit((lax.shift_right_logical(at, jnp.int32(1)) & ((tall - 1) * wide)) + (at & (wide - 1)))

    per_row = owners // tall

    def seat(shard):
        r = lax.shift_right_logical(shard, jnp.int32(wide.bit_length() - 1))
        rank = (shard + 3 * r) & (wide - 1)
        return rank < per_row, r * per_row + rank

    mine, my_block = seat(me)
    barrier = pltpu.get_barrier_semaphore()
    each_peer(lambda peer: pl.semaphore_signal(barrier, inc=1, device_id={"graph": peer}, device_id_type=MESH_ID))
    pl.semaphore_signal(barrier, inc=1, device_id={"chan": other}, device_id_type=MESH_ID)

    def to_graph(src, dst, k, peer):
        return pltpu.make_async_remote_copy(
            src_ref=src, dst_ref=dst, send_sem=ssem.at[k], recv_sem=rsem.at[k],
            device_id={"graph": peer}, device_id_type=MESH_ID)

    def to_core(src, dst, k):
        return pltpu.make_async_remote_copy(
            src_ref=src, dst_ref=dst, send_sem=ssem.at[k], recv_sem=rsem.at[k],
            device_id={"chan": other}, device_id_type=MESH_ID)

    def wait_in(ref, k):
        to_graph(ref, ref, k, me).wait_recv()

    def wait_out(ref, k):
        to_graph(ref, ref, k, me).wait_send()

    DST, EMB, BASE, NEAR, PART, FWDB, FWDN, HID, PRJ, BACK, NBACK, HOT, PRJ0, HIDH, PRJH = range(SEMS)

    blocks = (n * HALF) // CHUNK
    capacity = dst_ref.shape[2]
    SRC.wait()
    DSTS.wait()
    COUNT.wait()
    with jax.named_scope("index"):
        ids = lax.broadcasted_iota(jnp.int32, (n, n), 0)
        cols = lax.broadcasted_iota(jnp.int32, (n, n), 1)
        counts = count_ref[...]
        apart = jnp.abs(ids - cols)
        far_counts = jnp.where(jnp.minimum(apart, n - apart) > REACH, counts, 0)
        hot = jnp.max(jnp.where(far_counts > KEEP, cols, 0))
        first = jnp.min(jnp.where(far_counts > KEEP, cols, n))
        fits_ref[0] = jnp.where(hot <= first, 1, 0)
        sent = jnp.where(ids == me, counts, 0).sum(axis=0, keepdims=True)
        sent = jnp.where(ids == cols, sent, 0).sum(axis=1, keepdims=True)
        came = jnp.where(cols == me, counts, 0).sum(axis=1, keepdims=True)
        pos = lax.broadcasted_iota(jnp.int32, (n, capacity), 1)
        src_all = jnp.where(pos < sent, src_ref[0] + 1, 0).astype(jnp.float32)
        src_live[...] = src_all
        came = jnp.where(me == hot, 0, came)
        dst_all = jnp.where(pos < came, dst_ref[:, 0, :] + 1, 0).astype(jnp.float32)
        dst_live[...] = dst_all
        rows_id = lax.broadcasted_iota(jnp.int32, (n, capacity), 0)
        src_all = jnp.where(rows_id == hot, 0.0, src_all)
        near_id = lax.broadcasted_iota(jnp.int32, (8, capacity), 0)
        near_src = jnp.zeros((8, capacity), jnp.float32)
        near_dst = jnp.zeros((8, capacity), jnp.float32)
        for o in range(-REACH, REACH + 1):
            to = lax.rem(me + o + n, n)
            row = jnp.where(to == hot, 0.0, src_live[pl.ds(to, 1)])
            near_src = jnp.where(near_id == o + REACH, row, near_src)
            near_dst = jnp.where(near_id == o + REACH, dst_live[pl.ds(lax.rem(me - o + n, n), 1)], near_dst)
        for h in range(2):
            base = base_layout(capacity, h)
            srcx_ref[h, 0:blocks] = lay_out(src_all, *base)
            dstx_ref[h, 0:blocks] = lay_out(dst_all, *base)
            near = near_layout(capacity, h)
            srcx_ref[h, blocks:] = lay_out(near_src, *near)[:, 0:CHUNK]
            dstx_ref[h, blocks:] = lay_out(near_dst, *near)[:, 0:CHUNK]

    GRID.wait()

    for j in range(blocks):
        rows = pick_turned(grid_ref[...], srcx_ref[core, j:j + 1]).T.astype(bf)
        base_out[j * (CHUNK // HALF):(j + 1) * (CHUNK // HALF)] = rows.reshape(CHUNK // HALF, HALF, rows.shape[1])

    near_out[...] = pick_turned(grid_ref[...], srcx_ref[core, blocks:]).T.astype(bf)
    near_in[core, used:, :] = jnp.zeros((NEAR_ROWS - used, near_in.shape[2]), bf)

    pl.semaphore_wait(barrier, n)
    each_peer(lambda peer: to_graph(dst_ref.at[peer], dst_in.at[me], DST, peer).start())
    for o in range(-REACH, REACH + 1):
        rows = pl.ds((o + REACH) * span, span)
        if o == 0:
            near_in[core, (o + REACH) * span:(o + REACH + 1) * span] = near_out[(o + REACH) * span:(o + REACH + 1) * span]
        else:
            to_graph(near_out.at[rows], near_in.at[core, rows], NEAR, lax.rem(me + o + n, n)).start()
    each_peer(lambda peer: to_graph(base_out.at[peer], base_in.at[core, me], BASE, peer).start())
    base_in[core, pl.ds(me, 1)] = base_out[pl.ds(me, 1)]
    dst_in[pl.ds(me, 1)] = dst_ref[pl.ds(me, 1)]

    EMBED.wait()
    WDEC.wait()
    w_other = wdec_ref[:, pl.ds(pl.multiple_of(other * quarter, quarter), quarter)]
    w_own = wdec_ref[:, pl.ds(pl.multiple_of(core * quarter, quarter), quarter)]
    prj_out[...] = dot(embed_ref[...], w_other).astype(bf)
    send0 = to_core(prj_out, emb_half, PRJ0)
    send0.start()
    WSRC.wait()
    BIAS.wait()
    hot_src = src_live[pl.ds(hot, 1)].astype(jnp.int32) - 1
    msgs = silu(dot(pick_turned(grid_ref[...], hot_src).T.astype(bf), wsrc_ref[...]) + bias_ref[...]).astype(bf)
    emb_own = dot(embed_ref[...], w_own)
    send0.wait_recv()
    emb_out[...] = (emb_own + emb_half[...].astype(jnp.float32)).astype(bf).reshape(owners, OWN, quarter)

    wait_in(dst_in.at[pl.ds(0, n - 1)], DST)
    hot_dst = jnp.where(hot_src >= 0, dst_in[hot], -1)
    part_out[...] = dot(spread(mesh_rows, hot_dst), msgs).astype(bf).reshape(owners, OWN, half)

    def to_owner(copy_to):
        def visit(peer):
            owns, block = seat(peer)

            @pl.when(owns)
            def _():
                copy_to(peer, block).start()
        return visit

    each_peer(to_owner(lambda peer, block: to_graph(part_out.at[block], part_in.at[me], PART, peer)))

    wait_in(base_in.at[core, pl.ds(0, n - 1)], BASE)
    to_core(base_in.at[core], base_in.at[core], FWDB).start()
    wait_in(near_in.at[core, pl.ds(0, 2 * REACH * span)], NEAR)
    to_core(near_in.at[core], near_in.at[core], FWDN).start()
    each_peer(to_owner(lambda peer, block: to_graph(emb_out.at[block], emb_in.at[me], EMB, peer)))

    def share(rows, idx):
        m = silu(dot(rows, wsrc_ref[...]) + bias_ref[...]).astype(bf)
        return dot(spread(mesh_rows, idx), m)

    def half_sum(h):
        total = share(near_in[h], dstx_ref[h, blocks:])
        for j in range(blocks):
            rows = base_in[h, j * (CHUNK // HALF):(j + 1) * (CHUNK // HALF)].reshape(CHUNK, base_in.shape[3])
            total = total + share(rows, dstx_ref[h, j:j + 1])
        return total

    acc[...] = half_sum(core)
    to_core(base_in.at[other], base_in.at[other], FWDB).wait_recv()
    to_core(near_in.at[other], near_in.at[other], FWDN).wait_recv()

    WNODE.wait()
    n_other = wnode_ref[:, pl.ds(pl.multiple_of(other * half, half), half)]
    n_own = wnode_ref[:, pl.ds(pl.multiple_of(core * half, half), half)]
    agg = (acc[...] + half_sum(other)).astype(bf)
    hid_out[...] = dot(agg, n_other).astype(bf)
    send = to_core(hid_out, hid_in, HID)
    send.start()
    own = dot(agg, n_own)
    send0.wait_send()
    send.wait_recv()
    lat = (embed_ref[...].astype(jnp.float32) + silu(own + hid_in[...].astype(jnp.float32))).astype(bf)
    prj_out[...] = dot(lat, w_other).astype(bf)
    send2 = to_core(prj_out, prj_in, PRJ)
    send2.start()
    own_p = dot(lat, w_own)

    send2.wait_recv()
    prj_bf[...] = (own_p + prj_in[...].astype(jnp.float32)).astype(bf)
    for h in range(2):
        for j in range(blocks):
            rows = pick_turned(prj_bf[...], dstx_ref[h, j:j + 1]).T.astype(bf)
            back_out[h, j * (CHUNK // HALF):(j + 1) * (CHUNK // HALF)] = rows.reshape(CHUNK // HALF, HALF, quarter)
        back_in[h, pl.ds(me, 1)] = back_out[h, pl.ds(me, 1)]

    each_peer(lambda peer: to_graph(back_out.at[:, peer], back_in.at[:, me], BACK, peer).start())
    for h in range(2):
        nback_out[h] = pick_turned(prj_bf[...], dstx_ref[h, blocks:]).T.astype(bf)
        nback_in[h, used:, :] = jnp.zeros((NEAR_ROWS - used, quarter), bf)
        for o in range(-REACH, REACH + 1):
            a = (o + REACH) * span
            if o == 0:
                nback_in[h, a:a + span] = nback_out[h, a:a + span]
            else:
                to_graph(nback_out.at[h, pl.ds(a, span)], nback_in.at[h, pl.ds(a, span)], NBACK, lax.rem(me - o + n, n)).start()

    @pl.when(mine)
    def _():
        wait_in(part_in.at[pl.ds(0, n - 1)], PART)
        part_in[pl.ds(me, 1)] = part_out[pl.ds(my_block, 1)]

    hot_agg = part_in[...].astype(jnp.float32).sum(axis=0).astype(bf)
    hhid_out[...] = dot(hot_agg, n_other)
    send3 = to_core(hhid_out, hhid_in, HIDH)
    send3.start()
    hot_own = dot(hot_agg, n_own)

    send3.wait_recv()
    hot_lat = silu(hot_own + hhid_in[...]).astype(bf)
    hprj_out[...] = dot(hot_lat, w_other)
    send4 = to_core(hprj_out, hprj_in, PRJH)
    send4.start()
    hot_prj = dot(hot_lat, w_own)

    @pl.when(mine)
    def _():
        wait_in(emb_in.at[pl.ds(0, n - 1)], EMB)
        emb_in[pl.ds(me, 1)] = emb_out[pl.ds(my_block, 1)]

    send4.wait_recv()
    hot_out[...] = (hot_prj + hprj_in[...] + emb_in[hot].astype(jnp.float32)).astype(bf)

    @pl.when(mine)
    def _():
        each_peer(lambda peer: to_graph(hot_out, hot_in.at[my_block], HOT, peer).start())

    wait_in(nback_in.at[:, pl.ds(0, 2 * REACH * span)], NBACK)
    total = grid_ref[:, pl.ds(pl.multiple_of(core * quarter, quarter), quarter)].astype(jnp.float32)
    for h in range(2):
        total = total + dot(spread(grid_rows, srcx_ref[h, blocks:]), nback_in[h])
    dec[...] = total
    wait_in(back_in.at[:, pl.ds(0, n - 1)], BACK)
    total = dec[...]
    for h in range(2):
        for j in range(blocks):
            rows = back_in[h, j * (CHUNK // HALF):(j + 1) * (CHUNK // HALF)].reshape(CHUNK, quarter)
            total = total + dot(spread(grid_rows, srcx_ref[h, j:j + 1]), rows)
    dec[...] = total

    hot_to[...] = spread(grid_rows, hot_src)
    hot_from[...] = spread(mesh_rows, hot_dst)

    @pl.when(mine)
    def _():
        wait_in(hot_in.at[pl.ds(0, owners - 1)], HOT)
        hot_in[pl.ds(my_block, 1)] = hot_out[...].reshape(1, OWN, quarter)

    @pl.when(jnp.logical_not(mine))
    def _():
        wait_in(hot_in, HOT)

    hot_rows = lax.dot_general(
        hot_in[...].reshape(mesh_rows, quarter), hot_from[...], (((0,), (0,)), ((), ())), preferred_element_type=jnp.float32
    ).astype(bf)
    back = lax.dot_general(hot_to[...], hot_rows, (((1,), (1,)), ((), ())), preferred_element_type=jnp.float32)
    out_ref[...] = (dec[...] + back).astype(bf)

    wait_out(dst_ref.at[pl.ds(0, n - 1)], DST)
    wait_out(base_out.at[pl.ds(0, n - 1)], BASE)
    wait_out(near_out.at[pl.ds(0, 2 * REACH * span)], NEAR)

    @pl.when(mine)
    def _():
        wait_out(emb_out.at[pl.ds(0, owners - 1)], EMB)
        wait_out(part_out.at[pl.ds(0, owners - 1)], PART)
        wait_out(back_out.at[0, pl.ds(0, n - 1)], HOT)

    @pl.when(jnp.logical_not(mine))
    def _():
        wait_out(emb_out, EMB)
        wait_out(part_out, PART)

    to_core(base_in.at[core], base_in.at[core], FWDB).wait_send()
    to_core(near_in.at[core], near_in.at[core], FWDN).wait_send()
    for copy in (send, send2, send3, send4):
        copy.wait_send()
    wait_out(back_out.at[:, pl.ds(0, n - 1)], BACK)
    wait_out(nback_out.at[:, pl.ds(0, 2 * REACH * span)], NBACK)


def cap_near(capacity):
    return (capacity - KEEP) // 2


def lay_out(table, take, mark):
    high = jnp.floor(table * (1.0 / 32.0))
    low = table - 32.0 * high
    dot = functools.partial(jnp.dot, preferred_element_type=jnp.float32)
    moved = 32.0 * dot(high.astype(jnp.bfloat16), take) + dot(low.astype(jnp.bfloat16), take)
    group = mark.shape[0]
    moved = moved.reshape(table.shape[0] // group, group, take.shape[1])
    return (moved * mark[None]).sum(axis=1).astype(jnp.int32) - 1


def base_layout(capacity, h):
    shape = (capacity, CHUNK)
    lane = lax.broadcasted_iota(jnp.int32, shape, 1)
    slot = lax.broadcasted_iota(jnp.int32, shape, 0)
    take = jnp.where(slot == h * HALF + (lane & (HALF - 1)), 1.0, 0.0).astype(jnp.bfloat16)
    group = CHUNK // HALF
    lane = lax.broadcasted_iota(jnp.int32, (group, CHUNK), 1)
    row = lax.broadcasted_iota(jnp.int32, (group, CHUNK), 0)
    return take, jnp.where(row * HALF <= lane, 1.0, 0.0) * jnp.where(lane < row * HALF + HALF, 1.0, 0.0)


def near_layout(capacity, h):
    span = cap_near(capacity)
    count = 2 * REACH + 1
    shape = (capacity, NEAR_ROWS)
    lane = lax.broadcasted_iota(jnp.int32, shape, 1)
    slot = lax.broadcasted_iota(jnp.int32, shape, 0)
    within = lane
    for i in range(1, count + 1):
        within = within - jnp.where(lane >= i * span, span, 0)
    take = jnp.where(slot == KEEP + h * span + within, 1.0, 0.0).astype(jnp.bfloat16)
    lane = lax.broadcasted_iota(jnp.int32, (8, NEAR_ROWS), 1)
    row = lax.broadcasted_iota(jnp.int32, (8, NEAR_ROWS), 0)
    inside = jnp.where(row * span <= lane, 1.0, 0.0) * jnp.where(lane < row * span + span, 1.0, 0.0)
    return take, inside * jnp.where(row < count, 1.0, 0.0)


def compact(grid_state, w_src, bias_src, mesh_embed, w_node, w_dec, slot_src, slot_dst, slot_count):
    n = lax.axis_size("graph")
    capacity = slot_src.shape[2]
    grid_rows, width = grid_state.shape
    mesh_rows, half = mesh_embed.shape
    quarter = width // 2
    owners = mesh_rows // OWN
    bf, f32 = jnp.bfloat16, jnp.float32
    vm = pltpu.VMEM
    return pl.pallas_call(
        functools.partial(step_kernel, n),
        out_shape=(jax.ShapeDtypeStruct((grid_rows, quarter), bf), jax.ShapeDtypeStruct((1,), jnp.int32)),
        in_specs=[pl.BlockSpec(memory_space=pl.ANY)] * 9,
        out_specs=(pl.BlockSpec(memory_space=vm), pl.BlockSpec(memory_space=pltpu.SMEM)),
        scratch_shapes=[
            vm((grid_rows, width), bf), vm(w_src.shape, bf), vm((1, half), f32), vm((mesh_rows, half), bf), vm(w_node.shape, bf),
            vm(w_dec.shape, bf), vm(slot_src.shape, jnp.int32), vm(slot_dst.shape, jnp.int32), vm(slot_count.shape, jnp.int32),
            vm((n, capacity), f32), vm((n, capacity), f32),
            vm((2, n * HALF // CHUNK + 1, CHUNK), jnp.int32), vm((2, n * HALF // CHUNK + 1, CHUNK), jnp.int32),
            vm((n, HALF, width), bf), vm((NEAR_ROWS, width), bf),
            vm((2, n, HALF, width), bf), vm((2, NEAR_ROWS, width), bf),
            vm((n, 1, capacity), jnp.int32), vm((n, OWN, quarter), bf), vm((owners, OWN, quarter), bf), vm((mesh_rows, quarter), bf),
            vm((owners, OWN, half), bf), vm((n, OWN, half), bf),
            vm((mesh_rows, half), f32),
            vm((mesh_rows, half), bf), vm((mesh_rows, half), bf),
            vm((mesh_rows, quarter), bf), vm((mesh_rows, quarter), bf), vm((mesh_rows, quarter), bf),
            vm((2, n, HALF, quarter), bf), vm((2, NEAR_ROWS, quarter), bf),
            vm((2, n, HALF, quarter), bf), vm((2, NEAR_ROWS, quarter), bf),
            vm((OWN, quarter), bf), vm((owners, OWN, quarter), bf),
            vm((grid_rows, quarter), f32),
            vm((OWN, half), f32), vm((OWN, half), f32), vm((OWN, quarter), f32), vm((OWN, quarter), f32),
            vm((grid_rows, capacity), bf), vm((mesh_rows, capacity), bf),
            pltpu.SemaphoreType.DMA((9,)), pltpu.SemaphoreType.DMA((SEMS,)), pltpu.SemaphoreType.DMA((SEMS,)),
        ],
        compiler_params=pltpu.CompilerParams(collective_id=0, has_side_effects=True, vmem_limit_bytes=48 * 1024 * 1024),
    )(grid_state, w_src, bias_src[None, :], mesh_embed, w_node, w_dec, slot_src, slot_dst, slot_count)


def on_device(grid_state, w_src, bias_src, mesh_embed, w_node, w_dec, slot_src, slot_dst, slot_count):
    args = (grid_state, w_src, bias_src, mesh_embed, w_node, w_dec, slot_src, slot_dst, slot_count)
    result, fits = compact(*args)
    return lax.cond(fits[0] > 0, lambda: result, lambda: dense(*args))


def solution(mesh):
    placed = (
        P(("member", "graph"), None),
        P(None, "chan"),
        P("chan"),
        P("graph", "chan"),
        P("chan", None),
        P("chan", None),
        P("graph", None, None),
        P(None, "graph", None),
        P(),
    )
    return jax.shard_map(
        on_device,
        mesh=mesh,
        in_specs=placed,
        out_specs=P(("member", "graph"), "chan"),
        check_vma=False,
    )
```
